32 devices in a mesh: member: 2 (over y), blk: 16 (over z, x, core).
Axes of the slice: x: 2, y: 2, z: 4, core: 2. Of those that a mesh axis runs over, the one named last changes fastest.
Arguments:
- heat_anomaly: float32 [8, 1536, 512], P('member', 'blk'), parts along dimension 0, may hold values from -6 to 6
- saltiness_anomaly: float32 [8, 1536, 512], P('member', 'blk'), parts along dimension 0, may hold values from -6 to 6
- first_axis_flow: float32 [8, 1536, 512], P('member', 'blk'), parts along dimension 0, may hold values from -4 to 4
- second_axis_flow: float32 [8, 1536, 512], P('member', 'blk'), parts along dimension 0, may hold values from -4 to 4
- layer_spacing: float32 [4], replicated, may hold values from 0.5 to 4
- diagonal_shift: float32 [1536, 512], P('blk'), may hold values from 0.02 to 0.2
- water_tile_flags: int32 [16, 8], P('blk'), may hold values 0 or 1
Outputs:
- new_temperature: bfloat16 [8, 1536, 512], P('member', 'blk'), parts along dimension 0
- new_salinity: bfloat16 [8, 1536, 512], P('member', 'blk'), parts along dimension 0
- new_u: bfloat16 [8, 1536, 512], P('member', 'blk'), parts along dimension 0
- new_v: bfloat16 [8, 1536, 512], P('member', 'blk'), parts along dimension 0
- height: float32 [3072, 512], P(('member', 'blk')), parts along dimension 0
- residual: float32 [3072, 512], P(('member', 'blk')), parts along dimension 0
The draws below stay inside these ranges and needn't reach their ends.
There are 2 independent parts, one for each index of `member`. The reference program is written for one: setup_inputs(seed, part) draws one part's arguments, and reference() takes and returns one part's arrays. A program takes and returns all parts, laid end to end along the dimension named above; an argument that names none is the same for every part. Nothing has to cross between parts.
Inputs may be any that keep to these rules, and one draw needn't show every extreme that they name: `water_tile_flags`: 1 marks an ocean block, 0 a land block.
All inputs are finite; a program needn't handle non-finite values.
Results may differ from the reference program's by a relative error of at most 0.001.
Values sent between devices are 32-bit elements; how exact they have to be, the bound alone decides.
No kernel may reach another device: no remote copies, remote signals or barrier semaphores. Data moves between devices by JAX's collectives and lax.ppermute only.
A program may use at most 128 MiB of HBM per device.

```python
import math
import jax
import jax.numpy as jnp
import numpy as np
from jax import lax

BX = 96
BY = 64
HOME = 8
LAYER_TOTAL = 4
SSTEP = 4
CG_BLOCKS = 3
GRID_WIDTH_X = 1536
GRID_WIDTH_Y = 512
N_BLK = 16


def set_ends(drawn, own_key, low, largest):
    dims = drawn.shape
    index_at = [jax.random.randint(jax.random.fold_in(own_key, axis), (), 0, dims[axis]) for axis in range(len(dims))]
    drawn = drawn.at[tuple(index_at)].set(low)
    longest = dims.index(max(dims))
    index_at[longest] = (index_at[longest] + 1) % dims[longest]
    return drawn.at[tuple(index_at)].set(largest)


def steps_of(rng, shape, cuts, least, high):
    factor_of, own = 1.0, jax.random.fold_in(rng, 6)
    for axis_at, parts in cuts:
        draws = jnp.exp(jax.random.uniform(jax.random.fold_in(own, axis_at), (parts,), jnp.float32, least / len(cuts), high / len(cuts)))
        factor_of = factor_of * jnp.repeat(draws, shape[axis_at] // parts).reshape([-1 if axis == axis_at else 1 for axis in range(len(shape))])
    return factor_of


def gaussian(own_key, shape, scale, bound, pieces=(), kind=jnp.bfloat16):
    array = jax.random.normal(own_key, shape, jnp.float32) * scale
    if len(pieces) > 0:
        array = steps_of(own_key, shape, pieces, -0.22, 0.18) * array
    return jnp.clip(array, min=-bound, max=bound).astype(kind)


def setup_inputs(seed: int = 0, part: int = 0) -> dict:
    seeds = jax.random.split(jax.random.key(seed), 8)
    part_keys = jax.random.split(jax.random.fold_in(seeds[7], part), 8)
    return {
        "heat_anomaly": gaussian(part_keys[0], (LAYER_TOTAL, GRID_WIDTH_X, GRID_WIDTH_Y), 1.0, 6.0, ((1, 16),), jnp.float32),
        "saltiness_anomaly": gaussian(part_keys[1], (LAYER_TOTAL, GRID_WIDTH_X, GRID_WIDTH_Y), 1.0, 6.0, ((1, 16),), jnp.float32),
        "first_axis_flow": gaussian(part_keys[2], (LAYER_TOTAL, GRID_WIDTH_X, GRID_WIDTH_Y), 1.0, 4.0, ((1, 16),), jnp.float32),
        "second_axis_flow": gaussian(part_keys[3], (LAYER_TOTAL, GRID_WIDTH_X, GRID_WIDTH_Y), 1.0, 4.0, ((1, 16),), jnp.float32),
        "layer_spacing": jnp.clip(jnp.exp(jax.random.uniform(seeds[4], (LAYER_TOTAL,), jnp.float32, math.log(0.5), math.log(4.0))), 0.5, 4.0),
        "diagonal_shift": jnp.clip(jnp.exp(math.log(0.2) - 2.3025851 * jax.random.uniform(seeds[5], (GRID_WIDTH_X, GRID_WIDTH_Y), jnp.float32) ** steps_of(seeds[5], (GRID_WIDTH_X, GRID_WIDTH_Y), ((0, 16),), -0.2, 0.2)), 0.02, 0.2),
        "water_tile_flags": set_ends((jax.random.randint(seeds[6], (N_BLK, HOME), 0, 4) < 3).astype(jnp.int32), jax.random.fold_in(seeds[6], 1), 0, 1),
    }


COURANT = 0.2
HIGHEST = lax.Precision.HIGHEST


def wrap_east(field, margin):
    extent = field.shape[0]
    return jnp.concatenate([field[extent - margin:], field, field[:margin]], axis=0)


def pad_north(field):
    return jnp.pad(field, [(0, 0)] * (field.ndim - 1) + [(1, 1)])


def upwind(speed, behind, ahead):
    return jnp.where(speed > 0.0, speed * behind, speed * ahead)


def advect(tracer, east_vel, north_vel, wet_pad):
    east_face = 0.5 * (east_vel[..., :-1, 1:-1] + east_vel[..., 1:, 1:-1]) * (wet_pad[:-1, 1:-1] * wet_pad[1:, 1:-1])
    east_flux = upwind(east_face, tracer[..., :-1, 1:-1], tracer[..., 1:, 1:-1])
    north_face = 0.5 * (north_vel[..., 1:-1, :-1] + north_vel[..., 1:-1, 1:]) * (wet_pad[1:-1, :-1] * wet_pad[1:-1, 1:])
    north_flux = upwind(north_face, tracer[..., 1:-1, :-1], tracer[..., 1:-1, 1:])
    spread = (east_flux[..., 1:, :] - east_flux[..., :-1, :]) + (north_flux[..., 1:] - north_flux[..., :-1])
    return wet_pad[1:-1, 1:-1] * (tracer[..., 1:-1, 1:-1] - COURANT * spread)


def operate(field_band, wet_band, damp_core):
    values = pad_north(field_band)
    wetness = pad_north(wet_band)
    masked = wetness * values
    edges = (masked[:-2, 1:-1] + masked[2:, 1:-1]) + (masked[1:-1, :-2] + masked[1:-1, 2:])
    corners = (masked[:-2, :-2] + masked[:-2, 2:]) + (masked[2:, :-2] + masked[2:, 2:])
    centre = values[1:-1, 1:-1]
    wet_core = wetness[1:-1, 1:-1]
    return 0.125 * (wet_core * ((6.0 + damp_core) * centre - (edges + 0.5 * corners)) + (1.0 - wet_core) * centre)


def chebyshev_next(image, current, previous):
    if previous is None:
        return 2.0 * image - current
    return 4.0 * image - 2.0 * current - previous


def shift_table(powers):
    extent = 2 * powers + 1
    table = np.zeros((extent, extent), np.float32)
    for offset, count in ((0, powers), (powers + 1, powers - 1)):
        for place in range(count):
            source = offset + place
            if place == 0:
                table[source + 1, source] = 0.5
                table[source, source] = 0.5
            else:
                table[source + 1, source] = 0.25
                table[source, source] = 0.5
                table[source - 1, source] = 0.25
    return table


def inner_steps(gram, powers):
    extent = 2 * powers + 1
    table = jnp.asarray(shift_table(powers), gram.dtype)
    unit = jnp.eye(extent, dtype=gram.dtype)
    along = unit[0]
    resid = unit[powers + 1]
    offset = jnp.zeros((extent,), gram.dtype)
    for sweep in range(powers):
        norm_now = jnp.dot(resid, jnp.dot(gram, resid, precision=HIGHEST), precision=HIGHEST)
        image = jnp.dot(table, along, precision=HIGHEST)
        alpha = norm_now / jnp.dot(along, jnp.dot(gram, image, precision=HIGHEST), precision=HIGHEST)
        offset = offset + alpha * along
        resid = resid - alpha * image
        norm_next = jnp.dot(resid, jnp.dot(gram, resid, precision=HIGHEST), precision=HIGHEST)
        along = resid + (norm_next / norm_now) * along
    return offset, resid, along


def reference(heat_anomaly, saltiness_anomaly, first_axis_flow, second_axis_flow, layer_spacing, diagonal_shift, water_tile_flags):
    ocean = jnp.repeat(jnp.repeat(water_tile_flags.astype(diagonal_shift.dtype), BX, axis=0), BY, axis=1)
    wet_band = wrap_east(ocean, 1)
    wet_pad = pad_north(wet_band)

    def column_layer_advance(layers):
        padded = [pad_north(wrap_east(layer, 1)) for layer in layers]
        return jnp.stack([advect(tracer, padded[2], padded[3], wet_pad) for tracer in padded])

    stepped_fields = lax.map(column_layer_advance, (heat_anomaly, saltiness_anomaly, first_axis_flow, second_axis_flow))
    weights = layer_spacing / jnp.sum(layer_spacing)
    transport_u = jnp.einsum("k,kxy->xy", weights, stepped_fields[:, 2], precision=HIGHEST)
    transport_v = jnp.einsum("k,kxy->xy", weights, stepped_fields[:, 3], precision=HIGHEST)
    east_band = wrap_east(transport_u, 1)
    north_pad = pad_north(transport_v)
    forcing = ocean * (0.5 * ((east_band[2:] - east_band[:-2]) + (north_pad[:, 2:] - north_pad[:, :-2])))

    def apply_whole(field):
        return operate(wrap_east(field, 1), wet_band, diagonal_shift)

    def chebyshev_list(start, count):
        result = [start]
        previous = None
        for power in range(count):
            following = chebyshev_next(apply_whole(result[-1]), result[-1], previous)
            previous = result[-1]
            result.append(following)
        return result

    height = jnp.zeros_like(forcing)
    resid = forcing
    along = forcing
    for outer in range(CG_BLOCKS):
        along_list = chebyshev_list(along, SSTEP)
        resid_list = chebyshev_list(resid, SSTEP - 1)
        basis = jnp.stack(along_list + resid_list)
        gram = jnp.einsum("aij,bij->ab", basis, basis, precision=HIGHEST)
        offset, resid_coef, along_coef = inner_steps(gram, SSTEP)
        height = height + jnp.einsum("a,aij->ij", offset, basis, precision=HIGHEST)
        resid = jnp.einsum("a,aij->ij", resid_coef, basis, precision=HIGHEST)
        along = jnp.einsum("a,aij->ij", along_coef, basis, precision=HIGHEST)
    return (stepped_fields[:, 0].astype(jnp.bfloat16), stepped_fields[:, 1].astype(jnp.bfloat16),
            stepped_fields[:, 2].astype(jnp.bfloat16), stepped_fields[:, 3].astype(jnp.bfloat16), height, resid)
```

```python
import functools

import jax
import jax.numpy as jnp
from jax import lax
from jax.experimental import pallas as pl
from jax.experimental.pallas import tpu as pltpu
from jax.sharding import PartitionSpec as P

SSTEP = 4
CG_BLOCKS = 3
STEPS = SSTEP * CG_BLOCKS
COURANT = 0.2
PAD = 16
MARGIN = 8
BASE = PAD + MARGIN


def shift(value, amount, axis):
    return pltpu.roll(value, amount % value.shape[axis], axis)


def two_sum(a, b):
    s = a + b
    t = s - a
    return s, (a - (s - t)) + (b - t)


def fast_two_sum(a, b):
    s = a + b
    return s, b - (s - a)


def split(a):
    c = 4097.0 * a
    hi = c - (c - a)
    return hi, a - hi


def two_prod(a, b):
    p = a * b
    ah, al = split(a)
    bh, bl = split(b)
    return p, ((ah * bh - p) + ah * bl + al * bh) + al * bl


def pair_add(a, b):
    s, e = two_sum(a[0], b[0])
    return fast_two_sum(s, e + (a[1] + b[1]))


def pair_scale(a, c):
    p, e = two_prod(a[0], c)
    return p, e + a[1] * c


def upwind(speed, behind, ahead):
    return jnp.where(speed > 0.0, speed * behind, speed * ahead)


def face_speeds(u, v, east_wet, north_wet):
    east = 0.5 * (u + shift(u, -1, 0))[: 3 * MARGIN] * east_wet
    centre = v[MARGIN : 3 * MARGIN]
    north = 0.5 * (centre + shift(centre, -1, 1)) * north_wet
    return east, north


def advect(q, east, north, wet):
    east_flux = upwind(east, q[: 3 * MARGIN], shift(q, -1, 0)[: 3 * MARGIN])
    centre = q[MARGIN : 3 * MARGIN]
    north_flux = upwind(north, centre, shift(centre, -1, 1))
    spread = (east_flux - shift(east_flux, 1, 0))[MARGIN:] + (
        north_flux - shift(north_flux, 1, 1)
    )
    return wet * (centre - COURANT * spread)


def level_weight(spacing, level):
    total = spacing[0]
    for k in range(1, spacing.shape[0]):
        total = total + spacing[k]
    return spacing[level] / total


def north_wetness(wet):
    lane = lax.broadcasted_iota(jnp.int32, wet.shape, 1)
    return jnp.where(lane == wet.shape[1] - 1, 0.0, wet * shift(wet, -1, 1))


def inner_kernel(spacing, heat, salt, u, v, wet_ref, o_heat, o_salt, o_u, o_v, t_u, t_v):
    level = pl.program_id(0)
    width = u.shape[1]
    weight = level_weight(spacing, level)
    wet = wet_ref[0:1]
    wet8 = wet_ref[...]
    north_wet = north_wetness(wet8)[0:1]
    east_wet = wet * wet

    @pl.when(level == 0)
    def _():
        t_u[...] = jnp.zeros_like(t_u)
        t_v[...] = jnp.zeros_like(t_v)

    def strip(index, carry):
        start = pl.multiple_of(PAD + index * PAD, PAD)
        rows = pl.ds(pl.multiple_of(start - MARGIN, MARGIN), 4 * MARGIN)
        keep = pl.ds(start, PAD)
        qu = u[0, rows]
        qv = v[0, rows]
        east, north = face_speeds(qu, qv, east_wet, north_wet)
        au = advect(qu, east, north, wet)
        av = advect(qv, east, north, wet)
        o_u[0, keep] = au.astype(o_u.dtype)
        o_v[0, keep] = av.astype(o_v.dtype)
        t_u[keep] += weight * au
        t_v[keep] += weight * av
        o_heat[0, keep] = advect(heat[0, rows], east, north, wet).astype(o_heat.dtype)
        o_salt[0, keep] = advect(salt[0, rows], east, north, wet).astype(o_salt.dtype)
        return carry

    lax.fori_loop(0, width // PAD - 2, strip, 0)


def inner_advance(spacing, heat, salt, u, v, wet):
    levels, width, extent = u.shape
    block = pl.BlockSpec((1, width, extent), lambda k: (k, 0, 0))
    whole = pl.BlockSpec((width, extent), lambda k: (0, 0))
    tracer = jax.ShapeDtypeStruct(u.shape, jnp.bfloat16)
    plane = jax.ShapeDtypeStruct((width, extent), jnp.float32)
    return pl.pallas_call(
        inner_kernel,
        grid=(levels,),
        out_shape=[tracer] * 4 + [plane] * 2,
        in_specs=[pl.BlockSpec(memory_space=pltpu.SMEM)]
        + [block] * 4
        + [pl.BlockSpec(wet.shape, lambda k: (0, 0))],
        out_specs=[block] * 4 + [whole] * 2,
        cost_estimate=pl.CostEstimate(
            flops=10000000000, bytes_accessed=5000000, transcendentals=0
        ),
        name="inner_advance",
    )(spacing, heat, salt, u, v, wet)


def edge_kernel(
    spacing, heat, salt, u, v, damp, wet_ref, low, high, t_u, t_v, i_heat, i_salt, i_u, i_v,
    o_heat, o_salt, o_u, o_v, o_basis, o_sums,
    bands, tu, tv, ocean, diag, fields, corner, edge_out, acc, sems, out_sems, field_sems,
):
    levels, width, extent = u.shape
    span = width + 2 * BASE
    sources = (heat, salt, u, v)
    copies = []

    def fetch(src, dst):
        copy = pltpu.make_async_copy(src, dst, sems.at[len(copies)])
        copy.start()
        copies.append(copy)

    for side, message in ((0, low), (1, high)):
        fetch(message.at[2 * levels + 1], corner.at[side])
    for q in range(4):
        fetch(sources[q].at[:, 0:BASE], bands.at[q, 0, :, BASE : 2 * BASE])
        fetch(sources[q].at[:, width - BASE : width], bands.at[q, 1, :, 0:BASE])
    for side, message in ((0, low), (1, high)):
        rows = slice(MARGIN, BASE) if side == 0 else slice(BASE, BASE + PAD)
        fetch(message.at[0:levels], bands.at[2, side, :, rows])
        fetch(message.at[levels : 2 * levels], bands.at[3, side, :, rows])
    fetch(damp, diag.at[BASE : BASE + width])
    fetch(low.at[2 * levels], diag.at[MARGIN:BASE])
    fetch(high.at[2 * levels], diag.at[BASE + width : BASE + width + PAD])
    fetch(t_u.at[PAD : width - PAD], tu.at[BASE + PAD : BASE + width - PAD])
    fetch(t_v.at[PAD : width - PAD], tv.at[BASE + PAD : BASE + width - PAD])
    for copy in copies:
        copy.wait()

    wet8 = wet_ref[...]
    wet_low = corner[0, MARGIN:PAD]
    wet_high = corner[1, MARGIN:PAD]
    for block in range(span // MARGIN):
        value = wet8
        if block < BASE // MARGIN:
            value = wet_low
        if block >= (BASE + width) // MARGIN:
            value = wet_high
        ocean[block * MARGIN : (block + 1) * MARGIN] = value
    for q in range(2):
        for k in range(levels):
            row = q * levels + k
            bands[q, 0, k, BASE - 1 : BASE] = corner[0, row : row + 1]
            bands[q, 1, k, BASE : BASE + 1] = corner[1, row : row + 1]

    for side in range(2):
        first = 0 if side == 0 else width
        for place in range(2):
            start = MARGIN + place * PAD
            base = first + start
            owned = place == 1 - side
            wet = ocean[base : base + PAD]
            around = ocean[base - MARGIN : base + BASE]
            east_wet = (around * shift(around, -1, 0))[: 3 * MARGIN]
            north_wet = north_wetness(wet[:MARGIN])[0:1]

            def level_step(k, sums, side=side, start=start, owned=owned, wet=wet[0:1],
                           east_wet=east_wet, north_wet=north_wet):
                weight = level_weight(spacing, k)
                rows = slice(start - MARGIN, start + BASE)
                qu = bands[2, side, k, rows]
                qv = bands[3, side, k, rows]
                east, north = face_speeds(qu, qv, east_wet, north_wet)
                au = advect(qu, east, north, wet)
                av = advect(qv, east, north, wet)
                if owned:
                    edge_out[2, side, k] = au.astype(edge_out.dtype)
                    edge_out[3, side, k] = av.astype(edge_out.dtype)
                    for q in range(2):
                        edge_out[q, side, k] = advect(
                            bands[q, side, k, rows], east, north, wet
                        ).astype(edge_out.dtype)
                return sums[0] + weight * au, sums[1] + weight * av

            zero = jnp.zeros((PAD, extent), jnp.float32)
            su, sv = lax.fori_loop(0, levels, level_step, (zero, zero))
            tu[base : base + PAD] = su
            tv[base : base + PAD] = sv

    results = []
    for q, target in enumerate((o_heat, o_salt, o_u, o_v)):
        for side in range(2):
            first = 0 if side == 0 else width - PAD
            copy = pltpu.make_async_copy(
                edge_out.at[q, side], target.at[:, first : first + PAD], out_sems.at[2 * q + side]
            )
            copy.start()
            results.append(copy)

    lane = lax.broadcasted_iota(jnp.int32, (PAD, extent), 1)

    def north_of(x):
        return jnp.where(lane == extent - 1, 0.0, shift(x, -1, 1))

    def south_of(x):
        return jnp.where(lane == 0, 0.0, shift(x, 1, 1))

    strips = (width + 2 * PAD) // PAD
    none = jnp.zeros((MARGIN, 128), jnp.float32)

    def inner(a, b, total):
        product = a * b
        part = product[:MARGIN] + product[MARGIN:]
        pieces = [part[:, i : i + 128] for i in range(0, extent, 128)]
        while len(pieces) > 1:
            pieces = [x + y for x, y in zip(pieces[::2], pieces[1::2])]
        s, e = two_sum(total[0], pieces[0])
        return s, total[1] + e

    square = (none, none)
    for strip in range(strips):
        start = MARGIN + strip * PAD
        around = slice(start - MARGIN, start + BASE)
        keep = slice(start, start + PAD)
        wet = ocean[keep]
        flow = tu[around]
        east_part = (shift(flow, -1, 0) - shift(flow, 1, 0))[MARGIN:BASE]
        cross = tv[keep]
        start_field = wet * (0.5 * (east_part + (north_of(cross) - south_of(cross))))
        fields[0, keep] = jnp.zeros_like(start_field)
        fields[1, keep] = start_field
        diag[keep] = 0.5 * (wet * (6.0 + diag[keep]) + (1.0 - wet)) - 2.0
        if 0 < strip < strips - 1:
            square = inner(start_field, start_field, square)
    acc[0, 0:MARGIN] = square[0]
    acc[1, 0:MARGIN] = square[1]
    for row in range(2 * STEPS + 1, acc.shape[1] // MARGIN):
        acc[0, row * MARGIN : (row + 1) * MARGIN] = none
        acc[1, row * MARGIN : (row + 1) * MARGIN] = none

    def save(j):
        return pltpu.make_async_copy(
            fields.at[j + 1, BASE : BASE + width], o_basis.at[j], field_sems.at[j]
        )

    save(0).start()

    def basis_step(j, carry):
        scale = jnp.where(j == 0, 0.5, 1.0)
        mixed, square = (none, none), (none, none)
        for strip in range(strips):
            start = MARGIN + strip * PAD
            around = slice(start - MARGIN, start + BASE)
            keep = slice(start, start + PAD)
            wide = fields[j + 1, around]
            masked = wide * ocean[around]
            sides = (shift(masked, -1, 0) + shift(masked, 1, 0))[MARGIN:BASE]
            column = masked[MARGIN:BASE] + 0.5 * sides
            near = sides + (north_of(column) + south_of(column))
            centre = wide[MARGIN:BASE]
            image = diag[keep] * centre - (0.5 * ocean[keep]) * near
            following = scale * image - fields[j, keep]
            fields[j + 2, keep] = following
            if 0 < strip < strips - 1:
                mixed = inner(centre, following, mixed)
                square = inner(following, following, square)
        for place, value in ((2 * j + 1, mixed), (2 * j + 2, square)):
            at = pl.ds(pl.multiple_of(place * MARGIN, MARGIN), MARGIN)
            acc[0, at] = value[0]
            acc[1, at] = value[1]
        save(j + 1).start()
        return carry

    lax.fori_loop(0, STEPS, basis_step, 0)

    slots = acc.shape[1] // MARGIN
    pairs = [
        (acc[0, pl.ds(s, slots, stride=MARGIN)], acc[1, pl.ds(s, slots, stride=MARGIN)])
        for s in range(MARGIN)
    ]
    while len(pairs) > 1:
        pairs = [pair_add(x, y) for x, y in zip(pairs[::2], pairs[1::2])]
    total = pairs[0]
    step = 64
    while step:
        total = pair_add(total, (shift(total[0], step, 1), shift(total[1], step, 1)))
        step //= 2
    row = lax.broadcasted_iota(jnp.int32, (MARGIN, 128), 0)
    place = lax.broadcasted_iota(jnp.int32, (MARGIN, 128), 1)
    lined = []
    for part in total:
        merged = none
        for group in range(slots // MARGIN):
            merged = jnp.where(
                place // MARGIN == group, part[group * MARGIN : (group + 1) * MARGIN], merged
            )
        merged = jnp.where(place % MARGIN == row, merged, 0.0)
        for s in (4, 2, 1):
            merged = merged + shift(merged, s, 0)
        lined.append(merged)
    o_sums[...] = jnp.broadcast_to(jnp.where(row < 4, lined[0], lined[1])[None], o_sums.shape)
    for j in range(STEPS + 1):
        save(j).wait()
    for copy in results:
        copy.wait()


def edge_advance(spacing, heat, salt, u, v, damp, wet, low, high, inner, members):
    levels, width, extent = u.shape
    span = width + 2 * BASE
    slots = 32
    anywhere = pl.BlockSpec(memory_space=pl.ANY)
    tracer = jax.ShapeDtypeStruct(u.shape, jnp.bfloat16)
    f32 = jnp.float32
    return pl.pallas_call(
        edge_kernel,
        out_shape=[tracer] * 4
        + [
            jax.ShapeDtypeStruct((STEPS + 1, width, extent), f32),
            jax.ShapeDtypeStruct((members, MARGIN, 128), f32),
        ],
        in_specs=[pl.BlockSpec(memory_space=pltpu.SMEM)]
        + [anywhere] * 5
        + [pl.BlockSpec(memory_space=pltpu.VMEM)]
        + [anywhere] * 8,
        out_specs=[anywhere] * 5 + [pl.BlockSpec(memory_space=pltpu.VMEM)],
        scratch_shapes=[
            pltpu.VMEM((4, 2, levels, 2 * BASE, extent), f32),
            pltpu.VMEM((span, extent), f32),
            pltpu.VMEM((span, extent), f32),
            pltpu.VMEM((span, extent), f32),
            pltpu.VMEM((span, extent), f32),
            pltpu.VMEM((STEPS + 2, span, extent), f32),
            pltpu.VMEM((2, PAD, extent), f32),
            pltpu.VMEM((4, 2, levels, PAD, extent), jnp.bfloat16),
            pltpu.VMEM((2, slots * MARGIN, 128), f32),
            pltpu.SemaphoreType.DMA((24,)),
            pltpu.SemaphoreType.DMA((8,)),
            pltpu.SemaphoreType.DMA((STEPS + 1,)),
        ],
        input_output_aliases={11 + q: q for q in range(4)},
        cost_estimate=pl.CostEstimate(
            flops=10000000000, bytes_accessed=5000000, transcendentals=0
        ),
        name="edge_advance",
    )(spacing, heat, salt, u, v, damp, wet, low, high, inner[4], inner[5], *inner[:4])


def combine_kernel(sums, basis, height, resid, held, sems):
    copies = []
    for j in range(STEPS + 1):
        copy = pltpu.make_async_copy(basis.at[j], held.at[j], sems.at[j])
        copy.start()
        copies.append(copy)

    members = sums.shape[0]
    lane = lax.broadcasted_iota(jnp.int32, (MARGIN, 128), 1)
    row = lax.broadcasted_iota(jnp.int32, (MARGIN, 128), 0)
    pieces = [(sums[i], jnp.zeros((MARGIN, 128), jnp.float32)) for i in range(members)]
    while len(pieces) > 1:
        merged = []
        for x, y in zip(pieces[::2], pieces[1::2]):
            s, e = two_sum(x[0], y[0])
            merged.append((s, (x[1] + y[1]) + e))
        if len(pieces) % 2:
            merged.append(pieces[-1])
        pieces = merged
    total, error = pieces[0]
    other = shift(total, 4, 0)
    error_other = shift(error, 4, 0)
    upper = row < 4
    dots = fast_two_sum(
        jnp.where(upper, total, other),
        jnp.where(upper, other, total) + jnp.where(upper, error, error_other),
    )

    def at(x, k):
        return jnp.broadcast_to(x[:, k : k + 1], x.shape)

    odd = lane % 2 == 1
    anchor = tuple(jnp.where(odd, at(x, 1), at(x, 0)) for x in dots)
    moments = pair_add((2.0 * dots[0], 2.0 * dots[1]), (-anchor[0], -anchor[1]))
    inside = lane <= 2 * STEPS
    moments = tuple(jnp.where(inside, x, 0.0) for x in moments)

    def ahead(x):
        return shift(x, -1, 1)

    def behind(x):
        return shift(x, 1, 1)

    def image_of_products(x):
        after = tuple(ahead(c) for c in x)
        before = tuple(jnp.where(lane == 0, a, behind(c)) for a, c in zip(after, x))
        out = pair_add(pair_add(after, before), (2.0 * x[0], 2.0 * x[1]))
        return 0.25 * out[0], 0.25 * out[1]

    def image_of_coefficients(x):
        after = tuple(ahead(c) for c in x)
        before = tuple(
            jnp.where(lane == 0, 0.0, jnp.where(lane == 1, 2.0 * behind(c), behind(c))) for c in x
        )
        out = pair_add(pair_add(after, before), (2.0 * x[0], 2.0 * x[1]))
        return 0.25 * out[0], 0.25 * out[1]

    unit = jnp.where(lane == 0, 1.0, 0.0).astype(jnp.float32)
    zero = jnp.zeros_like(unit)
    r_products, p_products = moments, moments
    c_r, c_p, c_x = (unit, zero), (unit, zero), zero
    for k in range(STEPS):
        image = image_of_products(p_products)
        norm_now = at(r_products[0], k)
        alpha = norm_now / at(image[0], k)
        change = pair_scale(image, -alpha)
        r_products = pair_add(r_products, change)
        c_x = c_x + alpha * c_p[0]
        c_r = pair_add(c_r, pair_scale(image_of_coefficients(c_p), -alpha))
        if k + 1 < STEPS:
            lead = 0.5 if k == 0 else 0.25
            beta = (-lead * alpha) * at(r_products[0], k + 1) / norm_now
            p_products = pair_add(r_products, pair_scale(p_products, beta))
            c_p = pair_add(c_r, pair_scale(c_p, beta))

    width = height.shape[0]
    weights_x = [at(c_x, j)[0:1] for j in range(STEPS + 1)]
    weights_r = [at(c_r[0], j)[0:1] for j in range(STEPS + 1)]
    for copy in copies:
        copy.wait()
    for first in range(0, width, MARGIN):
        keep = slice(first, first + MARGIN)
        for left in range(0, height.shape[1], 128):
            cols = slice(left, left + 128)
            h = None
            for j in range(STEPS + 1):
                value = held[j, keep, cols]
                if h is None:
                    h, r = weights_x[0] * value, weights_r[0] * value
                else:
                    h, r = h + weights_x[j] * value, r + weights_r[j] * value
            height[keep, cols] = h
            resid[keep, cols] = r


def combine(sums, basis):
    plane = jax.ShapeDtypeStruct(basis.shape[1:], jnp.float32)
    return pl.pallas_call(
        combine_kernel,
        out_shape=[plane, plane],
        in_specs=[pl.BlockSpec(memory_space=pltpu.VMEM), pl.BlockSpec(memory_space=pl.ANY)],
        out_specs=[pl.BlockSpec(memory_space=pltpu.VMEM)] * 2,
        scratch_shapes=[
            pltpu.VMEM(basis.shape, jnp.float32),
            pltpu.SemaphoreType.DMA((STEPS + 1,)),
        ],
        name="combine",
    )(sums, basis)


def on_device(
    heat_anomaly,
    saltiness_anomaly,
    first_axis_flow,
    second_axis_flow,
    layer_spacing,
    diagonal_shift,
    water_tile_flags,
):
    members = lax.axis_size("blk")
    width, extent = diagonal_shift.shape
    fields = (heat_anomaly, saltiness_anomaly, first_axis_flow, second_axis_flow)
    wet = jnp.broadcast_to(
        jnp.repeat(
            water_tile_flags.astype(jnp.float32), extent // water_tile_flags.shape[1], axis=1
        ),
        (MARGIN, extent),
    )

    def message(first, edge):
        rows = slice(first, first + PAD)
        corner = jnp.concatenate(
            [
                heat_anomaly[:, edge],
                saltiness_anomaly[:, edge],
                wet,
            ],
            axis=0,
        )
        return jnp.concatenate(
            [
                first_axis_flow[:, rows],
                second_axis_flow[:, rows],
                diagonal_shift[rows][None],
                corner[None],
            ],
            axis=0,
        )

    forward = [(i, (i + 1) % members) for i in range(members)]
    backward = [(target, source) for source, target in forward]
    low = lax.ppermute(message(width - PAD, width - 1), "blk", forward)
    high = lax.ppermute(message(0, 0), "blk", backward)
    inner = inner_advance(layer_spacing, *fields, wet)
    *tracers, basis, sums = edge_advance(
        layer_spacing, *fields, diagonal_shift, wet, low, high, inner, members
    )
    gathered = lax.all_to_all(sums, "blk", 0, 0)
    height, resid = combine(gathered, basis)
    return (*tracers, height, resid)


def solution(mesh):
    columns = P("member", "blk", None)
    return jax.shard_map(
        on_device,
        mesh=mesh,
        in_specs=(columns, columns, columns, columns, P(), P("blk", None), P("blk", None)),
        out_specs=(
            columns,
            columns,
            columns,
            columns,
            P(("member", "blk"), None),
            P(("member", "blk"), None),
        ),
        check_vma=False,
    )
```

```python
import functools

import jax
import jax.numpy as jnp
from jax import lax
from jax.experimental import pallas as pl
from jax.experimental.pallas import tpu as pltpu
from jax.sharding import PartitionSpec as P

SSTEP = 4
CG_BLOCKS = 3
STEPS = SSTEP * CG_BLOCKS
COURANT = 0.2
PAD = 16
MARGIN = 8
BASE = PAD + MARGIN
KIB = 1024
VMEM_BYTES = 65472 * KIB
PACK_ROOM = 10740 * KIB
INNER_ROOM = 12660 * KIB
EDGE_ROOM = 45 * KIB * KIB


def shift(value, amount, axis):
    return pltpu.roll(value, amount % value.shape[axis], axis)


def two_sum(a, b):
    s = a + b
    t = s - a
    return s, (a - (s - t)) + (b - t)


def fast_two_sum(a, b):
    s = a + b
    return s, b - (s - a)


def split(a):
    c = 4097.0 * a
    hi = c - (c - a)
    return hi, a - hi


def two_prod(a, b):
    p = a * b
    ah, al = split(a)
    bh, bl = split(b)
    return p, ((ah * bh - p) + ah * bl + al * bh) + al * bl


def pair_add(a, b):
    s, e = two_sum(a[0], b[0])
    return fast_two_sum(s, e + (a[1] + b[1]))


def pair_scale(a, c):
    p, e = two_prod(a[0], c)
    return p, e + a[1] * c


def upwind(speed, behind, ahead):
    return jnp.where(speed > 0.0, speed * behind, speed * ahead)


def face_speeds(u, v, east_wet, north_wet):
    east = 0.5 * (u + shift(u, -1, 0))[:-MARGIN] * east_wet
    centre = v[MARGIN:-MARGIN]
    north = 0.5 * (centre + shift(centre, -1, 1)) * north_wet
    return east, north


def advect(q, east, north, wet):
    east_flux = upwind(east, q[:-MARGIN], shift(q, -1, 0)[:-MARGIN])
    centre = q[MARGIN:-MARGIN]
    north_flux = upwind(north, centre, shift(centre, -1, 1))
    spread = (east_flux - shift(east_flux, 1, 0))[MARGIN:] + (
        north_flux - shift(north_flux, 1, 1)
    )
    return wet * (centre - COURANT * spread)


def lanes(shape):
    return lax.broadcasted_iota(jnp.int32, shape, 1)


def rows_in(shape):
    return lax.broadcasted_iota(jnp.int32, shape, 0)


def north_of(x):
    return jnp.where(lanes(x.shape) == x.shape[1] - 1, 0.0, shift(x, -1, 1))


def south_of(x):
    return jnp.where(lanes(x.shape) == 0, 0.0, shift(x, 1, 1))


def north_wetness(wet):
    return wet * north_of(wet)


def divergence(wet, flow, cross):
    east_part = shift(flow, -1, 0) - shift(flow, 1, 0)
    return wet * (0.5 * (east_part + (north_of(cross) - south_of(cross))))


def spacing_total(spacing):
    total = spacing[0]
    for k in range(1, spacing.shape[0]):
        total = total + spacing[k]
    return total


def pack_kernel(
    flags, spacing, heat, salt, u, v, damp, o_low, o_high, o_table, o_damp, windows, tips, sems
):
    levels, width, extent = u.shape
    tiles = flags.shape[1]
    messages = (o_high, o_low)
    copies = []
    for end in range(2):
        rows = pl.ds(0 if end == 0 else width - BASE, BASE)
        into = pl.ds(MARGIN if end == 0 else 0, BASE)
        tip = pl.ds(0 if end == 0 else width - MARGIN, MARGIN)
        for src, dst in (
            (u.at[:, rows], windows.at[0, end, :, into]),
            (v.at[:, rows], windows.at[1, end, :, into]),
            (heat.at[:, tip], tips.at[0, end]),
            (salt.at[:, tip], tips.at[1, end]),
        ):
            copy = pltpu.make_async_copy(src, dst, sems.at[len(copies)])
            copy.start()
            copies.append(copy)
    copy = pltpu.make_async_copy(damp, o_damp, sems.at[len(copies)])
    copy.start()
    copies.append(copy)
    lane = lanes((MARGIN, extent))
    wet = jnp.zeros((MARGIN, extent), jnp.float32)
    for tile in range(tiles):
        inside = (lane >= tile * (extent // tiles)) & (lane < (tile + 1) * (extent // tiles))
        wet = jnp.where(inside, flags[0, tile].astype(jnp.float32), wet)
    o_table[0:MARGIN] = wet
    wet_row = wet[0:1]
    east_wet = wet_row * wet_row
    north_wet = north_wetness(wet)[0:1]
    total = spacing_total(spacing)
    row = rows_in((MARGIN, extent))
    weights = jnp.zeros((MARGIN, extent), jnp.float32)
    for k in range(levels):
        weights = jnp.where(row == k, spacing[k], weights)
    o_table[MARGIN:PAD] = weights / total
    for copy in copies:
        copy.wait()
    for end in range(2):
        message = messages[end]

        def level_step(k, sums, end=end):
            weight = o_table[pl.ds(MARGIN + k, 1)]
            qu = windows[0, end, k]
            qv = windows[1, end, k]
            east, north = face_speeds(qu, qv, east_wet, north_wet)
            au = advect(qu, east, north, wet_row)
            av = advect(qv, east, north, wet_row)
            return sums[0] + weight * au, sums[1] + weight * av

        zero = jnp.zeros((PAD, extent), jnp.float32)
        flow, cross = lax.fori_loop(0, levels, level_step, (zero, zero))
        message[0] = divergence(wet_row, flow, cross)
        first = 0 if end == 0 else width - PAD
        message[1] = o_damp[first : first + PAD]
        for q in range(2):
            merged = jnp.zeros((MARGIN, extent), jnp.float32)
            for k in range(levels):
                if end == 0:
                    piece = shift(windows[q, 0, k, MARGIN:PAD], 2 * k, 0)
                else:
                    piece = shift(windows[q, 1, k, PAD:BASE], 2 * k + 2 - MARGIN, 0)
                merged = jnp.where(row // 2 == k, piece, merged)
            message[2, q * MARGIN : (q + 1) * MARGIN] = merged
        merged = jnp.zeros((MARGIN, extent), jnp.float32)
        for q in range(2):
            for k in range(levels):
                place = q * levels + k
                piece = shift(tips[q, end, k], place if end == 0 else place + 1, 0)
                merged = jnp.where(row == place, piece, merged)
        message[3, 0:MARGIN] = merged
        if end == 0:
            flow_piece = shift(flow[:MARGIN], -1, 0)
            cross_piece = shift(cross[:MARGIN], 1, 0)
        else:
            flow_piece = shift(flow[MARGIN:], -5, 0)
            cross_piece = shift(cross[MARGIN:], -4, 0)
        message[3, MARGIN:PAD] = jnp.where(
            row < 2, flow_piece, jnp.where(row == 2, cross_piece, wet)
        )


def pack(flags, spacing, heat, salt, u, v, damp):
    levels, width, extent = u.shape
    message = jax.ShapeDtypeStruct((4, PAD, extent), jnp.float32)
    smem = pl.BlockSpec(memory_space=pltpu.SMEM)
    return pl.pallas_call(
        pack_kernel,
        out_shape=[
            message,
            message,
            jax.ShapeDtypeStruct((PAD, extent), jnp.float32),
            jax.ShapeDtypeStruct(damp.shape, jnp.float32),
        ],
        in_specs=[smem, smem] + [pl.BlockSpec(memory_space=pl.ANY)] * 5,
        out_specs=[pl.BlockSpec(memory_space=pltpu.VMEM)] * 4,
        scratch_shapes=[
            pltpu.VMEM((2, 2, levels, 2 * PAD, extent), jnp.float32),
            pltpu.VMEM((2, 2, levels, MARGIN, extent), jnp.float32),
            pltpu.SemaphoreType.DMA((9,)),
        ],
        compiler_params=pltpu.CompilerParams(vmem_limit_bytes=VMEM_BYTES - PACK_ROOM),
        name="pack",
    )(flags, spacing, heat, salt, u, v, damp)


def inner_kernel(
    heat, salt, u, v, table,
    o_heat, o_salt, o_u, o_v, r_heat, r_salt, r_u, r_v, o_edge, o_start,
    bands, staged, tu, tv, sems, out_sems,
):
    levels, width, extent = u.shape
    sources = (heat, salt, u, v)
    targets = (o_heat, o_salt, o_u, o_v)
    rims = (r_heat, r_salt, r_u, r_v)
    inside = width - 2 * PAD

    def load(q, k):
        return pltpu.make_async_copy(
            sources[q].at[k], bands.at[q, k, pl.ds(MARGIN, width)], sems.at[q, k]
        )

    def store(q, k):
        return pltpu.make_async_copy(
            staged.at[q, k, pl.ds(PAD, inside)],
            targets[q].at[k, pl.ds(PAD, inside)],
            out_sems.at[q, k],
        )

    for k in range(levels):
        for q in (2, 3, 0, 1):
            load(q, k).start()
    wet = table[0:1]
    north_wet = north_wetness(table[0:MARGIN])[0:1]
    east_wet = wet * wet
    tu[...] = jnp.zeros_like(tu)
    tv[...] = jnp.zeros_like(tv)

    def level_step(k, carry):
        weight = table[pl.ds(MARGIN + k, 1)]
        for q in (2, 3, 0, 1):
            load(q, k).wait()

        def strip(index, carry):
            local = pl.ds(pl.multiple_of(index * PAD, PAD), PAD)
            later = pl.ds(pl.multiple_of(index * PAD + MARGIN, MARGIN), PAD)
            rows = pl.ds(pl.multiple_of(index * PAD, MARGIN), 2 * PAD)
            qu = bands[2, k, rows]
            qv = bands[3, k, rows]
            east, north = face_speeds(qu, qv, east_wet, north_wet)
            au = advect(qu, east, north, wet)
            av = advect(qv, east, north, wet)
            staged[2, k, local] = au.astype(staged.dtype)
            staged[3, k, local] = av.astype(staged.dtype)
            tu[later] += weight * au
            tv[later] += weight * av
            staged[0, k, local] = advect(bands[0, k, rows], east, north, wet).astype(staged.dtype)
            staged[1, k, local] = advect(bands[1, k, rows], east, north, wet).astype(staged.dtype)
            return carry

        lax.fori_loop(0, width // PAD, strip, 0)
        for q in range(4):
            store(q, k).start()
            rims[q][0, k] = bands[q, k, MARGIN:BASE]
            rims[q][1, k] = bands[q, k, width - MARGIN : width + MARGIN]
            o_edge[q, 0, k] = staged[q, k, 0:PAD]
            o_edge[q, 1, k] = staged[q, k, width - PAD : width]
        return carry

    lax.fori_loop(0, levels, level_step, 0)
    for first in range(0, width, PAD):
        keep = slice(first, first + PAD)
        flow = tu[first : first + 2 * PAD]
        cross = tv[first + MARGIN : first + BASE]
        east_part = (shift(flow, -1, 0) - shift(flow, 1, 0))[MARGIN:BASE]
        o_start[keep] = wet * (0.5 * (east_part + (north_of(cross) - south_of(cross))))
    for k in range(levels):
        for q in range(4):
            store(q, k).wait()


def inner_advance(heat, salt, u, v, table):
    levels, width, extent = u.shape
    f32 = jnp.float32
    tracer = jax.ShapeDtypeStruct(u.shape, jnp.bfloat16)
    plane = jax.ShapeDtypeStruct((width, extent), f32)
    vmem = pl.BlockSpec(memory_space=pltpu.VMEM)
    anywhere = pl.BlockSpec(memory_space=pl.ANY)
    return pl.pallas_call(
        inner_kernel,
        out_shape=[tracer] * 4
        + [jax.ShapeDtypeStruct((2, levels, PAD, extent), f32)] * 4
        + [jax.ShapeDtypeStruct((4, 2, levels, PAD, extent), jnp.bfloat16), plane],
        in_specs=[anywhere] * 4 + [vmem],
        out_specs=[anywhere] * 4 + [vmem] * 6,
        scratch_shapes=[
            pltpu.VMEM((4, levels, width + PAD, extent), f32),
            pltpu.VMEM((4, levels, width, extent), jnp.bfloat16),
            pltpu.VMEM((width + PAD, extent), f32),
            pltpu.VMEM((width + PAD, extent), f32),
            pltpu.SemaphoreType.DMA((4, levels)),
            pltpu.SemaphoreType.DMA((4, levels)),
        ],
        cost_estimate=pl.CostEstimate(
            flops=10000000000, bytes_accessed=5000000, transcendentals=0
        ),
        compiler_params=pltpu.CompilerParams(vmem_limit_bytes=VMEM_BYTES - INNER_ROOM),
        name="inner_advance",
    )(heat, salt, u, v, table)


def edge_kernel(
    r_heat, r_salt, r_u, r_v, edge_in, start_in, damp, table, low, high, i_heat, i_salt, i_u, i_v,
    o_heat, o_salt, o_u, o_v, fields, o_sums,
    ocean, diag, edge_out, acc, out_sems,
):
    rims = (r_heat, r_salt, r_u, r_v)
    levels, extent = r_u.shape[1], r_u.shape[3]
    width = start_in.shape[0]
    span = width + 2 * BASE
    wet8 = table[0:MARGIN]
    row = rows_in((MARGIN, extent))
    for block in range(BASE // MARGIN, (BASE + width) // MARGIN):
        ocean[block * MARGIN : (block + 1) * MARGIN] = wet8
    diag[BASE : BASE + width] = (
        0.5 * (table[0:1] * (6.0 + damp[...]) + (1.0 - table[0:1])) - 2.0
    )
    fields[1, BASE : BASE + width] = start_in[...]

    for side, message in ((0, low), (1, high)):
        wet_out = jnp.broadcast_to(message[3, PAD - 1 : PAD], (MARGIN, extent))
        outer = 0 if side == 0 else BASE + width
        for block in range(BASE // MARGIN):
            ocean[outer + block * MARGIN : outer + (block + 1) * MARGIN] = wet_out
        halo = MARGIN if side == 0 else BASE + width
        wet_row = wet_out[0:1]
        diag[halo : halo + PAD] = 0.5 * (
            wet_row * (6.0 + message[1]) + (1.0 - wet_row)
        ) - 2.0
        if side == 0:
            around = jnp.concatenate([wet_out, wet8, wet8], axis=0)
            beyond = jnp.concatenate([wet_out, wet_out, wet8], axis=0)
        else:
            around = jnp.concatenate([wet8, wet8, wet_out], axis=0)
            beyond = jnp.concatenate([wet8, wet_out, wet_out], axis=0)
        east_own = (around * shift(around, -1, 0))[:PAD]
        east_out = (beyond * shift(beyond, -1, 0))[:PAD]
        north_own = north_wetness(wet8)
        north_out = north_wetness(wet_out)

        def level_step(k, sums, side=side, message=message, east_own=east_own,
                       east_out=east_out, north_own=north_own, north_out=north_out,
                       wet_out=wet_out):
            weight = table[pl.ds(MARGIN + k, 1)]
            own, out = [], []
            for q in (2, 3):
                pair = message[2, (q - 2) * MARGIN : (q - 1) * MARGIN]
                mine = rims[q][side, k]
                if side == 0:
                    piece = pltpu.roll(pair, MARGIN - 2 - 2 * k, 0)
                    own.append(jnp.concatenate([piece, mine], axis=0))
                    out.append(jnp.concatenate([piece, piece, mine[:MARGIN]], axis=0))
                else:
                    piece = pltpu.roll(pair, (MARGIN - 2 * k) % MARGIN, 0)
                    own.append(jnp.concatenate([mine, piece], axis=0))
                    out.append(jnp.concatenate([mine[MARGIN:], piece, piece], axis=0))
            east, north = face_speeds(own[0], own[1], east_own, north_own)
            au = advect(own[0], east, north, wet8)
            av = advect(own[1], east, north, wet8)
            fresh = [None, None, au, av]
            for q in range(2):
                mine = rims[q][side, k]
                single = message[3, 0:MARGIN]
                place = q * levels + k
                if side == 0:
                    piece = pltpu.roll(single, (2 * MARGIN - 1 - place) % MARGIN, 0)
                    window = jnp.concatenate([piece, mine], axis=0)
                else:
                    piece = pltpu.roll(single, (MARGIN - place) % MARGIN, 0)
                    window = jnp.concatenate([mine, piece], axis=0)
                fresh[q] = advect(window, east, north, wet8)
            for q in range(4):
                old = edge_in[q, side, k].astype(jnp.float32)
                if side == 0:
                    value = jnp.concatenate([fresh[q], old[MARGIN:]], axis=0)
                else:
                    value = jnp.concatenate([old[:MARGIN], fresh[q]], axis=0)
                edge_out[q, side, k] = value.astype(edge_out.dtype)
            east, north = face_speeds(out[0], out[1], east_out, north_out)
            bu = advect(out[0], east, north, wet_out)
            bv = advect(out[1], east, north, wet_out)
            return (
                sums[0] + weight * au,
                sums[1] + weight * av,
                sums[2] + weight * bu,
                sums[3] + weight * bv,
            )

        zero = jnp.zeros((MARGIN, extent), jnp.float32)
        flow, cross, flow_out, cross_out = lax.fori_loop(
            0, levels, level_step, (zero, zero, zero, zero)
        )
        known = message[3, MARGIN:PAD]
        given = message[0]
        if side == 0:
            flow_out = jnp.where(row == MARGIN - 1, flow_out, shift(known, 5, 0))
            cross_out = jnp.where(row == MARGIN - 1, cross_out, shift(known, 4, 0))
            whole = divergence(
                jnp.concatenate([wet_out, wet8], axis=0),
                jnp.concatenate([flow_out, flow], axis=0),
                jnp.concatenate([cross_out, cross], axis=0),
            )
            fields[1, MARGIN : 2 * MARGIN] = given[:MARGIN]
            fields[1, 2 * MARGIN : BASE] = jnp.where(
                row >= MARGIN - 2, whole[:MARGIN], given[MARGIN:]
            )
            fields[1, BASE : BASE + MARGIN] = jnp.where(
                row < 2, whole[MARGIN:], start_in[0:MARGIN]
            )
        else:
            flow_out = jnp.where(row == 0, flow_out, shift(known, 1, 0))
            cross_out = jnp.where(row == 0, cross_out, shift(known, -1, 0))
            whole = divergence(
                jnp.concatenate([wet8, wet_out], axis=0),
                jnp.concatenate([flow, flow_out], axis=0),
                jnp.concatenate([cross, cross_out], axis=0),
            )
            top = BASE + width
            fields[1, top - MARGIN : top] = jnp.where(
                row >= MARGIN - 2, whole[:MARGIN], start_in[width - MARGIN : width]
            )
            fields[1, top : top + MARGIN] = jnp.where(row < 2, whole[MARGIN:], given[:MARGIN])
            fields[1, top + MARGIN : top + PAD] = given[MARGIN:]

    results = []
    for q, target in enumerate((o_heat, o_salt, o_u, o_v)):
        for side in range(2):
            first = 0 if side == 0 else width - PAD
            copy = pltpu.make_async_copy(
                edge_out.at[q, side],
                target.at[:, pl.ds(first, PAD)],
                out_sems.at[2 * q + side],
            )
            copy.start()
            results.append(copy)

    strips = (width + 2 * PAD) // PAD
    none = jnp.zeros((MARGIN, 128), jnp.float32)

    def inner(a, b, total):
        product = a * b
        part = product[:MARGIN] + product[MARGIN:]
        pieces = [part[:, i : i + 128] for i in range(0, extent, 128)]
        while len(pieces) > 1:
            pieces = [x + y for x, y in zip(pieces[::2], pieces[1::2])]
        s, e = two_sum(total[0], pieces[0])
        return s, total[1] + e

    square = (none, none)
    for strip in range(strips):
        keep = slice(MARGIN + strip * PAD, BASE + strip * PAD)
        fields[0, keep] = jnp.zeros((PAD, extent), jnp.float32)
        if 0 < strip < strips - 1:
            value = fields[1, keep]
            square = inner(value, value, square)
    acc[0, 0:MARGIN] = square[0]
    acc[1, 0:MARGIN] = square[1]
    for slot in range(2 * STEPS + 1, acc.shape[1] // MARGIN):
        acc[0, slot * MARGIN : (slot + 1) * MARGIN] = none
        acc[1, slot * MARGIN : (slot + 1) * MARGIN] = none

    def basis_step(j, carry):
        scale = jnp.where(j == 0, 0.5, 1.0)
        mixed, square = (none, none), (none, none)
        for strip in range(strips):
            start = MARGIN + strip * PAD
            around = slice(start - MARGIN, start + BASE)
            keep = slice(start, start + PAD)
            wide = fields[j + 1, around]
            masked = wide * ocean[around]
            sides = (shift(masked, -1, 0) + shift(masked, 1, 0))[MARGIN:BASE]
            column = masked[MARGIN:BASE] + 0.5 * sides
            near = sides + (north_of(column) + south_of(column))
            centre = wide[MARGIN:BASE]
            image = diag[keep] * centre - (0.5 * ocean[keep]) * near
            following = scale * image - fields[j, keep]
            fields[j + 2, keep] = following
            if 0 < strip < strips - 1:
                mixed = inner(centre, following, mixed)
                square = inner(following, following, square)
        for place, value in ((2 * j + 1, mixed), (2 * j + 2, square)):
            at = pl.ds(pl.multiple_of(place * MARGIN, MARGIN), MARGIN)
            acc[0, at] = value[0]
            acc[1, at] = value[1]
        return carry

    lax.fori_loop(0, STEPS, basis_step, 0)

    slots = acc.shape[1] // MARGIN
    pairs = [
        (acc[0, pl.ds(s, slots, stride=MARGIN)], acc[1, pl.ds(s, slots, stride=MARGIN)])
        for s in range(MARGIN)
    ]
    while len(pairs) > 1:
        pairs = [pair_add(x, y) for x, y in zip(pairs[::2], pairs[1::2])]
    total = pairs[0]
    step = 64
    while step:
        total = pair_add(total, (shift(total[0], step, 1), shift(total[1], step, 1)))
        step //= 2
    row = lax.broadcasted_iota(jnp.int32, (MARGIN, 128), 0)
    place = lax.broadcasted_iota(jnp.int32, (MARGIN, 128), 1)
    lined = []
    for part in total:
        merged = none
        for group in range(slots // MARGIN):
            merged = jnp.where(
                place // MARGIN == group, part[group * MARGIN : (group + 1) * MARGIN], merged
            )
        merged = jnp.where(place % MARGIN == row, merged, 0.0)
        for s in (4, 2, 1):
            merged = merged + shift(merged, s, 0)
        lined.append(merged)
    o_sums[...] = jnp.broadcast_to(jnp.where(row < 4, lined[0], lined[1])[None], o_sums.shape)
    for copy in results:
        copy.wait()


def edge_advance(damp, table, low, high, inner, members):
    *tracers, r_heat, r_salt, r_u, r_v, edge, start = inner
    levels, width, extent = tracers[0].shape
    span = width + 2 * BASE
    slots = 32
    anywhere = pl.BlockSpec(memory_space=pl.ANY)
    vmem = pl.BlockSpec(memory_space=pltpu.VMEM)
    tracer = jax.ShapeDtypeStruct(tracers[0].shape, jnp.bfloat16)
    f32 = jnp.float32
    return pl.pallas_call(
        edge_kernel,
        out_shape=[tracer] * 4
        + [
            jax.ShapeDtypeStruct((STEPS + 2, span, extent), f32),
            jax.ShapeDtypeStruct((members, MARGIN, 128), f32),
        ],
        in_specs=[vmem] * 10 + [anywhere] * 4,
        out_specs=[anywhere] * 4 + [vmem] * 2,
        scratch_shapes=[
            pltpu.VMEM((span, extent), f32),
            pltpu.VMEM((span, extent), f32),
            pltpu.VMEM((4, 2, levels, PAD, extent), jnp.bfloat16),
            pltpu.VMEM((2, slots * MARGIN, 128), f32),
            pltpu.SemaphoreType.DMA((8,)),
        ],
        input_output_aliases={10 + q: q for q in range(4)},
        cost_estimate=pl.CostEstimate(
            flops=10000000000, bytes_accessed=5000000, transcendentals=0
        ),
        compiler_params=pltpu.CompilerParams(vmem_limit_bytes=VMEM_BYTES - EDGE_ROOM),
        name="edge_advance",
    )(r_heat, r_salt, r_u, r_v, edge, start, damp, table, low, high, *tracers)


def combine_kernel(sums, fields, height, resid):
    members = sums.shape[0]
    lane = lax.broadcasted_iota(jnp.int32, (MARGIN, 128), 1)
    row = lax.broadcasted_iota(jnp.int32, (MARGIN, 128), 0)
    pieces = [(sums[i], jnp.zeros((MARGIN, 128), jnp.float32)) for i in range(members)]
    while len(pieces) > 1:
        merged = []
        for x, y in zip(pieces[::2], pieces[1::2]):
            s, e = two_sum(x[0], y[0])
            merged.append((s, (x[1] + y[1]) + e))
        if len(pieces) % 2:
            merged.append(pieces[-1])
        pieces = merged
    total, error = pieces[0]
    other = shift(total, 4, 0)
    error_other = shift(error, 4, 0)
    upper = row < 4
    dots = fast_two_sum(
        jnp.where(upper, total, other),
        jnp.where(upper, other, total) + jnp.where(upper, error, error_other),
    )

    def at(x, k):
        return jnp.broadcast_to(x[:, k : k + 1], x.shape)

    odd = lane % 2 == 1
    anchor = tuple(jnp.where(odd, at(x, 1), at(x, 0)) for x in dots)
    moments = pair_add((2.0 * dots[0], 2.0 * dots[1]), (-anchor[0], -anchor[1]))
    inside = lane <= 2 * STEPS
    moments = tuple(jnp.where(inside, x, 0.0) for x in moments)

    def ahead(x):
        return shift(x, -1, 1)

    def behind(x):
        return shift(x, 1, 1)

    def image_of_products(x):
        after = tuple(ahead(c) for c in x)
        before = tuple(jnp.where(lane == 0, a, behind(c)) for a, c in zip(after, x))
        out = pair_add(pair_add(after, before), (2.0 * x[0], 2.0 * x[1]))
        return 0.25 * out[0], 0.25 * out[1]

    def image_of_coefficients(x):
        after = tuple(ahead(c) for c in x)
        before = tuple(
            jnp.where(lane == 0, 0.0, jnp.where(lane == 1, 2.0 * behind(c), behind(c))) for c in x
        )
        out = pair_add(pair_add(after, before), (2.0 * x[0], 2.0 * x[1]))
        return 0.25 * out[0], 0.25 * out[1]

    unit = jnp.where(lane == 0, 1.0, 0.0).astype(jnp.float32)
    zero = jnp.zeros_like(unit)
    r_products, p_products = moments, moments
    c_r, c_p, c_x = (unit, zero), (unit, zero), zero
    for k in range(STEPS):
        image = image_of_products(p_products)
        norm_now = at(r_products[0], k)
        alpha = norm_now / at(image[0], k)
        change = pair_scale(image, -alpha)
        r_products = pair_add(r_products, change)
        c_x = c_x + alpha * c_p[0]
        c_r = pair_add(c_r, pair_scale(image_of_coefficients(c_p), -alpha))
        if k + 1 < STEPS:
            lead = 0.5 if k == 0 else 0.25
            beta = (-lead * alpha) * at(r_products[0], k + 1) / norm_now
            p_products = pair_add(r_products, pair_scale(p_products, beta))
            c_p = pair_add(c_r, pair_scale(c_p, beta))

    width = height.shape[0]
    weights_x = [at(c_x, j)[0:1] for j in range(STEPS + 1)]
    weights_r = [at(c_r[0], j)[0:1] for j in range(STEPS + 1)]
    for first in range(0, width, MARGIN):
        keep = slice(first, first + MARGIN)
        wide = slice(BASE + first, BASE + first + MARGIN)
        for left in range(0, height.shape[1], 128):
            cols = slice(left, left + 128)
            h = None
            for j in range(STEPS + 1):
                value = fields[j + 1, wide, cols]
                if h is None:
                    h, r = weights_x[0] * value, weights_r[0] * value
                else:
                    h, r = h + weights_x[j] * value, r + weights_r[j] * value
            height[keep, cols] = h
            resid[keep, cols] = r


def combine(sums, fields, width):
    plane = jax.ShapeDtypeStruct((width, fields.shape[2]), jnp.float32)
    vmem = pl.BlockSpec(memory_space=pltpu.VMEM)
    return pl.pallas_call(
        combine_kernel,
        out_shape=[plane, plane],
        in_specs=[vmem, vmem],
        out_specs=[vmem, vmem],
        compiler_params=pltpu.CompilerParams(vmem_limit_bytes=8 * 1024 * 1024),
        name="combine",
    )(sums, fields)


def on_device(
    heat_anomaly,
    saltiness_anomaly,
    first_axis_flow,
    second_axis_flow,
    layer_spacing,
    diagonal_shift,
    water_tile_flags,
):
    members = lax.axis_size("blk")
    fields = (heat_anomaly, saltiness_anomaly, first_axis_flow, second_axis_flow)
    to_next, to_last, table, damp = pack(water_tile_flags, layer_spacing, *fields, diagonal_shift)
    forward = [(i, (i + 1) % members) for i in range(members)]
    backward = [(target, source) for source, target in forward]
    low = lax.ppermute(to_next, "blk", forward)
    high = lax.ppermute(to_last, "blk", backward)
    inner = inner_advance(*fields, table)
    *tracers, basis, sums = edge_advance(damp, table, low, high, inner, members)
    gathered = lax.all_to_all(sums, "blk", 0, 0)
    height, resid = combine(gathered, basis, diagonal_shift.shape[0])
    return (*tracers, height, resid)


def solution(mesh):
    columns = P("member", "blk", None)
    return jax.shard_map(
        on_device,
        mesh=mesh,
        in_specs=(columns, columns, columns, columns, P(), P("blk", None), P("blk", None)),
        out_specs=(
            columns,
            columns,
            columns,
            columns,
            P(("member", "blk"), None),
            P(("member", "blk"), None),
        ),
        check_vma=False,
    )
```

```python
import functools

import jax
import jax.numpy as jnp
from jax import lax
from jax.experimental import pallas as pl
from jax.experimental.pallas import tpu as pltpu
from jax.sharding import PartitionSpec as P

SSTEP = 4
CG_BLOCKS = 3
STEPS = SSTEP * CG_BLOCKS
COURANT = 0.2
PAD = 16
MARGIN = 8
BASE = PAD + MARGIN
KIB = 1024
PARTS = 2
VMEM_BYTES = 65472 * KIB
FETCH_ROOM = 14480 * KIB
PACK_ROOM = 32000 * KIB
INNER_ROOM = 32000 * KIB
EDGE_ROOM = 45 * KIB * KIB


def shift(value, amount, axis):
    return pltpu.roll(value, amount % value.shape[axis], axis)


def two_sum(a, b):
    s = a + b
    t = s - a
    return s, (a - (s - t)) + (b - t)


def fast_two_sum(a, b):
    s = a + b
    return s, b - (s - a)


def split(a):
    c = 4097.0 * a
    hi = c - (c - a)
    return hi, a - hi


def two_prod(a, b):
    p = a * b
    ah, al = split(a)
    bh, bl = split(b)
    return p, ((ah * bh - p) + ah * bl + al * bh) + al * bl


def pair_add(a, b):
    s, e = two_sum(a[0], b[0])
    return fast_two_sum(s, e + (a[1] + b[1]))


def pair_scale(a, c):
    p, e = two_prod(a[0], c)
    return p, e + a[1] * c


def upwind(speed, behind, ahead):
    return speed * jnp.where(speed > 0.0, behind, ahead)


def face_speeds(u, v, east_wet, north_wet):
    east = 0.5 * (u + shift(u, -1, 0))[:-MARGIN] * east_wet
    centre = v[MARGIN:-MARGIN]
    north = 0.5 * (centre + shift(centre, -1, 1)) * north_wet
    return east, north


def advect(q, east, north, wet):
    east_flux = upwind(east, q[:-MARGIN], shift(q, -1, 0)[:-MARGIN])
    centre = q[MARGIN:-MARGIN]
    north_flux = upwind(north, centre, shift(centre, -1, 1))
    spread = (east_flux - shift(east_flux, 1, 0))[MARGIN:] + (
        north_flux - shift(north_flux, 1, 1)
    )
    return wet * (centre - COURANT * spread)


def lanes(shape):
    return lax.broadcasted_iota(jnp.int32, shape, 1)


def rows_in(shape):
    return lax.broadcasted_iota(jnp.int32, shape, 0)


def north_of(x):
    return jnp.where(lanes(x.shape) == x.shape[1] - 1, 0.0, shift(x, -1, 1))


def south_of(x):
    return jnp.where(lanes(x.shape) == 0, 0.0, shift(x, 1, 1))


def north_wetness(wet):
    return wet * north_of(wet)


def divergence(wet, flow, cross):
    east_part = shift(flow, -1, 0) - shift(flow, 1, 0)
    return wet * (0.5 * (east_part + (north_of(cross) - south_of(cross))))


class Band:
    def __init__(self, parts):
        self.parts = parts

    def __getitem__(self, at):
        return jnp.concatenate([part[at] for part in self.parts], axis=-1)


def bands_of(refs):
    return [Band(refs[q * PARTS : (q + 1) * PARTS]) for q in range(4)]


def fetch_kernel(heat, salt, u, v, *refs):
    width, extent = u.shape[1:]
    parts, sems = refs[: 4 * PARTS], refs[4 * PARTS]
    share = extent // PARTS
    copies = []
    for q, source in enumerate((heat, salt, u, v)):
        for part in range(PARTS):
            copy = pltpu.make_async_copy(
                source.at[:, :, pl.ds(part * share, share)],
                parts[q * PARTS + part].at[:, pl.ds(MARGIN, width)],
                sems.at[len(copies)],
            )
            copy.start()
            copies.append(copy)
    for copy in copies:
        copy.wait()


def fetch(heat, salt, u, v):
    levels, width, extent = u.shape
    band = jax.ShapeDtypeStruct((levels, width + PAD, extent // PARTS), u.dtype)
    return pl.pallas_call(
        fetch_kernel,
        out_shape=[band] * (4 * PARTS),
        in_specs=[pl.BlockSpec(memory_space=pl.ANY)] * 4,
        out_specs=[pl.BlockSpec(memory_space=pltpu.VMEM)] * (4 * PARTS),
        scratch_shapes=[pltpu.SemaphoreType.DMA((4 * PARTS,))],
        cost_estimate=pl.CostEstimate(
            flops=10000000000, bytes_accessed=5000000, transcendentals=0
        ),
        compiler_params=pltpu.CompilerParams(vmem_limit_bytes=VMEM_BYTES - FETCH_ROOM),
        name="fetch",
    )(heat, salt, u, v)


def pack_kernel(flags, spacing, damp, *refs):
    heat, salt, u, v = bands_of(refs)
    o_low, o_high, o_table = refs[4 * PARTS :]
    levels = spacing.shape[1]
    width, extent = damp.shape
    tiles = flags.shape[1]
    flows, tracers = (u, v), (heat, salt)
    messages = (o_high, o_low)
    lane = lanes((MARGIN, extent))
    wet = jnp.zeros((MARGIN, extent), jnp.float32)
    flag = flags[...].astype(jnp.float32)
    for tile in range(tiles):
        inside = (lane >= tile * (extent // tiles)) & (lane < (tile + 1) * (extent // tiles))
        wet = jnp.where(inside, flag[:, tile : tile + 1], wet)
    o_table[0:MARGIN] = wet
    wet_row = wet[0:1]
    east_wet = wet_row * wet_row
    north_wet = north_wetness(wet)[0:1]
    row = rows_in((MARGIN, extent))
    thick = [spacing[:, k : k + 1] for k in range(levels)]
    total = thick[0]
    for k in range(1, levels):
        total = total + thick[k]
    weights = jnp.zeros((MARGIN, extent), jnp.float32)
    for k in range(levels):
        weights = jnp.where(row == k, thick[k], weights)
    o_table[MARGIN:PAD] = weights / total
    for end in range(2):
        message = messages[end]
        rows = slice(0, 2 * PAD) if end == 0 else slice(width - PAD, width + PAD)

        def level_step(k, sums, rows=rows):
            weight = o_table[pl.ds(MARGIN + k, 1)]
            qu = u[k, rows]
            qv = v[k, rows]
            east, north = face_speeds(qu, qv, east_wet, north_wet)
            au = advect(qu, east, north, wet_row)
            av = advect(qv, east, north, wet_row)
            return sums[0] + weight * au, sums[1] + weight * av

        zero = jnp.zeros((PAD, extent), jnp.float32)
        flow, cross = lax.fori_loop(0, levels, level_step, (zero, zero))
        message[0] = divergence(wet_row, flow, cross)
        first = 0 if end == 0 else width - PAD
        message[1] = damp[first : first + PAD]
        tip = slice(MARGIN, PAD) if end == 0 else slice(width, width + MARGIN)
        for q in range(2):
            merged = jnp.zeros((MARGIN, extent), jnp.float32)
            for k in range(levels):
                offset = 2 * k if end == 0 else 2 * k + 2 - MARGIN
                merged = jnp.where(row // 2 == k, shift(flows[q][k, tip], offset, 0), merged)
            message[2, q * MARGIN : (q + 1) * MARGIN] = merged
        merged = jnp.zeros((MARGIN, extent), jnp.float32)
        for q in range(2):
            for k in range(levels):
                place = q * levels + k
                piece = shift(tracers[q][k, tip], place if end == 0 else place + 1, 0)
                merged = jnp.where(row == place, piece, merged)
        message[3, 0:MARGIN] = merged
        if end == 0:
            flow_piece = shift(flow[:MARGIN], -1, 0)
            cross_piece = shift(cross[:MARGIN], 1, 0)
        else:
            flow_piece = shift(flow[MARGIN:], -5, 0)
            cross_piece = shift(cross[MARGIN:], -4, 0)
        message[3, MARGIN:PAD] = jnp.where(
            row < 2, flow_piece, jnp.where(row == 2, cross_piece, wet)
        )


def pack(flags, spacing, damp, bands):
    extent = damp.shape[1]
    f32 = jnp.float32
    message = jax.ShapeDtypeStruct((4, PAD, extent), f32)
    vmem = pl.BlockSpec(memory_space=pltpu.VMEM)
    return pl.pallas_call(
        pack_kernel,
        out_shape=[message, message, jax.ShapeDtypeStruct((PAD, extent), f32)],
        in_specs=[vmem] * (3 + len(bands)),
        out_specs=[vmem] * 3,
        compiler_params=pltpu.CompilerParams(vmem_limit_bytes=VMEM_BYTES - PACK_ROOM),
        name="pack",
    )(flags, spacing, damp, *bands)


def inner_kernel(table, *refs):
    heat, salt, u, v = bands_of(refs)
    staged, o_start, tu, tv = refs[4 * PARTS :]
    levels = staged.shape[1]
    width, extent = o_start.shape
    wet = table[0:1]
    north_wet = north_wetness(table[0:MARGIN])[0:1]
    east_wet = wet * wet
    tu[...] = jnp.zeros_like(tu)
    tv[...] = jnp.zeros_like(tv)

    def level_step(k, carry):
        weight = table[pl.ds(MARGIN + k, 1)]

        def strip(index, carry):
            local = pl.ds(pl.multiple_of(index * PAD, PAD), PAD)
            later = pl.ds(pl.multiple_of(index * PAD + MARGIN, MARGIN), PAD)
            rows = pl.ds(pl.multiple_of(index * PAD, MARGIN), 2 * PAD)
            qu = u[k, rows]
            qv = v[k, rows]
            east, north = face_speeds(qu, qv, east_wet, north_wet)
            au = advect(qu, east, north, wet)
            av = advect(qv, east, north, wet)
            staged[2, k, local] = au.astype(staged.dtype)
            staged[3, k, local] = av.astype(staged.dtype)
            tu[later] += weight * au
            tv[later] += weight * av
            staged[0, k, local] = advect(heat[k, rows], east, north, wet).astype(staged.dtype)
            staged[1, k, local] = advect(salt[k, rows], east, north, wet).astype(staged.dtype)
            return carry

        lax.fori_loop(0, width // PAD, strip, 0)
        return carry

    lax.fori_loop(0, levels, level_step, 0)
    for first in range(0, width, PAD):
        keep = slice(first, first + PAD)
        flow = tu[first : first + 2 * PAD]
        cross = tv[first + MARGIN : first + BASE]
        east_part = (shift(flow, -1, 0) - shift(flow, 1, 0))[MARGIN:BASE]
        o_start[keep] = wet * (0.5 * (east_part + (north_of(cross) - south_of(cross))))


def inner_advance(table, bands):
    levels, padded, share = bands[0].shape
    width, extent = padded - PAD, share * PARTS
    f32 = jnp.float32
    vmem = pl.BlockSpec(memory_space=pltpu.VMEM)
    return pl.pallas_call(
        inner_kernel,
        out_shape=[
            jax.ShapeDtypeStruct((4, levels, width, extent), jnp.bfloat16),
            jax.ShapeDtypeStruct((width, extent), f32),
        ],
        in_specs=[vmem] * (1 + len(bands)),
        out_specs=[vmem] * 2,
        scratch_shapes=[
            pltpu.VMEM((width + PAD, extent), f32),
            pltpu.VMEM((width + PAD, extent), f32),
        ],
        cost_estimate=pl.CostEstimate(
            flops=10000000000, bytes_accessed=5000000, transcendentals=0
        ),
        compiler_params=pltpu.CompilerParams(vmem_limit_bytes=VMEM_BYTES - INNER_ROOM),
        name="inner_advance",
    )(table, *bands)


def edge_kernel(staged, start_in, damp, table, low, high, *refs):
    heat, salt, u, v = bands_of(refs)
    refs = refs[4 * PARTS :]
    levels = staged.shape[1]
    width, extent = start_in.shape
    span = width + 2 * BASE
    flows, tracers = (u, v), (heat, salt)
    o_heat, o_salt, o_u, o_v, fields, o_sums = refs[:6]
    ocean, diag, even, odd, edge_out, acc, out_sems = refs[6:]
    masked = (even, odd)
    targets = (o_heat, o_salt, o_u, o_v)
    inside = pl.ds(PAD, width - 2 * PAD)
    results = []
    for q in range(4):
        copy = pltpu.make_async_copy(
            staged.at[q, :, inside], targets[q].at[:, inside], out_sems.at[8 + q]
        )
        copy.start()
        results.append(copy)
    wet8 = table[0:MARGIN]
    row = rows_in((MARGIN, extent))
    for block in range(BASE // MARGIN, (BASE + width) // MARGIN):
        ocean[block * MARGIN : (block + 1) * MARGIN] = wet8
    diag[BASE : BASE + width] = (
        0.5 * (table[0:1] * (6.0 + damp[...]) + (1.0 - table[0:1])) - 2.0
    )
    fields[1, BASE : BASE + width] = start_in[...]

    for side, message in ((0, low), (1, high)):
        wet_out = jnp.broadcast_to(message[3, PAD - 1 : PAD], (MARGIN, extent))
        outer = 0 if side == 0 else BASE + width
        for block in range(BASE // MARGIN):
            ocean[outer + block * MARGIN : outer + (block + 1) * MARGIN] = wet_out
        halo = MARGIN if side == 0 else BASE + width
        wet_row = wet_out[0:1]
        diag[halo : halo + PAD] = 0.5 * (
            wet_row * (6.0 + message[1]) + (1.0 - wet_row)
        ) - 2.0
        if side == 0:
            around = jnp.concatenate([wet_out, wet8, wet8], axis=0)
            beyond = jnp.concatenate([wet_out, wet_out, wet8], axis=0)
        else:
            around = jnp.concatenate([wet8, wet8, wet_out], axis=0)
            beyond = jnp.concatenate([wet8, wet_out, wet_out], axis=0)
        east_own = (around * shift(around, -1, 0))[:PAD]
        east_out = (beyond * shift(beyond, -1, 0))[:PAD]
        north_own = north_wetness(wet8)
        north_out = north_wetness(wet_out)

        mine_at = slice(MARGIN, BASE) if side == 0 else slice(width - MARGIN, width + MARGIN)
        rim_at = slice(0, PAD) if side == 0 else slice(width - PAD, width)

        def level_step(k, sums, side=side, message=message, east_own=east_own,
                       east_out=east_out, north_own=north_own, north_out=north_out,
                       wet_out=wet_out, mine_at=mine_at, rim_at=rim_at):
            weight = table[pl.ds(MARGIN + k, 1)]
            own, out = [], []
            for q in (2, 3):
                pair = message[2, (q - 2) * MARGIN : (q - 1) * MARGIN]
                mine = flows[q - 2][k, mine_at]
                if side == 0:
                    piece = pltpu.roll(pair, (2 * MARGIN - 2 - 2 * k) % MARGIN, 0)
                    own.append(jnp.concatenate([piece, mine], axis=0))
                    out.append(jnp.concatenate([piece, piece, mine[:MARGIN]], axis=0))
                else:
                    piece = pltpu.roll(pair, (MARGIN - 2 * k) % MARGIN, 0)
                    own.append(jnp.concatenate([mine, piece], axis=0))
                    out.append(jnp.concatenate([mine[MARGIN:], piece, piece], axis=0))
            east, north = face_speeds(own[0], own[1], east_own, north_own)
            au = advect(own[0], east, north, wet8)
            av = advect(own[1], east, north, wet8)
            fresh = [None, None, au, av]
            for q in range(2):
                mine = tracers[q][k, mine_at]
                single = message[3, 0:MARGIN]
                place = q * levels + k
                if side == 0:
                    piece = pltpu.roll(single, (2 * MARGIN - 1 - place) % MARGIN, 0)
                    window = jnp.concatenate([piece, mine], axis=0)
                else:
                    piece = pltpu.roll(single, (MARGIN - place) % MARGIN, 0)
                    window = jnp.concatenate([mine, piece], axis=0)
                fresh[q] = advect(window, east, north, wet8)
            for q in range(4):
                old = staged[q, k, rim_at].astype(jnp.float32)
                if side == 0:
                    value = jnp.concatenate([fresh[q], old[MARGIN:]], axis=0)
                else:
                    value = jnp.concatenate([old[:MARGIN], fresh[q]], axis=0)
                edge_out[q, side, k] = value.astype(edge_out.dtype)
            east, north = face_speeds(out[0], out[1], east_out, north_out)
            bu = advect(out[0], east, north, wet_out)
            bv = advect(out[1], east, north, wet_out)
            return (
                sums[0] + weight * au,
                sums[1] + weight * av,
                sums[2] + weight * bu,
                sums[3] + weight * bv,
            )

        zero = jnp.zeros((MARGIN, extent), jnp.float32)
        flow, cross, flow_out, cross_out = lax.fori_loop(
            0, levels, level_step, (zero, zero, zero, zero)
        )
        known = message[3, MARGIN:PAD]
        given = message[0]
        if side == 0:
            flow_out = jnp.where(row == MARGIN - 1, flow_out, shift(known, 5, 0))
            cross_out = jnp.where(row == MARGIN - 1, cross_out, shift(known, 4, 0))
            whole = divergence(
                jnp.concatenate([wet_out, wet8], axis=0),
                jnp.concatenate([flow_out, flow], axis=0),
                jnp.concatenate([cross_out, cross], axis=0),
            )
            fields[1, MARGIN : 2 * MARGIN] = given[:MARGIN]
            fields[1, 2 * MARGIN : BASE] = jnp.where(
                row >= MARGIN - 2, whole[:MARGIN], given[MARGIN:]
            )
            fields[1, BASE : BASE + MARGIN] = jnp.where(
                row < 2, whole[MARGIN:], start_in[0:MARGIN]
            )
        else:
            flow_out = jnp.where(row == 0, flow_out, shift(known, 1, 0))
            cross_out = jnp.where(row == 0, cross_out, shift(known, -1, 0))
            whole = divergence(
                jnp.concatenate([wet8, wet_out], axis=0),
                jnp.concatenate([flow, flow_out], axis=0),
                jnp.concatenate([cross, cross_out], axis=0),
            )
            top = BASE + width
            fields[1, top - MARGIN : top] = jnp.where(
                row >= MARGIN - 2, whole[:MARGIN], start_in[width - MARGIN : width]
            )
            fields[1, top : top + MARGIN] = jnp.where(row < 2, whole[MARGIN:], given[:MARGIN])
            fields[1, top + MARGIN : top + PAD] = given[MARGIN:]

    for q, target in enumerate(targets):
        for side in range(2):
            first = 0 if side == 0 else width - PAD
            copy = pltpu.make_async_copy(
                edge_out.at[q, side],
                target.at[:, pl.ds(first, PAD)],
                out_sems.at[2 * q + side],
            )
            copy.start()
            results.append(copy)

    strips = (width + 2 * PAD) // PAD
    none = jnp.zeros((MARGIN, 128), jnp.float32)

    def inner(a, b, total):
        product = a * b
        part = product[:MARGIN] + product[MARGIN:]
        pieces = [part[:, i : i + 128] for i in range(0, extent, 128)]
        while len(pieces) > 1:
            pieces = [x + y for x, y in zip(pieces[::2], pieces[1::2])]
        s, e = two_sum(total[0], pieces[0])
        return s, total[1] + e

    square = (none, none)
    for strip in range(strips):
        keep = slice(MARGIN + strip * PAD, BASE + strip * PAD)
        masked[0][keep] = (0.5 * ocean[keep]) * fields[1, keep]
        fields[0, keep] = jnp.zeros((PAD, extent), jnp.float32)
        if 0 < strip < strips - 1:
            value = fields[1, keep]
            square = inner(value, value, square)
    acc[0, 0:MARGIN] = square[0]
    acc[1, 0:MARGIN] = square[1]
    for slot in range(2 * STEPS + 1, acc.shape[1] // MARGIN):
        acc[0, slot * MARGIN : (slot + 1) * MARGIN] = none
        acc[1, slot * MARGIN : (slot + 1) * MARGIN] = none

    def basis_step(j, now, scale):
        mixed, square = (none, none), (none, none)
        for strip in range(strips):
            start = MARGIN + strip * PAD
            around = slice(start - MARGIN, start + BASE)
            keep = slice(start, start + PAD)
            wide = masked[now][around]
            sides = (shift(wide, -1, 0) + shift(wide, 1, 0))[MARGIN:BASE]
            column = wide[MARGIN:BASE] + 0.5 * sides
            near = sides + (north_of(column) + south_of(column))
            centre = fields[j + 1, keep]
            wet = ocean[keep]
            following = diag[keep] * centre - wet * near
            if scale is not None:
                following = scale * following
            following = following - fields[j, keep]
            fields[j + 2, keep] = following
            masked[1 - now][keep] = (0.5 * wet) * following
            if 0 < strip < strips - 1:
                mixed = inner(centre, following, mixed)
                square = inner(following, following, square)
        for place, value in ((2 * j + 1, mixed), (2 * j + 2, square)):
            at = pl.ds(pl.multiple_of(place * MARGIN, MARGIN), MARGIN)
            acc[0, at] = value[0]
            acc[1, at] = value[1]

    def step_pair(index, carry):
        basis_step(2 * index, 0, jnp.where(index == 0, 0.5, 1.0))
        basis_step(2 * index + 1, 1, None)
        return carry

    lax.fori_loop(0, STEPS // 2, step_pair, 0)

    slots = acc.shape[1] // MARGIN
    pairs = [
        (acc[0, pl.ds(s, slots, stride=MARGIN)], acc[1, pl.ds(s, slots, stride=MARGIN)])
        for s in range(MARGIN)
    ]
    while len(pairs) > 1:
        pairs = [pair_add(x, y) for x, y in zip(pairs[::2], pairs[1::2])]
    total = pairs[0]
    step = 64
    while step:
        total = pair_add(total, (shift(total[0], step, 1), shift(total[1], step, 1)))
        step //= 2
    row = lax.broadcasted_iota(jnp.int32, (MARGIN, 128), 0)
    place = lax.broadcasted_iota(jnp.int32, (MARGIN, 128), 1)
    lined = []
    for part in total:
        merged = none
        for group in range(slots // MARGIN):
            merged = jnp.where(
                place // MARGIN == group, part[group * MARGIN : (group + 1) * MARGIN], merged
            )
        merged = jnp.where(place % MARGIN == row, merged, 0.0)
        for s in (4, 2, 1):
            merged = merged + shift(merged, s, 0)
        lined.append(merged)
    o_sums[...] = jnp.broadcast_to(jnp.where(row < 4, lined[0], lined[1])[None], o_sums.shape)
    for copy in results:
        copy.wait()


def edge_advance(staged, start, damp, table, low, high, bands, members):
    levels, width, extent = staged.shape[1:]
    span = width + 2 * BASE
    slots = 32
    anywhere = pl.BlockSpec(memory_space=pl.ANY)
    vmem = pl.BlockSpec(memory_space=pltpu.VMEM)
    tracer = jax.ShapeDtypeStruct((levels, width, extent), staged.dtype)
    f32 = jnp.float32
    return pl.pallas_call(
        edge_kernel,
        out_shape=[tracer] * 4
        + [
            jax.ShapeDtypeStruct((STEPS + 2, span, extent), f32),
            jax.ShapeDtypeStruct((members, MARGIN, 128), f32),
        ],
        in_specs=[vmem] * (6 + len(bands)),
        out_specs=[anywhere] * 4 + [vmem] * 2,
        scratch_shapes=[
            pltpu.VMEM((span, extent), f32),
            pltpu.VMEM((span, extent), f32),
            pltpu.VMEM((span, extent), f32),
            pltpu.VMEM((span, extent), f32),
            pltpu.VMEM((4, 2, levels, PAD, extent), jnp.bfloat16),
            pltpu.VMEM((2, slots * MARGIN, 128), f32),
            pltpu.SemaphoreType.DMA((12,)),
        ],
        cost_estimate=pl.CostEstimate(
            flops=10000000000, bytes_accessed=5000000, transcendentals=0
        ),
        compiler_params=pltpu.CompilerParams(vmem_limit_bytes=VMEM_BYTES - EDGE_ROOM),
        name="edge_advance",
    )(staged, start, damp, table, low, high, *bands)


def combine_kernel(sums, fields, height, resid):
    members = sums.shape[0]
    lane = lax.broadcasted_iota(jnp.int32, (MARGIN, 128), 1)
    row = lax.broadcasted_iota(jnp.int32, (MARGIN, 128), 0)
    pieces = [(sums[i], jnp.zeros((MARGIN, 128), jnp.float32)) for i in range(members)]
    while len(pieces) > 1:
        merged = []
        for x, y in zip(pieces[::2], pieces[1::2]):
            s, e = two_sum(x[0], y[0])
            merged.append((s, (x[1] + y[1]) + e))
        if len(pieces) % 2:
            merged.append(pieces[-1])
        pieces = merged
    total, error = pieces[0]
    other = shift(total, 4, 0)
    error_other = shift(error, 4, 0)
    upper = row < 4
    dots = fast_two_sum(
        jnp.where(upper, total, other),
        jnp.where(upper, other, total) + jnp.where(upper, error, error_other),
    )

    def at(x, k):
        return jnp.broadcast_to(x[:, k : k + 1], x.shape)

    odd = lane % 2 == 1
    anchor = tuple(jnp.where(odd, at(x, 1), at(x, 0)) for x in dots)
    moments = pair_add((2.0 * dots[0], 2.0 * dots[1]), (-anchor[0], -anchor[1]))
    inside = lane <= 2 * STEPS
    moments = tuple(jnp.where(inside, x, 0.0) for x in moments)

    def ahead(x):
        return shift(x, -1, 1)

    def behind(x):
        return shift(x, 1, 1)

    def image_of_products(x):
        after = tuple(ahead(c) for c in x)
        before = tuple(jnp.where(lane == 0, a, behind(c)) for a, c in zip(after, x))
        out = pair_add(pair_add(after, before), (2.0 * x[0], 2.0 * x[1]))
        return 0.25 * out[0], 0.25 * out[1]

    def image_of_coefficients(x):
        after = tuple(ahead(c) for c in x)
        before = tuple(
            jnp.where(lane == 0, 0.0, jnp.where(lane == 1, 2.0 * behind(c), behind(c))) for c in x
        )
        out = pair_add(pair_add(after, before), (2.0 * x[0], 2.0 * x[1]))
        return 0.25 * out[0], 0.25 * out[1]

    unit = jnp.where(lane == 0, 1.0, 0.0).astype(jnp.float32)
    zero = jnp.zeros_like(unit)
    r_products, p_products = moments, moments
    c_r, c_p, c_x = (unit, zero), (unit, zero), zero

    def pick(x, k):
        return at(x[0], k), at(x[1], k)

    def quarter_sum(before, here, after):
        out = pair_add(pair_add(after, before), (2.0 * here[0], 2.0 * here[1]))
        return 0.25 * out[0], 0.25 * out[1]

    norm = pick(r_products, 0)
    for k in range(STEPS):
        near = [pick(p_products, abs(k - 1)), pick(p_products, k)]
        near += [pick(p_products, k + 1), pick(p_products, k + 2)]
        energy = quarter_sum(near[0], near[1], near[2])
        alpha = norm[0] / energy[0]
        c_x = c_x + alpha * c_p[0]
        c_r = pair_add(c_r, pair_scale(image_of_coefficients(c_p), -alpha))
        if k + 1 < STEPS:
            change = pair_scale(image_of_products(p_products), -alpha)
            following = pair_scale(quarter_sum(near[1], near[2], near[3]), -alpha)
            following = pair_add(pick(r_products, k + 1), following)
            r_products = pair_add(r_products, change)
            lead = 0.5 if k == 0 else 0.25
            beta = (-lead * alpha) * following[0] / norm[0]
            p_products = pair_add(r_products, pair_scale(p_products, beta))
            c_p = pair_add(c_r, pair_scale(c_p, beta))
            norm = following

    width = height.shape[0]
    weights_x = [at(c_x, j)[0:1] for j in range(STEPS + 1)]
    weights_r = [at(c_r[0], j)[0:1] for j in range(STEPS + 1)]
    for first in range(0, width, MARGIN):
        keep = slice(first, first + MARGIN)
        wide = slice(BASE + first, BASE + first + MARGIN)
        for left in range(0, height.shape[1], 128):
            cols = slice(left, left + 128)
            value = fields[1, wide, cols]
            h, r = weights_x[0] * value, weights_r[0] * value
            for j in range(1, STEPS + 1):
                value = fields[j + 1, wide, cols]
                h, r = h + weights_x[j] * value, r + weights_r[j] * value
            height[keep, cols] = h
            resid[keep, cols] = r


def combine(sums, fields, width):
    plane = jax.ShapeDtypeStruct((width, fields.shape[2]), jnp.float32)
    vmem = pl.BlockSpec(memory_space=pltpu.VMEM)
    return pl.pallas_call(
        combine_kernel,
        out_shape=[plane, plane],
        in_specs=[vmem, vmem],
        out_specs=[vmem, vmem],
        compiler_params=pltpu.CompilerParams(vmem_limit_bytes=8 * 1024 * 1024),
        name="combine",
    )(sums, fields)


def on_device(
    heat_anomaly,
    saltiness_anomaly,
    first_axis_flow,
    second_axis_flow,
    layer_spacing,
    diagonal_shift,
    water_tile_flags,
):
    members = lax.axis_size("blk")
    bands = fetch(heat_anomaly, saltiness_anomaly, first_axis_flow, second_axis_flow)
    to_next, to_last, table = pack(water_tile_flags, layer_spacing[None], diagonal_shift, bands)
    forward = [(i, (i + 1) % members) for i in range(members)]
    backward = [(target, source) for source, target in forward]
    low = lax.ppermute(to_next, "blk", forward)
    high = lax.ppermute(to_last, "blk", backward)
    staged, start = inner_advance(table, bands)
    *tracers, basis, sums = edge_advance(
        staged, start, diagonal_shift, table, low, high, bands, members
    )
    gathered = lax.all_to_all(sums, "blk", 0, 0)
    height, resid = combine(gathered, basis, diagonal_shift.shape[0])
    return (*tracers, height, resid)


def solution(mesh):
    columns = P("member", "blk", None)
    return jax.shard_map(
        on_device,
        mesh=mesh,
        in_specs=(columns, columns, columns, columns, P(), P("blk", None), P("blk", None)),
        out_specs=(
            columns,
            columns,
            columns,
            columns,
            P(("member", "blk"), None),
            P(("member", "blk"), None),
        ),
        check_vma=False,
    )
```

```python
import functools

import jax
import jax.numpy as jnp
from jax import lax
from jax.experimental import pallas as pl
from jax.experimental.pallas import tpu as pltpu
from jax.sharding import PartitionSpec as P

SSTEP = 4
CG_BLOCKS = 3
STEPS = SSTEP * CG_BLOCKS
COURANT = 0.2
PAD = 16
MARGIN = 8
BASE = PAD + MARGIN
KIB = 1024
PARTS = 2
VMEM_BYTES = 65472 * KIB
FETCH_ROOM = 14480 * KIB
PACK_ROOM = 32000 * KIB
INNER_ROOM = 32000 * KIB
EDGE_ROOM = 45 * KIB * KIB


def shift(value, amount, axis):
    return pltpu.roll(value, amount % value.shape[axis], axis)


def two_sum(a, b):
    s = a + b
    t = s - a
    return s, (a - (s - t)) + (b - t)


def fast_two_sum(a, b):
    s = a + b
    return s, b - (s - a)


def split(a):
    c = 4097.0 * a
    hi = c - (c - a)
    return hi, a - hi


def two_prod(a, b):
    p = a * b
    ah, al = split(a)
    bh, bl = split(b)
    return p, ((ah * bh - p) + ah * bl + al * bh) + al * bl


def pair_add(a, b):
    s, e = two_sum(a[0], b[0])
    return fast_two_sum(s, e + (a[1] + b[1]))


def pair_scale(a, c):
    p, e = two_prod(a[0], c)
    return p, e + a[1] * c


def upwind(speed, behind, ahead):
    return speed * jnp.where(speed > 0.0, behind, ahead)


def face_speeds(u, v, east_wet, north_wet):
    east = 0.5 * (u + shift(u, -1, 0))[:-MARGIN] * east_wet
    centre = v[MARGIN:-MARGIN]
    north = 0.5 * (centre + shift(centre, -1, 1)) * north_wet
    return east, north


def advect(q, east, north, wet):
    east_flux = upwind(east, q[:-MARGIN], shift(q, -1, 0)[:-MARGIN])
    centre = q[MARGIN:-MARGIN]
    north_flux = upwind(north, centre, shift(centre, -1, 1))
    spread = (east_flux - shift(east_flux, 1, 0))[MARGIN:] + (
        north_flux - shift(north_flux, 1, 1)
    )
    return wet * (centre - COURANT * spread)


def lanes(shape):
    return lax.broadcasted_iota(jnp.int32, shape, 1)


def rows_in(shape):
    return lax.broadcasted_iota(jnp.int32, shape, 0)


def north_of(x):
    return jnp.where(lanes(x.shape) == x.shape[1] - 1, 0.0, shift(x, -1, 1))


def south_of(x):
    return jnp.where(lanes(x.shape) == 0, 0.0, shift(x, 1, 1))


def north_wetness(wet):
    return wet * north_of(wet)


def divergence(wet, flow, cross):
    east_part = shift(flow, -1, 0) - shift(flow, 1, 0)
    return wet * (0.5 * (east_part + (north_of(cross) - south_of(cross))))


class Band:
    def __init__(self, parts):
        self.parts = parts

    def __getitem__(self, at):
        return jnp.concatenate([part[at] for part in self.parts], axis=-1)


def bands_of(refs):
    return [Band(refs[q * PARTS : (q + 1) * PARTS]) for q in range(4)]


def fetch_kernel(heat, salt, u, v, *refs):
    width, extent = u.shape[1:]
    parts, sems = refs[: 4 * PARTS], refs[4 * PARTS]
    share = extent // PARTS
    copies = []
    for q, source in enumerate((heat, salt, u, v)):
        for part in range(PARTS):
            copy = pltpu.make_async_copy(
                source.at[:, :, pl.ds(part * share, share)],
                parts[q * PARTS + part].at[:, pl.ds(MARGIN, width)],
                sems.at[len(copies)],
            )
            copy.start()
            copies.append(copy)
    for copy in copies:
        copy.wait()


def fetch(heat, salt, u, v):
    levels, width, extent = u.shape
    band = jax.ShapeDtypeStruct((levels, width + PAD, extent // PARTS), u.dtype)
    return pl.pallas_call(
        fetch_kernel,
        out_shape=[band] * (4 * PARTS),
        in_specs=[pl.BlockSpec(memory_space=pl.ANY)] * 4,
        out_specs=[pl.BlockSpec(memory_space=pltpu.VMEM)] * (4 * PARTS),
        scratch_shapes=[pltpu.SemaphoreType.DMA((4 * PARTS,))],
        cost_estimate=pl.CostEstimate(
            flops=10000000000, bytes_accessed=5000000, transcendentals=0
        ),
        compiler_params=pltpu.CompilerParams(vmem_limit_bytes=VMEM_BYTES - FETCH_ROOM),
        name="fetch",
    )(heat, salt, u, v)


def pack_kernel(flags, spacing, damp, *refs):
    heat, salt, u, v = bands_of(refs)
    o_low, o_high, o_table = refs[4 * PARTS :]
    levels = spacing.shape[1]
    width, extent = damp.shape
    tiles = flags.shape[1]
    flows, tracers = (u, v), (heat, salt)
    messages = (o_high, o_low)
    lane = lanes((MARGIN, extent))
    wet = jnp.zeros((MARGIN, extent), jnp.float32)
    flag = flags[...].astype(jnp.float32)
    for tile in range(tiles):
        inside = (lane >= tile * (extent // tiles)) & (lane < (tile + 1) * (extent // tiles))
        wet = jnp.where(inside, flag[:, tile : tile + 1], wet)
    o_table[0:MARGIN] = wet
    wet_row = wet[0:1]
    east_wet = wet_row * wet_row
    north_wet = north_wetness(wet)[0:1]
    row = rows_in((MARGIN, extent))
    thick = [spacing[:, k : k + 1] for k in range(levels)]
    total = thick[0]
    for k in range(1, levels):
        total = total + thick[k]
    weights = jnp.zeros((MARGIN, extent), jnp.float32)
    for k in range(levels):
        weights = jnp.where(row == k, thick[k], weights)
    o_table[MARGIN:PAD] = weights / total
    for end in range(2):
        message = messages[end]
        rows = slice(0, 2 * PAD) if end == 0 else slice(width - PAD, width + PAD)

        def level_step(k, sums, rows=rows):
            weight = o_table[pl.ds(MARGIN + k, 1)]
            qu = u[k, rows]
            qv = v[k, rows]
            east, north = face_speeds(qu, qv, east_wet, north_wet)
            au = advect(qu, east, north, wet_row)
            av = advect(qv, east, north, wet_row)
            return sums[0] + weight * au, sums[1] + weight * av

        zero = jnp.zeros((PAD, extent), jnp.float32)
        flow, cross = lax.fori_loop(0, levels, level_step, (zero, zero), unroll=4)
        message[0] = divergence(wet_row, flow, cross)
        first = 0 if end == 0 else width - PAD
        message[1] = damp[first : first + PAD]
        tip = slice(MARGIN, PAD) if end == 0 else slice(width, width + MARGIN)
        for q in range(2):
            merged = jnp.zeros((MARGIN, extent), jnp.float32)
            for k in range(levels):
                offset = 2 * k if end == 0 else 2 * k + 2 - MARGIN
                merged = jnp.where(row // 2 == k, shift(flows[q][k, tip], offset, 0), merged)
            message[2, q * MARGIN : (q + 1) * MARGIN] = merged
        merged = jnp.zeros((MARGIN, extent), jnp.float32)
        for q in range(2):
            for k in range(levels):
                place = q * levels + k
                piece = shift(tracers[q][k, tip], place if end == 0 else place + 1, 0)
                merged = jnp.where(row == place, piece, merged)
        message[3, 0:MARGIN] = merged
        if end == 0:
            flow_piece = shift(flow[:MARGIN], -1, 0)
            cross_piece = shift(cross[:MARGIN], 1, 0)
        else:
            flow_piece = shift(flow[MARGIN:], -5, 0)
            cross_piece = shift(cross[MARGIN:], -4, 0)
        message[3, MARGIN:PAD] = jnp.where(
            row < 2, flow_piece, jnp.where(row == 2, cross_piece, wet)
        )


def pack(flags, spacing, damp, bands):
    extent = damp.shape[1]
    f32 = jnp.float32
    message = jax.ShapeDtypeStruct((4, PAD, extent), f32)
    vmem = pl.BlockSpec(memory_space=pltpu.VMEM)
    return pl.pallas_call(
        pack_kernel,
        out_shape=[message, message, jax.ShapeDtypeStruct((PAD, extent), f32)],
        in_specs=[vmem] * (3 + len(bands)),
        out_specs=[vmem] * 3,
        compiler_params=pltpu.CompilerParams(vmem_limit_bytes=VMEM_BYTES - PACK_ROOM),
        name="pack",
    )(flags, spacing, damp, *bands)


def inner_kernel(table, *refs):
    heat, salt, u, v = bands_of(refs)
    staged, o_start, tu, tv = refs[4 * PARTS :]
    levels = staged.shape[1]
    width, extent = o_start.shape
    wet = table[0:1]
    north_wet = north_wetness(table[0:MARGIN])[0:1]
    east_wet = wet * wet
    tu[...] = jnp.zeros_like(tu)
    tv[...] = jnp.zeros_like(tv)

    def level_step(k, carry):
        weight = table[pl.ds(MARGIN + k, 1)]

        def strip(index, carry):
            local = pl.ds(pl.multiple_of(index * PAD, PAD), PAD)
            later = pl.ds(pl.multiple_of(index * PAD + MARGIN, MARGIN), PAD)
            rows = pl.ds(pl.multiple_of(index * PAD, MARGIN), 2 * PAD)
            qu = u[k, rows]
            qv = v[k, rows]
            east, north = face_speeds(qu, qv, east_wet, north_wet)
            au = advect(qu, east, north, wet)
            av = advect(qv, east, north, wet)
            staged[2, k, local] = au.astype(staged.dtype)
            staged[3, k, local] = av.astype(staged.dtype)
            tu[later] += weight * au
            tv[later] += weight * av
            staged[0, k, local] = advect(heat[k, rows], east, north, wet).astype(staged.dtype)
            staged[1, k, local] = advect(salt[k, rows], east, north, wet).astype(staged.dtype)
            return carry

        lax.fori_loop(0, width // PAD, strip, 0, unroll=2)
        return carry

    lax.fori_loop(0, levels, level_step, 0)
    for first in range(0, width, PAD):
        keep = slice(first, first + PAD)
        flow = tu[first : first + 2 * PAD]
        cross = tv[first + MARGIN : first + BASE]
        east_part = (shift(flow, -1, 0) - shift(flow, 1, 0))[MARGIN:BASE]
        o_start[keep] = wet * (0.5 * (east_part + (north_of(cross) - south_of(cross))))


def inner_advance(table, bands):
    levels, padded, share = bands[0].shape
    width, extent = padded - PAD, share * PARTS
    f32 = jnp.float32
    vmem = pl.BlockSpec(memory_space=pltpu.VMEM)
    return pl.pallas_call(
        inner_kernel,
        out_shape=[
            jax.ShapeDtypeStruct((4, levels, width, extent), jnp.bfloat16),
            jax.ShapeDtypeStruct((width, extent), f32),
        ],
        in_specs=[vmem] * (1 + len(bands)),
        out_specs=[vmem] * 2,
        scratch_shapes=[
            pltpu.VMEM((width + PAD, extent), f32),
            pltpu.VMEM((width + PAD, extent), f32),
        ],
        cost_estimate=pl.CostEstimate(
            flops=10000000000, bytes_accessed=5000000, transcendentals=0
        ),
        compiler_params=pltpu.CompilerParams(vmem_limit_bytes=VMEM_BYTES - INNER_ROOM),
        name="inner_advance",
    )(table, *bands)


def edge_kernel(staged, start_in, damp, table, low, high, *refs):
    heat, salt, u, v = bands_of(refs)
    refs = refs[4 * PARTS :]
    levels = staged.shape[1]
    width, extent = start_in.shape
    span = width + 2 * BASE
    flows, tracers = (u, v), (heat, salt)
    o_heat, o_salt, o_u, o_v, fields, o_sums = refs[:6]
    ocean, half, diag, even, odd, edge_out, acc, out_sems = refs[6:]
    masked = (even, odd)
    targets = (o_heat, o_salt, o_u, o_v)
    inside = pl.ds(PAD, width - 2 * PAD)
    results = []
    for q in range(4):
        copy = pltpu.make_async_copy(
            staged.at[q, :, inside], targets[q].at[:, inside], out_sems.at[8 + q]
        )
        copy.start()
        results.append(copy)
    wet8 = table[0:MARGIN]
    row = rows_in((MARGIN, extent))
    for block in range(BASE // MARGIN, (BASE + width) // MARGIN):
        ocean[block * MARGIN : (block + 1) * MARGIN] = wet8
    diag[BASE : BASE + width] = (
        0.5 * (table[0:1] * (6.0 + damp[...]) + (1.0 - table[0:1])) - 2.0
    )
    fields[1, BASE : BASE + width] = start_in[...]

    for side, message in ((0, low), (1, high)):
        wet_out = jnp.broadcast_to(message[3, PAD - 1 : PAD], (MARGIN, extent))
        outer = 0 if side == 0 else BASE + width
        for block in range(BASE // MARGIN):
            ocean[outer + block * MARGIN : outer + (block + 1) * MARGIN] = wet_out
        halo = MARGIN if side == 0 else BASE + width
        wet_row = wet_out[0:1]
        diag[halo : halo + PAD] = 0.5 * (
            wet_row * (6.0 + message[1]) + (1.0 - wet_row)
        ) - 2.0
        if side == 0:
            around = jnp.concatenate([wet_out, wet8, wet8], axis=0)
            beyond = jnp.concatenate([wet_out, wet_out, wet8], axis=0)
        else:
            around = jnp.concatenate([wet8, wet8, wet_out], axis=0)
            beyond = jnp.concatenate([wet8, wet_out, wet_out], axis=0)
        east_own = (around * shift(around, -1, 0))[:PAD]
        east_out = (beyond * shift(beyond, -1, 0))[:PAD]
        north_own = north_wetness(wet8)
        north_out = north_wetness(wet_out)

        mine_at = slice(MARGIN, BASE) if side == 0 else slice(width - MARGIN, width + MARGIN)
        rim_at = slice(0, PAD) if side == 0 else slice(width - PAD, width)

        def level_step(k, sums, side=side, message=message, east_own=east_own,
                       east_out=east_out, north_own=north_own, north_out=north_out,
                       wet_out=wet_out, mine_at=mine_at, rim_at=rim_at):
            weight = table[pl.ds(MARGIN + k, 1)]
            own, out = [], []
            for q in (2, 3):
                place = (q - 2) * MARGIN + 2 * k
                nearer, farther = message[2, pl.ds(place, 1)], message[2, pl.ds(place + 1, 1)]
                mine = flows[q - 2][k, mine_at]
                if side == 0:
                    piece = jnp.where(row == MARGIN - 1, farther, nearer)
                    own.append(jnp.concatenate([piece, mine], axis=0))
                    out.append(jnp.concatenate([piece, piece, mine[:MARGIN]], axis=0))
                else:
                    piece = jnp.where(row == 0, nearer, farther)
                    own.append(jnp.concatenate([mine, piece], axis=0))
                    out.append(jnp.concatenate([mine[MARGIN:], piece, piece], axis=0))
            east, north = face_speeds(own[0], own[1], east_own, north_own)
            au = advect(own[0], east, north, wet8)
            av = advect(own[1], east, north, wet8)
            fresh = [None, None, au, av]
            for q in range(2):
                mine = tracers[q][k, mine_at]
                piece = jnp.broadcast_to(
                    message[3, pl.ds(q * levels + k, 1)], (MARGIN, extent)
                )
                if side == 0:
                    window = jnp.concatenate([piece, mine], axis=0)
                else:
                    window = jnp.concatenate([mine, piece], axis=0)
                fresh[q] = advect(window, east, north, wet8)
            for q in range(4):
                old = staged[q, k, rim_at].astype(jnp.float32)
                if side == 0:
                    value = jnp.concatenate([fresh[q], old[MARGIN:]], axis=0)
                else:
                    value = jnp.concatenate([old[:MARGIN], fresh[q]], axis=0)
                edge_out[q, side, k] = value.astype(edge_out.dtype)
            east, north = face_speeds(out[0], out[1], east_out, north_out)
            bu = advect(out[0], east, north, wet_out)
            bv = advect(out[1], east, north, wet_out)
            return (
                sums[0] + weight * au,
                sums[1] + weight * av,
                sums[2] + weight * bu,
                sums[3] + weight * bv,
            )

        zero = jnp.zeros((MARGIN, extent), jnp.float32)
        flow, cross, flow_out, cross_out = lax.fori_loop(
            0, levels, level_step, (zero, zero, zero, zero), unroll=2
        )
        known = message[3, MARGIN:PAD]
        given = message[0]
        if side == 0:
            flow_out = jnp.where(row == MARGIN - 1, flow_out, shift(known, 5, 0))
            cross_out = jnp.where(row == MARGIN - 1, cross_out, shift(known, 4, 0))
            whole = divergence(
                jnp.concatenate([wet_out, wet8], axis=0),
                jnp.concatenate([flow_out, flow], axis=0),
                jnp.concatenate([cross_out, cross], axis=0),
            )
            fields[1, MARGIN : 2 * MARGIN] = given[:MARGIN]
            fields[1, 2 * MARGIN : BASE] = jnp.where(
                row >= MARGIN - 2, whole[:MARGIN], given[MARGIN:]
            )
            fields[1, BASE : BASE + MARGIN] = jnp.where(
                row < 2, whole[MARGIN:], start_in[0:MARGIN]
            )
        else:
            flow_out = jnp.where(row == 0, flow_out, shift(known, 1, 0))
            cross_out = jnp.where(row == 0, cross_out, shift(known, -1, 0))
            whole = divergence(
                jnp.concatenate([wet8, wet_out], axis=0),
                jnp.concatenate([flow, flow_out], axis=0),
                jnp.concatenate([cross, cross_out], axis=0),
            )
            top = BASE + width
            fields[1, top - MARGIN : top] = jnp.where(
                row >= MARGIN - 2, whole[:MARGIN], start_in[width - MARGIN : width]
            )
            fields[1, top : top + MARGIN] = jnp.where(row < 2, whole[MARGIN:], given[:MARGIN])
            fields[1, top + MARGIN : top + PAD] = given[MARGIN:]

    for q, target in enumerate(targets):
        for side in range(2):
            first = 0 if side == 0 else width - PAD
            copy = pltpu.make_async_copy(
                edge_out.at[q, side],
                target.at[:, pl.ds(first, PAD)],
                out_sems.at[2 * q + side],
            )
            copy.start()
            results.append(copy)

    strips = (width + 2 * PAD) // PAD
    none = jnp.zeros((MARGIN, 128), jnp.float32)

    def inner(a, b, total):
        product = a * b
        part = product[:MARGIN] + product[MARGIN:]
        pieces = [part[:, i : i + 128] for i in range(0, extent, 128)]
        while len(pieces) > 1:
            pieces = [x + y for x, y in zip(pieces[::2], pieces[1::2])]
        s, e = two_sum(total[0], pieces[0])
        return s, total[1] + e

    square = (none, none)
    for strip in range(strips):
        keep = slice(MARGIN + strip * PAD, BASE + strip * PAD)
        half[keep] = 0.5 * ocean[keep]
        masked[0][keep] = half[keep] * fields[1, keep]
        fields[0, keep] = jnp.zeros((PAD, extent), jnp.float32)
        if 0 < strip < strips - 1:
            value = fields[1, keep]
            square = inner(value, value, square)
    acc[0, 0:MARGIN] = square[0]
    acc[1, 0:MARGIN] = square[1]
    for slot in range(2 * STEPS + 1, acc.shape[1] // MARGIN):
        acc[0, slot * MARGIN : (slot + 1) * MARGIN] = none
        acc[1, slot * MARGIN : (slot + 1) * MARGIN] = none

    def basis_step(j, now, scale):
        mixed, square = (none, none), (none, none)
        for strip in range(strips):
            start = MARGIN + strip * PAD
            around = slice(start - MARGIN, start + BASE)
            keep = slice(start, start + PAD)
            wide = masked[now][around]
            sides = (shift(wide, -1, 0) + shift(wide, 1, 0))[MARGIN:BASE]
            column = wide[MARGIN:BASE] + 0.5 * sides
            near = sides + (north_of(column) + south_of(column))
            centre = fields[j + 1, keep]
            following = diag[keep] * centre - ocean[keep] * near
            if scale is not None:
                following = scale * following
            following = following - fields[j, keep]
            fields[j + 2, keep] = following
            masked[1 - now][keep] = half[keep] * following
            if 0 < strip < strips - 1:
                mixed = inner(centre, following, mixed)
                square = inner(following, following, square)
        for place, value in ((2 * j + 1, mixed), (2 * j + 2, square)):
            at = pl.ds(pl.multiple_of(place * MARGIN, MARGIN), MARGIN)
            acc[0, at] = value[0]
            acc[1, at] = value[1]

    def step_pair(index, carry):
        basis_step(2 * index, 0, jnp.where(index == 0, 0.5, 1.0))
        basis_step(2 * index + 1, 1, None)
        return carry

    lax.fori_loop(0, STEPS // 2, step_pair, 0)

    slots = acc.shape[1] // MARGIN
    pairs = [
        (acc[0, pl.ds(s, slots, stride=MARGIN)], acc[1, pl.ds(s, slots, stride=MARGIN)])
        for s in range(MARGIN)
    ]
    while len(pairs) > 1:
        pairs = [pair_add(x, y) for x, y in zip(pairs[::2], pairs[1::2])]
    total = pairs[0]
    step = 64
    while step:
        total = pair_add(total, (shift(total[0], step, 1), shift(total[1], step, 1)))
        step //= 2
    row = lax.broadcasted_iota(jnp.int32, (MARGIN, 128), 0)
    place = lax.broadcasted_iota(jnp.int32, (MARGIN, 128), 1)
    lined = []
    for part in total:
        merged = none
        for group in range(slots // MARGIN):
            merged = jnp.where(
                place // MARGIN == group, part[group * MARGIN : (group + 1) * MARGIN], merged
            )
        merged = jnp.where(place % MARGIN == row, merged, 0.0)
        for s in (4, 2, 1):
            merged = merged + shift(merged, s, 0)
        lined.append(merged)
    o_sums[...] = jnp.broadcast_to(jnp.where(row < 4, lined[0], lined[1])[None], o_sums.shape)
    for copy in results:
        copy.wait()


def edge_advance(staged, start, damp, table, low, high, bands, members):
    levels, width, extent = staged.shape[1:]
    span = width + 2 * BASE
    slots = 32
    anywhere = pl.BlockSpec(memory_space=pl.ANY)
    vmem = pl.BlockSpec(memory_space=pltpu.VMEM)
    tracer = jax.ShapeDtypeStruct((levels, width, extent), staged.dtype)
    f32 = jnp.float32
    return pl.pallas_call(
        edge_kernel,
        out_shape=[tracer] * 4
        + [
            jax.ShapeDtypeStruct((STEPS + 2, span, extent), f32),
            jax.ShapeDtypeStruct((members, MARGIN, 128), f32),
        ],
        in_specs=[vmem] * (6 + len(bands)),
        out_specs=[anywhere] * 4 + [vmem] * 2,
        scratch_shapes=[
            pltpu.VMEM((span, extent), f32),
            pltpu.VMEM((span, extent), f32),
            pltpu.VMEM((span, extent), f32),
            pltpu.VMEM((span, extent), f32),
            pltpu.VMEM((span, extent), f32),
            pltpu.VMEM((4, 2, levels, PAD, extent), jnp.bfloat16),
            pltpu.VMEM((2, slots * MARGIN, 128), f32),
            pltpu.SemaphoreType.DMA((12,)),
        ],
        cost_estimate=pl.CostEstimate(
            flops=10000000000, bytes_accessed=5000000, transcendentals=0
        ),
        compiler_params=pltpu.CompilerParams(vmem_limit_bytes=VMEM_BYTES - EDGE_ROOM),
        name="edge_advance",
    )(staged, start, damp, table, low, high, *bands)


def combine_kernel(sums, fields, height, resid):
    members = sums.shape[0]
    lane = lax.broadcasted_iota(jnp.int32, (MARGIN, 128), 1)
    row = lax.broadcasted_iota(jnp.int32, (MARGIN, 128), 0)
    pieces = [(sums[i], jnp.zeros((MARGIN, 128), jnp.float32)) for i in range(members)]
    while len(pieces) > 1:
        merged = []
        for x, y in zip(pieces[::2], pieces[1::2]):
            s, e = two_sum(x[0], y[0])
            merged.append((s, (x[1] + y[1]) + e))
        if len(pieces) % 2:
            merged.append(pieces[-1])
        pieces = merged
    total, error = pieces[0]
    other = shift(total, 4, 0)
    error_other = shift(error, 4, 0)
    upper = row < 4
    dots = fast_two_sum(
        jnp.where(upper, total, other),
        jnp.where(upper, other, total) + jnp.where(upper, error, error_other),
    )

    def at(x, k):
        return jnp.broadcast_to(x[:, k : k + 1], x.shape)

    odd = lane % 2 == 1
    anchor = tuple(jnp.where(odd, at(x, 1), at(x, 0)) for x in dots)
    moments = pair_add((2.0 * dots[0], 2.0 * dots[1]), (-anchor[0], -anchor[1]))
    inside = lane <= 2 * STEPS
    moments = tuple(jnp.where(inside, x, 0.0) for x in moments)

    def ahead(x):
        return shift(x, -1, 1)

    def behind(x):
        return shift(x, 1, 1)

    def image_of_products(x):
        after = tuple(ahead(c) for c in x)
        before = tuple(jnp.where(lane == 0, a, behind(c)) for a, c in zip(after, x))
        out = pair_add(pair_add(after, before), (2.0 * x[0], 2.0 * x[1]))
        return 0.25 * out[0], 0.25 * out[1]

    def image_of_coefficients(x):
        after = tuple(ahead(c) for c in x)
        before = tuple(
            jnp.where(lane == 0, 0.0, jnp.where(lane == 1, 2.0 * behind(c), behind(c))) for c in x
        )
        out = pair_add(pair_add(after, before), (2.0 * x[0], 2.0 * x[1]))
        return 0.25 * out[0], 0.25 * out[1]

    unit = jnp.where(lane == 0, 1.0, 0.0).astype(jnp.float32)
    zero = jnp.zeros_like(unit)
    r_products, p_products = moments, moments
    c_r, c_p, c_x = (unit, zero), (unit, zero), zero

    def pick(x, k):
        return at(x[0], k), at(x[1], k)

    def quarter_sum(before, here, after):
        out = pair_add(pair_add(after, before), (2.0 * here[0], 2.0 * here[1]))
        return 0.25 * out[0], 0.25 * out[1]

    norm = pick(r_products, 0)
    for k in range(STEPS):
        near = [pick(p_products, abs(k - 1)), pick(p_products, k)]
        near += [pick(p_products, k + 1), pick(p_products, k + 2)]
        energy = quarter_sum(near[0], near[1], near[2])
        alpha = norm[0] / energy[0]
        c_x = c_x + alpha * c_p[0]
        c_r = pair_add(c_r, pair_scale(image_of_coefficients(c_p), -alpha))
        if k + 1 < STEPS:
            change = pair_scale(image_of_products(p_products), -alpha)
            following = pair_scale(quarter_sum(near[1], near[2], near[3]), -alpha)
            following = pair_add(pick(r_products, k + 1), following)
            r_products = pair_add(r_products, change)
            lead = 0.5 if k == 0 else 0.25
            beta = (-lead * alpha) * following[0] / norm[0]
            p_products = pair_add(r_products, pair_scale(p_products, beta))
            c_p = pair_add(c_r, pair_scale(c_p, beta))
            norm = following

    width = height.shape[0]
    weights_x = [at(c_x, j)[0:1] for j in range(STEPS + 1)]
    weights_r = [at(c_r[0], j)[0:1] for j in range(STEPS + 1)]
    for first in range(0, width, MARGIN):
        keep = slice(first, first + MARGIN)
        wide = slice(BASE + first, BASE + first + MARGIN)
        for left in range(0, height.shape[1], 128):
            cols = slice(left, left + 128)
            value = fields[1, wide, cols]
            h, r = weights_x[0] * value, weights_r[0] * value
            for j in range(1, STEPS + 1):
                value = fields[j + 1, wide, cols]
                h, r = h + weights_x[j] * value, r + weights_r[j] * value
            height[keep, cols] = h
            resid[keep, cols] = r


def combine(sums, fields, width):
    plane = jax.ShapeDtypeStruct((width, fields.shape[2]), jnp.float32)
    vmem = pl.BlockSpec(memory_space=pltpu.VMEM)
    return pl.pallas_call(
        combine_kernel,
        out_shape=[plane, plane],
        in_specs=[vmem, vmem],
        out_specs=[vmem, vmem],
        compiler_params=pltpu.CompilerParams(vmem_limit_bytes=8 * 1024 * 1024),
        name="combine",
    )(sums, fields)


def on_device(
    heat_anomaly,
    saltiness_anomaly,
    first_axis_flow,
    second_axis_flow,
    layer_spacing,
    diagonal_shift,
    water_tile_flags,
):
    members = lax.axis_size("blk")
    bands = fetch(heat_anomaly, saltiness_anomaly, first_axis_flow, second_axis_flow)
    to_next, to_last, table = pack(water_tile_flags, layer_spacing[None], diagonal_shift, bands)
    forward = [(i, (i + 1) % members) for i in range(members)]
    backward = [(target, source) for source, target in forward]
    low = lax.ppermute(to_next, "blk", forward)
    high = lax.ppermute(to_last, "blk", backward)
    staged, start = inner_advance(table, bands)
    *tracers, basis, sums = edge_advance(
        staged, start, diagonal_shift, table, low, high, bands, members
    )
    gathered = lax.all_to_all(sums, "blk", 0, 0)
    height, resid = combine(gathered, basis, diagonal_shift.shape[0])
    return (*tracers, height, resid)


def solution(mesh):
    columns = P("member", "blk", None)
    return jax.shard_map(
        on_device,
        mesh=mesh,
        in_specs=(columns, columns, columns, columns, P(), P("blk", None), P("blk", None)),
        out_specs=(
            columns,
            columns,
            columns,
            columns,
            P(("member", "blk"), None),
            P(("member", "blk"), None),
        ),
        check_vma=False,
    )
```

```python
import functools

import jax
import jax.numpy as jnp
from jax import lax
from jax.experimental import pallas as pl
from jax.experimental.pallas import tpu as pltpu
from jax.sharding import PartitionSpec as P

SSTEP = 4
CG_BLOCKS = 3
STEPS = SSTEP * CG_BLOCKS
COURANT = 0.2
PAD = 16
MARGIN = 8
BASE = PAD + MARGIN
KIB = 1024
PARTS = 2
VMEM_BYTES = 65472 * KIB
FETCH_ROOM = 14480 * KIB
PACK_ROOM = 32000 * KIB
INNER_ROOM = 32000 * KIB
EDGE_ROOM = 45 * KIB * KIB


def shift(value, amount, axis):
    return pltpu.roll(value, amount % value.shape[axis], axis)


def two_sum(a, b):
    s = a + b
    t = s - a
    return s, (a - (s - t)) + (b - t)


def fast_two_sum(a, b):
    s = a + b
    return s, b - (s - a)


def split(a):
    c = 4097.0 * a
    hi = c - (c - a)
    return hi, a - hi


def two_prod(a, b):
    p = a * b
    ah, al = split(a)
    bh, bl = split(b)
    return p, ((ah * bh - p) + ah * bl + al * bh) + al * bl


def pair_add(a, b):
    s, e = two_sum(a[0], b[0])
    return fast_two_sum(s, e + (a[1] + b[1]))


def pair_scale(a, c):
    p, e = two_prod(a[0], c)
    return p, e + a[1] * c


def upwind(speed, behind, ahead):
    return speed * jnp.where(speed > 0.0, behind, ahead)


def face_speeds(u, v, east_wet, north_wet):
    east = 0.5 * (u + shift(u, -1, 0))[:-MARGIN] * east_wet
    centre = v[MARGIN:-MARGIN]
    north = 0.5 * (centre + shift(centre, -1, 1)) * north_wet
    return east, north


def east_flow(q, east):
    return upwind(east, q[:-MARGIN], shift(q, -1, 0)[:-MARGIN])


def advect(q, east, north, wet, east_flux=None):
    if east_flux is None:
        east_flux = east_flow(q, east)
    centre = q[MARGIN:-MARGIN]
    north_flux = upwind(north, centre, shift(centre, -1, 1))
    spread = (east_flux - shift(east_flux, 1, 0))[MARGIN:] + (
        north_flux - shift(north_flux, 1, 1)
    )
    return wet * (centre - COURANT * spread)


def lanes(shape):
    return lax.broadcasted_iota(jnp.int32, shape, 1)


def rows_in(shape):
    return lax.broadcasted_iota(jnp.int32, shape, 0)


def north_of(x):
    return jnp.where(lanes(x.shape) == x.shape[1] - 1, 0.0, shift(x, -1, 1))


def south_of(x):
    return jnp.where(lanes(x.shape) == 0, 0.0, shift(x, 1, 1))


def north_wetness(wet):
    return wet * north_of(wet)


def divergence(wet, flow, cross):
    east_part = shift(flow, -1, 0) - shift(flow, 1, 0)
    return wet * (0.5 * (east_part + (north_of(cross) - south_of(cross))))


class Band:
    def __init__(self, parts):
        self.parts = parts

    def __getitem__(self, at):
        return jnp.concatenate([part[at] for part in self.parts], axis=-1)


def bands_of(refs):
    return [Band(refs[q * PARTS : (q + 1) * PARTS]) for q in range(4)]


def fetch_kernel(heat, salt, u, v, *refs):
    width, extent = u.shape[1:]
    parts, sems = refs[: 4 * PARTS], refs[4 * PARTS]
    share = extent // PARTS
    copies = []
    for q, source in enumerate((heat, salt, u, v)):
        for part in range(PARTS):
            copy = pltpu.make_async_copy(
                source.at[:, :, pl.ds(part * share, share)],
                parts[q * PARTS + part].at[:, pl.ds(MARGIN, width)],
                sems.at[len(copies)],
            )
            copy.start()
            copies.append(copy)
    for copy in copies:
        copy.wait()


def fetch(heat, salt, u, v):
    levels, width, extent = u.shape
    band = jax.ShapeDtypeStruct((levels, width + PAD, extent // PARTS), u.dtype)
    return pl.pallas_call(
        fetch_kernel,
        out_shape=[band] * (4 * PARTS),
        in_specs=[pl.BlockSpec(memory_space=pl.ANY)] * 4,
        out_specs=[pl.BlockSpec(memory_space=pltpu.VMEM)] * (4 * PARTS),
        scratch_shapes=[pltpu.SemaphoreType.DMA((4 * PARTS,))],
        cost_estimate=pl.CostEstimate(
            flops=10000000000, bytes_accessed=5000000, transcendentals=0
        ),
        compiler_params=pltpu.CompilerParams(vmem_limit_bytes=VMEM_BYTES - FETCH_ROOM),
        name="fetch",
    )(heat, salt, u, v)


def pack_kernel(flags, spacing, damp, *refs):
    heat, salt, u, v = bands_of(refs)
    o_low, o_high, o_table = refs[4 * PARTS :]
    levels = spacing.shape[1]
    width, extent = damp.shape
    tiles = flags.shape[1]
    flows, tracers = (u, v), (heat, salt)
    messages = (o_high, o_low)
    lane = lanes((MARGIN, extent))
    wet = jnp.zeros((MARGIN, extent), jnp.float32)
    flag = flags[...].astype(jnp.float32)
    for tile in range(tiles):
        inside = (lane >= tile * (extent // tiles)) & (lane < (tile + 1) * (extent // tiles))
        wet = jnp.where(inside, flag[:, tile : tile + 1], wet)
    o_table[0:MARGIN] = wet
    wet_row = wet[0:1]
    east_wet = wet_row * wet_row
    north_wet = north_wetness(wet)[0:1]
    row = rows_in((MARGIN, extent))
    thick = [spacing[:, k : k + 1] for k in range(levels)]
    total = thick[0]
    for k in range(1, levels):
        total = total + thick[k]
    weights = jnp.zeros((MARGIN, extent), jnp.float32)
    for k in range(levels):
        weights = jnp.where(row == k, thick[k], weights)
    o_table[MARGIN:PAD] = weights / total
    for end in range(2):
        message = messages[end]
        rows = slice(0, 2 * PAD) if end == 0 else slice(width - PAD, width + PAD)

        face = MARGIN - 1 if end == 0 else BASE - 1
        closed = rows_in((BASE, extent)) == face

        def level_step(k, sums, rows=rows, closed=closed):
            weight = o_table[pl.ds(MARGIN + k, 1)]
            qu = u[k, rows]
            qv = v[k, rows]
            east, north = face_speeds(qu, qv, east_wet, north_wet)
            fu = jnp.where(closed, 0.0, east_flow(qu, east))
            fv = jnp.where(closed, 0.0, east_flow(qv, east))
            au = advect(qu, east, north, wet_row, fu)
            av = advect(qv, east, north, wet_row, fv)
            return sums[0] + weight * au, sums[1] + weight * av

        zero = jnp.zeros((PAD, extent), jnp.float32)
        flow, cross = lax.fori_loop(0, levels, level_step, (zero, zero), unroll=4)
        start = divergence(wet_row, flow, cross)
        first = 0 if end == 0 else width - PAD
        damping = damp[first : first + PAD]
        near = slice(0, MARGIN) if end == 0 else slice(MARGIN, PAD)
        far = slice(MARGIN, PAD) if end == 0 else slice(0, MARGIN)
        message[0] = start[near]
        message[1] = damping[near]
        natural = row < 4 if end == 0 else row >= 4
        message[2] = jnp.where(natural, start[far], shift(damping[far], 4, 0))
        tip = slice(MARGIN, PAD) if end == 0 else slice(width, width + MARGIN)
        for slot, pair in ((3, flows), (4, tracers)):
            merged = jnp.zeros((MARGIN, extent), jnp.float32)
            for q in range(2):
                for k in range(levels):
                    place = q * levels + k
                    piece = shift(pair[q][k, tip], place if end == 0 else place + 1, 0)
                    merged = jnp.where(row == place, piece, merged)
            message[slot] = merged
        flow, cross = flow[near], cross[near]
        turns = (0, 1, 1, 3) if end == 0 else (1, 2, 5, 6)
        tail = jnp.where(row == 4, shift(cross, turns[3], 0), wet)
        tail = jnp.where((row == 2) | (row == 3), shift(flow, turns[2], 0), tail)
        tail = jnp.where(row == 1, shift(cross, turns[1], 0), tail)
        message[5] = jnp.where(row == 0, shift(flow, turns[0], 0) if end else flow, tail)


def pack(flags, spacing, damp, bands):
    extent = damp.shape[1]
    f32 = jnp.float32
    message = jax.ShapeDtypeStruct((6, MARGIN, extent), f32)
    vmem = pl.BlockSpec(memory_space=pltpu.VMEM)
    return pl.pallas_call(
        pack_kernel,
        out_shape=[message, message, jax.ShapeDtypeStruct((PAD, extent), f32)],
        in_specs=[vmem] * (3 + len(bands)),
        out_specs=[vmem] * 3,
        compiler_params=pltpu.CompilerParams(vmem_limit_bytes=VMEM_BYTES - PACK_ROOM),
        name="pack",
    )(flags, spacing, damp, *bands)


def inner_kernel(table, *refs):
    heat, salt, u, v = bands_of(refs)
    staged, o_start, tu, tv = refs[4 * PARTS :]
    levels = staged.shape[1]
    width, extent = o_start.shape
    wet = table[0:1]
    north_wet = north_wetness(table[0:MARGIN])[0:1]
    east_wet = wet * wet
    tu[...] = jnp.zeros_like(tu)
    tv[...] = jnp.zeros_like(tv)

    def level_step(k, carry):
        weight = table[pl.ds(MARGIN + k, 1)]

        def strip(index, carry):
            local = pl.ds(pl.multiple_of(index * PAD, PAD), PAD)
            later = pl.ds(pl.multiple_of(index * PAD + MARGIN, MARGIN), PAD)
            rows = pl.ds(pl.multiple_of(index * PAD, MARGIN), 2 * PAD)
            qu = u[k, rows]
            qv = v[k, rows]
            east, north = face_speeds(qu, qv, east_wet, north_wet)
            au = advect(qu, east, north, wet)
            av = advect(qv, east, north, wet)
            staged[2, k, local] = au.astype(staged.dtype)
            staged[3, k, local] = av.astype(staged.dtype)
            tu[later] += weight * au
            tv[later] += weight * av
            staged[0, k, local] = advect(heat[k, rows], east, north, wet).astype(staged.dtype)
            staged[1, k, local] = advect(salt[k, rows], east, north, wet).astype(staged.dtype)
            return carry

        lax.fori_loop(0, width // PAD, strip, 0, unroll=2)
        return carry

    lax.fori_loop(0, levels, level_step, 0)
    for first in range(0, width, PAD):
        keep = slice(first, first + PAD)
        flow = tu[first : first + 2 * PAD]
        cross = tv[first + MARGIN : first + BASE]
        east_part = (shift(flow, -1, 0) - shift(flow, 1, 0))[MARGIN:BASE]
        o_start[keep] = wet * (0.5 * (east_part + (north_of(cross) - south_of(cross))))


def inner_advance(table, bands):
    levels, padded, share = bands[0].shape
    width, extent = padded - PAD, share * PARTS
    f32 = jnp.float32
    vmem = pl.BlockSpec(memory_space=pltpu.VMEM)
    return pl.pallas_call(
        inner_kernel,
        out_shape=[
            jax.ShapeDtypeStruct((4, levels, width, extent), jnp.bfloat16),
            jax.ShapeDtypeStruct((width, extent), f32),
        ],
        in_specs=[vmem] * (1 + len(bands)),
        out_specs=[vmem] * 2,
        scratch_shapes=[
            pltpu.VMEM((width + PAD, extent), f32),
            pltpu.VMEM((width + PAD, extent), f32),
        ],
        cost_estimate=pl.CostEstimate(
            flops=10000000000, bytes_accessed=5000000, transcendentals=0
        ),
        compiler_params=pltpu.CompilerParams(vmem_limit_bytes=VMEM_BYTES - INNER_ROOM),
        name="inner_advance",
    )(table, *bands)


def edge_kernel(staged, start_in, damp, table, low, high, *refs):
    heat, salt, u, v = bands_of(refs)
    refs = refs[4 * PARTS :]
    levels = staged.shape[1]
    width, extent = start_in.shape
    span = width + 2 * BASE
    flows, tracers = (u, v), (heat, salt)
    o_heat, o_salt, o_u, o_v, fields, o_sums = refs[:6]
    ocean, half, diag, even, odd, edge_out, acc, out_sems = refs[6:]
    masked = (even, odd)
    targets = (o_heat, o_salt, o_u, o_v)
    inside = pl.ds(PAD, width - 2 * PAD)
    results = []
    for q in range(4):
        copy = pltpu.make_async_copy(
            staged.at[q, :, inside], targets[q].at[:, inside], out_sems.at[8 + q]
        )
        copy.start()
        results.append(copy)
    wet8 = table[0:MARGIN]
    row = rows_in((MARGIN, extent))
    for block in range(BASE // MARGIN, (BASE + width) // MARGIN):
        ocean[block * MARGIN : (block + 1) * MARGIN] = wet8
    diag[BASE : BASE + width] = (
        0.5 * (table[0:1] * (6.0 + damp[...]) + (1.0 - table[0:1])) - 2.0
    )
    fields[1, BASE : BASE + width] = start_in[...]

    for side, message in ((0, low), (1, high)):
        wet_out = jnp.broadcast_to(message[5, MARGIN - 1 : MARGIN], (MARGIN, extent))
        outer = 0 if side == 0 else BASE + width
        for block in range(BASE // MARGIN):
            ocean[outer + block * MARGIN : outer + (block + 1) * MARGIN] = wet_out
        wet_row = wet_out[0:1]
        near = 2 * MARGIN if side == 0 else BASE + width
        far = MARGIN if side == 0 else BASE + width + MARGIN
        for at, damping in ((near, message[1]), (far, shift(message[2], 4, 0))):
            diag[at : at + MARGIN] = 0.5 * (
                wet_row * (6.0 + damping) + (1.0 - wet_row)
            ) - 2.0
        if side == 0:
            around = jnp.concatenate([wet_out, wet8, wet8], axis=0)
        else:
            around = jnp.concatenate([wet8, wet8, wet_out], axis=0)
        east_own = (around * shift(around, -1, 0))[:PAD]
        north_own = north_wetness(wet8)

        mine_at = slice(MARGIN, BASE) if side == 0 else slice(width - MARGIN, width + MARGIN)
        rim_at = slice(0, PAD) if side == 0 else slice(width - PAD, width)

        def level_step(k, sums, side=side, message=message, east_own=east_own,
                       north_own=north_own, mine_at=mine_at, rim_at=rim_at):
            weight = table[pl.ds(MARGIN + k, 1)]
            windows = []
            for slot, pair in ((4, tracers), (3, flows)):
                for q in range(2):
                    mine = pair[q][k, mine_at]
                    piece = jnp.broadcast_to(
                        message[slot, pl.ds(q * levels + k, 1)], (MARGIN, extent)
                    )
                    pieces = [piece, mine] if side == 0 else [mine, piece]
                    windows.append(jnp.concatenate(pieces, axis=0))
            east, north = face_speeds(windows[2], windows[3], east_own, north_own)
            fluxes = [east_flow(window, east) for window in windows]
            fresh = [
                advect(window, east, north, wet8, flux)
                for window, flux in zip(windows, fluxes)
            ]
            for q in range(4):
                old = staged[q, k, rim_at].astype(jnp.float32)
                if side == 0:
                    value = jnp.concatenate([fresh[q], old[MARGIN:]], axis=0)
                else:
                    value = jnp.concatenate([old[:MARGIN], fresh[q]], axis=0)
                edge_out[q, side, k] = value.astype(edge_out.dtype)
            face_at = slice(0, MARGIN) if side == 0 else slice(MARGIN, PAD)
            return (
                sums[0] + weight * fresh[2],
                sums[1] + weight * fresh[3],
                sums[2] + weight * fluxes[2][face_at],
                sums[3] + weight * fluxes[3][face_at],
            )

        zero = jnp.zeros((MARGIN, extent), jnp.float32)
        flow, cross, flow_face, cross_face = lax.fori_loop(
            0, levels, level_step, (zero, zero, zero, zero), unroll=2
        )
        given, farther = message[0], message[2]
        known = [message[5, i : i + 1] for i in range(5)]
        change = (-COURANT if side == 0 else COURANT) * wet_out
        flow_tip = known[0] + change * jnp.broadcast_to(flow_face[MARGIN - 1 :], wet_out.shape)
        cross_tip = known[1] + change * jnp.broadcast_to(cross_face[MARGIN - 1 :], wet_out.shape)
        if side == 0:
            flow_out = jnp.where(row == MARGIN - 2, known[3], known[2])
            flow_out = jnp.where(row == MARGIN - 1, flow_tip, flow_out)
            cross_out = jnp.where(row == MARGIN - 1, cross_tip, known[4])
            whole = divergence(
                jnp.concatenate([wet_out, wet8], axis=0),
                jnp.concatenate([flow_out, flow], axis=0),
                jnp.concatenate([cross_out, cross], axis=0),
            )
            fields[1, MARGIN : 2 * MARGIN] = farther
            fields[1, 2 * MARGIN : BASE] = jnp.where(
                row >= MARGIN - 2, whole[:MARGIN], given
            )
            fields[1, BASE : BASE + MARGIN] = jnp.where(
                row < 2, whole[MARGIN:], start_in[0:MARGIN]
            )
        else:
            flow_out = jnp.where(row == 1, known[2], known[3])
            flow_out = jnp.where(row == 0, flow_tip, flow_out)
            cross_out = jnp.where(row == 0, cross_tip, known[4])
            whole = divergence(
                jnp.concatenate([wet8, wet_out], axis=0),
                jnp.concatenate([flow, flow_out], axis=0),
                jnp.concatenate([cross, cross_out], axis=0),
            )
            top = BASE + width
            fields[1, top - MARGIN : top] = jnp.where(
                row >= MARGIN - 2, whole[:MARGIN], start_in[width - MARGIN : width]
            )
            fields[1, top : top + MARGIN] = jnp.where(row < 2, whole[MARGIN:], given)
            fields[1, top + MARGIN : top + PAD] = farther

    for q, target in enumerate(targets):
        for side in range(2):
            first = 0 if side == 0 else width - PAD
            copy = pltpu.make_async_copy(
                edge_out.at[q, side],
                target.at[:, pl.ds(first, PAD)],
                out_sems.at[2 * q + side],
            )
            copy.start()
            results.append(copy)

    strips = (width + 2 * PAD) // PAD
    none = jnp.zeros((MARGIN, 128), jnp.float32)

    def inner(a, b, total):
        product = a * b
        part = product[:MARGIN] + product[MARGIN:]
        pieces = [part[:, i : i + 128] for i in range(0, extent, 128)]
        while len(pieces) > 1:
            pieces = [x + y for x, y in zip(pieces[::2], pieces[1::2])]
        s, e = two_sum(total[0], pieces[0])
        return s, total[1] + e

    square = (none, none)
    for strip in range(strips):
        keep = slice(MARGIN + strip * PAD, BASE + strip * PAD)
        half[keep] = 0.5 * ocean[keep]
        masked[0][keep] = half[keep] * fields[1, keep]
        fields[0, keep] = jnp.zeros((PAD, extent), jnp.float32)
        if 0 < strip < strips - 1:
            value = fields[1, keep]
            square = inner(value, value, square)
    acc[0, 0:MARGIN] = square[0]
    acc[1, 0:MARGIN] = square[1]
    for slot in range(2 * STEPS + 1, acc.shape[1] // MARGIN):
        acc[0, slot * MARGIN : (slot + 1) * MARGIN] = none
        acc[1, slot * MARGIN : (slot + 1) * MARGIN] = none

    def basis_step(j, now, scale):
        mixed, square = (none, none), (none, none)
        for strip in range(strips):
            start = MARGIN + strip * PAD
            around = slice(start - MARGIN, start + BASE)
            keep = slice(start, start + PAD)
            wide = masked[now][around]
            sides = (shift(wide, -1, 0) + shift(wide, 1, 0))[MARGIN:BASE]
            column = wide[MARGIN:BASE] + 0.5 * sides
            near = sides + (north_of(column) + south_of(column))
            centre = fields[j + 1, keep]
            following = diag[keep] * centre - ocean[keep] * near
            if scale is not None:
                following = scale * following
            following = following - fields[j, keep]
            fields[j + 2, keep] = following
            masked[1 - now][keep] = half[keep] * following
            if 0 < strip < strips - 1:
                mixed = inner(centre, following, mixed)
                square = inner(following, following, square)
        for place, value in ((2 * j + 1, mixed), (2 * j + 2, square)):
            at = pl.ds(pl.multiple_of(place * MARGIN, MARGIN), MARGIN)
            acc[0, at] = value[0]
            acc[1, at] = value[1]

    def step_pair(index, carry):
        basis_step(2 * index, 0, jnp.where(index == 0, 0.5, 1.0))
        basis_step(2 * index + 1, 1, None)
        return carry

    lax.fori_loop(0, STEPS // 2, step_pair, 0, unroll=2)

    slots = acc.shape[1] // MARGIN
    pairs = [
        (acc[0, pl.ds(s, slots, stride=MARGIN)], acc[1, pl.ds(s, slots, stride=MARGIN)])
        for s in range(MARGIN)
    ]
    while len(pairs) > 1:
        pairs = [pair_add(x, y) for x, y in zip(pairs[::2], pairs[1::2])]
    total = pairs[0]
    step = 64
    while step:
        total = pair_add(total, (shift(total[0], step, 1), shift(total[1], step, 1)))
        step //= 2
    row = lax.broadcasted_iota(jnp.int32, (MARGIN, 128), 0)
    place = lax.broadcasted_iota(jnp.int32, (MARGIN, 128), 1)
    lined = []
    for part in total:
        merged = none
        for group in range(slots // MARGIN):
            merged = jnp.where(
                place // MARGIN == group, part[group * MARGIN : (group + 1) * MARGIN], merged
            )
        merged = jnp.where(place % MARGIN == row, merged, 0.0)
        for s in (4, 2, 1):
            merged = merged + shift(merged, s, 0)
        lined.append(merged)
    o_sums[...] = jnp.broadcast_to(jnp.where(row < 4, lined[0], lined[1])[None], o_sums.shape)
    for copy in results:
        copy.wait()


def edge_advance(staged, start, damp, table, low, high, bands, members):
    levels, width, extent = staged.shape[1:]
    span = width + 2 * BASE
    slots = 32
    anywhere = pl.BlockSpec(memory_space=pl.ANY)
    vmem = pl.BlockSpec(memory_space=pltpu.VMEM)
    tracer = jax.ShapeDtypeStruct((levels, width, extent), staged.dtype)
    f32 = jnp.float32
    return pl.pallas_call(
        edge_kernel,
        out_shape=[tracer] * 4
        + [
            jax.ShapeDtypeStruct((STEPS + 2, span, extent), f32),
            jax.ShapeDtypeStruct((members, MARGIN, 128), f32),
        ],
        in_specs=[vmem] * (6 + len(bands)),
        out_specs=[anywhere] * 4 + [vmem] * 2,
        scratch_shapes=[
            pltpu.VMEM((span, extent), f32),
            pltpu.VMEM((span, extent), f32),
            pltpu.VMEM((span, extent), f32),
            pltpu.VMEM((span, extent), f32),
            pltpu.VMEM((span, extent), f32),
            pltpu.VMEM((4, 2, levels, PAD, extent), jnp.bfloat16),
            pltpu.VMEM((2, slots * MARGIN, 128), f32),
            pltpu.SemaphoreType.DMA((12,)),
        ],
        cost_estimate=pl.CostEstimate(
            flops=10000000000, bytes_accessed=5000000, transcendentals=0
        ),
        compiler_params=pltpu.CompilerParams(vmem_limit_bytes=VMEM_BYTES - EDGE_ROOM),
        name="edge_advance",
    )(staged, start, damp, table, low, high, *bands)


def combine_kernel(sums, fields, height, resid):
    members = sums.shape[0]
    lane = lax.broadcasted_iota(jnp.int32, (MARGIN, 128), 1)
    row = lax.broadcasted_iota(jnp.int32, (MARGIN, 128), 0)
    pieces = [(sums[i], jnp.zeros((MARGIN, 128), jnp.float32)) for i in range(members)]
    while len(pieces) > 1:
        merged = []
        for x, y in zip(pieces[::2], pieces[1::2]):
            s, e = two_sum(x[0], y[0])
            merged.append((s, (x[1] + y[1]) + e))
        if len(pieces) % 2:
            merged.append(pieces[-1])
        pieces = merged
    total, error = pieces[0]
    other = shift(total, 4, 0)
    error_other = shift(error, 4, 0)
    upper = row < 4
    dots = fast_two_sum(
        jnp.where(upper, total, other),
        jnp.where(upper, other, total) + jnp.where(upper, error, error_other),
    )

    def at(x, k):
        return jnp.broadcast_to(x[:, k : k + 1], x.shape)

    odd = lane % 2 == 1
    anchor = tuple(jnp.where(odd, at(x, 1), at(x, 0)) for x in dots)
    moments = pair_add((2.0 * dots[0], 2.0 * dots[1]), (-anchor[0], -anchor[1]))
    inside = lane <= 2 * STEPS
    moments = tuple(jnp.where(inside, x, 0.0) for x in moments)

    def ahead(x):
        return shift(x, -1, 1)

    def behind(x):
        return shift(x, 1, 1)

    def image_of_products(x):
        after = tuple(ahead(c) for c in x)
        before = tuple(jnp.where(lane == 0, a, behind(c)) for a, c in zip(after, x))
        out = pair_add(pair_add(after, before), (2.0 * x[0], 2.0 * x[1]))
        return 0.25 * out[0], 0.25 * out[1]

    def image_of_coefficients(x):
        after = tuple(ahead(c) for c in x)
        before = tuple(
            jnp.where(lane == 0, 0.0, jnp.where(lane == 1, 2.0 * behind(c), behind(c))) for c in x
        )
        out = pair_add(pair_add(after, before), (2.0 * x[0], 2.0 * x[1]))
        return 0.25 * out[0], 0.25 * out[1]

    unit = jnp.where(lane == 0, 1.0, 0.0).astype(jnp.float32)
    zero = jnp.zeros_like(unit)
    r_products, p_products = moments, moments
    c_r, c_p, c_x = (unit, zero), (unit, zero), zero

    def pick(x, k):
        return at(x[0], k), at(x[1], k)

    def quarter_sum(before, here, after):
        out = pair_add(pair_add(after, before), (2.0 * here[0], 2.0 * here[1]))
        return 0.25 * out[0], 0.25 * out[1]

    norm = pick(r_products, 0)
    for k in range(STEPS):
        near = [pick(p_products, abs(k - 1)), pick(p_products, k)]
        near += [pick(p_products, k + 1), pick(p_products, k + 2)]
        energy = quarter_sum(near[0], near[1], near[2])
        alpha = norm[0] / energy[0]
        c_x = c_x + alpha * c_p[0]
        c_r = pair_add(c_r, pair_scale(image_of_coefficients(c_p), -alpha))
        if k + 1 < STEPS:
            change = pair_scale(image_of_products(p_products), -alpha)
            following = pair_scale(quarter_sum(near[1], near[2], near[3]), -alpha)
            following = pair_add(pick(r_products, k + 1), following)
            r_products = pair_add(r_products, change)
            lead = 0.5 if k == 0 else 0.25
            beta = (-lead * alpha) * following[0] / norm[0]
            p_products = pair_add(r_products, pair_scale(p_products, beta))
            c_p = pair_add(c_r, pair_scale(c_p, beta))
            norm = following

    width = height.shape[0]
    weights_x = [at(c_x, j)[0:1] for j in range(STEPS + 1)]
    weights_r = [at(c_r[0], j)[0:1] for j in range(STEPS + 1)]
    for first in range(0, width, MARGIN):
        keep = slice(first, first + MARGIN)
        wide = slice(BASE + first, BASE + first + MARGIN)
        for left in range(0, height.shape[1], 128):
            cols = slice(left, left + 128)
            value = fields[1, wide, cols]
            h, r = weights_x[0] * value, weights_r[0] * value
            for j in range(1, STEPS + 1):
                value = fields[j + 1, wide, cols]
                h, r = h + weights_x[j] * value, r + weights_r[j] * value
            height[keep, cols] = h
            resid[keep, cols] = r


def combine(sums, fields, width):
    plane = jax.ShapeDtypeStruct((width, fields.shape[2]), jnp.float32)
    vmem = pl.BlockSpec(memory_space=pltpu.VMEM)
    return pl.pallas_call(
        combine_kernel,
        out_shape=[plane, plane],
        in_specs=[vmem, vmem],
        out_specs=[vmem, vmem],
        compiler_params=pltpu.CompilerParams(vmem_limit_bytes=8 * 1024 * 1024),
        name="combine",
    )(sums, fields)


def on_device(
    heat_anomaly,
    saltiness_anomaly,
    first_axis_flow,
    second_axis_flow,
    layer_spacing,
    diagonal_shift,
    water_tile_flags,
):
    members = lax.axis_size("blk")
    bands = fetch(heat_anomaly, saltiness_anomaly, first_axis_flow, second_axis_flow)
    to_next, to_last, table = pack(water_tile_flags, layer_spacing[None], diagonal_shift, bands)
    forward = [(i, (i + 1) % members) for i in range(members)]
    backward = [(target, source) for source, target in forward]
    low = lax.ppermute(to_next, "blk", forward)
    high = lax.ppermute(to_last, "blk", backward)
    staged, start = inner_advance(table, bands)
    *tracers, basis, sums = edge_advance(
        staged, start, diagonal_shift, table, low, high, bands, members
    )
    gathered = lax.all_to_all(sums, "blk", 0, 0)
    height, resid = combine(gathered, basis, diagonal_shift.shape[0])
    return (*tracers, height, resid)


def solution(mesh):
    columns = P("member", "blk", None)
    return jax.shard_map(
        on_device,
        mesh=mesh,
        in_specs=(columns, columns, columns, columns, P(), P("blk", None), P("blk", None)),
        out_specs=(
            columns,
            columns,
            columns,
            columns,
            P(("member", "blk"), None),
            P(("member", "blk"), None),
        ),
        check_vma=False,
    )
```

```python
import functools

import jax
import jax.numpy as jnp
from jax import lax
from jax.experimental import pallas as pl
from jax.experimental.pallas import tpu as pltpu
from jax.sharding import PartitionSpec as P

SSTEP = 4
CG_BLOCKS = 3
STEPS = SSTEP * CG_BLOCKS
COURANT = 0.2
PAD = 16
MARGIN = 8
BASE = PAD + MARGIN
KIB = 1024
PARTS = 2
UNROLL = 2
VMEM_BYTES = 65472 * KIB
FETCH_ROOM = 14480 * KIB
PACK_ROOM = 32000 * KIB
INNER_ROOM = 32000 * KIB
EDGE_ROOM = 45 * KIB * KIB


def shift(value, amount, axis):
    return pltpu.roll(value, amount % value.shape[axis], axis)


def two_sum(a, b):
    s = a + b
    t = s - a
    return s, (a - (s - t)) + (b - t)


def fast_two_sum(a, b):
    s = a + b
    return s, b - (s - a)


def split(a):
    c = 4097.0 * a
    hi = c - (c - a)
    return hi, a - hi


def two_prod(a, b):
    p = a * b
    ah, al = split(a)
    bh, bl = split(b)
    return p, ((ah * bh - p) + ah * bl + al * bh) + al * bl


def pair_add(a, b):
    s, e = two_sum(a[0], b[0])
    return fast_two_sum(s, e + (a[1] + b[1]))


def pair_scale(a, c):
    p, e = two_prod(a[0], c)
    return p, e + a[1] * c


def upwind(speed, behind, ahead):
    return speed * jnp.where(speed > 0.0, behind, ahead)


def face_speeds(u, v, east_wet, north_wet):
    east = 0.5 * (u + shift(u, -1, 0))[:-MARGIN] * east_wet
    centre = v[MARGIN:-MARGIN]
    north = 0.5 * (centre + shift(centre, -1, 1)) * north_wet
    return east, north


def east_flow(q, east):
    return upwind(east, q[:-MARGIN], shift(q, -1, 0)[:-MARGIN])


def advect(q, east, north, wet, east_flux=None):
    if east_flux is None:
        east_flux = east_flow(q, east)
    centre = q[MARGIN:-MARGIN]
    north_flux = upwind(north, centre, shift(centre, -1, 1))
    spread = (east_flux - shift(east_flux, 1, 0))[MARGIN:] + (
        north_flux - shift(north_flux, 1, 1)
    )
    return wet * (centre - COURANT * spread)


def lanes(shape):
    return lax.broadcasted_iota(jnp.int32, shape, 1)


def rows_in(shape):
    return lax.broadcasted_iota(jnp.int32, shape, 0)


def north_of(x):
    return jnp.where(lanes(x.shape) == x.shape[1] - 1, 0.0, shift(x, -1, 1))


def south_of(x):
    return jnp.where(lanes(x.shape) == 0, 0.0, shift(x, 1, 1))


def north_wetness(wet):
    return wet * north_of(wet)


def divergence(wet, flow, cross):
    east_part = shift(flow, -1, 0) - shift(flow, 1, 0)
    return wet * (0.5 * (east_part + (north_of(cross) - south_of(cross))))


class Band:
    def __init__(self, parts):
        self.parts = parts

    def __getitem__(self, at):
        return jnp.concatenate([part[at] for part in self.parts], axis=-1)


def bands_of(refs):
    return [Band(refs[q * PARTS : (q + 1) * PARTS]) for q in range(4)]


def fetch_kernel(heat, salt, u, v, *refs):
    width, extent = u.shape[1:]
    parts, sems = refs[: 4 * PARTS], refs[4 * PARTS]
    share = extent // PARTS
    copies = []
    for q, source in enumerate((heat, salt, u, v)):
        for part in range(PARTS):
            copy = pltpu.make_async_copy(
                source.at[:, :, pl.ds(part * share, share)],
                parts[q * PARTS + part].at[:, pl.ds(MARGIN, width)],
                sems.at[len(copies)],
            )
            copy.start()
            copies.append(copy)
    for copy in copies:
        copy.wait()


def fetch(heat, salt, u, v):
    levels, width, extent = u.shape
    band = jax.ShapeDtypeStruct((levels, width + PAD, extent // PARTS), u.dtype)
    return pl.pallas_call(
        fetch_kernel,
        out_shape=[band] * (4 * PARTS),
        in_specs=[pl.BlockSpec(memory_space=pl.ANY)] * 4,
        out_specs=[pl.BlockSpec(memory_space=pltpu.VMEM)] * (4 * PARTS),
        scratch_shapes=[pltpu.SemaphoreType.DMA((4 * PARTS,))],
        cost_estimate=pl.CostEstimate(
            flops=10000000000, bytes_accessed=5000000, transcendentals=0
        ),
        compiler_params=pltpu.CompilerParams(vmem_limit_bytes=VMEM_BYTES - FETCH_ROOM),
        name="fetch",
    )(heat, salt, u, v)


def pack_kernel(flags, spacing, damp, *refs):
    heat, salt, u, v = bands_of(refs)
    o_low, o_high, o_table = refs[4 * PARTS :]
    levels = spacing.shape[1]
    width, extent = damp.shape
    tiles = flags.shape[1]
    flows, tracers = (u, v), (heat, salt)
    messages = (o_high, o_low)
    lane = lanes((MARGIN, extent))
    wet = jnp.zeros((MARGIN, extent), jnp.float32)
    flag = flags[...].astype(jnp.float32)
    for tile in range(tiles):
        inside = (lane >= tile * (extent // tiles)) & (lane < (tile + 1) * (extent // tiles))
        wet = jnp.where(inside, flag[:, tile : tile + 1], wet)
    o_table[0:MARGIN] = wet
    wet_row = wet[0:1]
    east_wet = wet_row * wet_row
    north_wet = north_wetness(wet)[0:1]
    row = rows_in((MARGIN, extent))
    thick = [spacing[:, k : k + 1] for k in range(levels)]
    total = thick[0]
    for k in range(1, levels):
        total = total + thick[k]
    weights = jnp.zeros((MARGIN, extent), jnp.float32)
    for k in range(levels):
        weights = jnp.where(row == k, thick[k], weights)
    o_table[MARGIN:PAD] = weights / total
    for end in range(2):
        message = messages[end]
        rows = slice(0, 2 * PAD) if end == 0 else slice(width - PAD, width + PAD)

        face = MARGIN - 1 if end == 0 else BASE - 1
        closed = rows_in((BASE, extent)) == face

        def level_step(k, sums, rows=rows, closed=closed):
            weight = o_table[pl.ds(MARGIN + k, 1)]
            qu = u[k, rows]
            qv = v[k, rows]
            east, north = face_speeds(qu, qv, east_wet, north_wet)
            fu = jnp.where(closed, 0.0, east_flow(qu, east))
            fv = jnp.where(closed, 0.0, east_flow(qv, east))
            au = advect(qu, east, north, wet_row, fu)
            av = advect(qv, east, north, wet_row, fv)
            return sums[0] + weight * au, sums[1] + weight * av

        zero = jnp.zeros((PAD, extent), jnp.float32)
        flow, cross = lax.fori_loop(0, levels, level_step, (zero, zero), unroll=4)
        start = divergence(wet_row, flow, cross)
        first = 0 if end == 0 else width - PAD
        damping = damp[first : first + PAD]
        near = slice(0, MARGIN) if end == 0 else slice(MARGIN, PAD)
        far = slice(MARGIN, PAD) if end == 0 else slice(0, MARGIN)
        message[0] = start[near]
        message[1] = damping[near]
        natural = row < 4 if end == 0 else row >= 4
        message[2] = jnp.where(natural, start[far], shift(damping[far], 4, 0))
        tip = slice(MARGIN, PAD) if end == 0 else slice(width, width + MARGIN)
        for slot, pair in ((3, flows), (4, tracers)):
            merged = jnp.zeros((MARGIN, extent), jnp.float32)
            for q in range(2):
                for k in range(levels):
                    place = q * levels + k
                    piece = shift(pair[q][k, tip], place if end == 0 else place + 1, 0)
                    merged = jnp.where(row == place, piece, merged)
            message[slot] = merged
        flow, cross = flow[near], cross[near]
        turns = (0, 1, 1, 3) if end == 0 else (1, 2, 5, 6)
        tail = jnp.where(row == 4, shift(cross, turns[3], 0), wet)
        tail = jnp.where((row == 2) | (row == 3), shift(flow, turns[2], 0), tail)
        tail = jnp.where(row == 1, shift(cross, turns[1], 0), tail)
        message[5] = jnp.where(row == 0, shift(flow, turns[0], 0) if end else flow, tail)


def pack(flags, spacing, damp, bands):
    extent = damp.shape[1]
    f32 = jnp.float32
    message = jax.ShapeDtypeStruct((6, MARGIN, extent), f32)
    vmem = pl.BlockSpec(memory_space=pltpu.VMEM)
    return pl.pallas_call(
        pack_kernel,
        out_shape=[message, message, jax.ShapeDtypeStruct((PAD, extent), f32)],
        in_specs=[vmem] * (3 + len(bands)),
        out_specs=[vmem] * 3,
        compiler_params=pltpu.CompilerParams(vmem_limit_bytes=VMEM_BYTES - PACK_ROOM),
        name="pack",
    )(flags, spacing, damp, *bands)


def inner_kernel(table, *refs):
    heat, salt, u, v = bands_of(refs)
    staged, o_start, tu, tv = refs[4 * PARTS :]
    levels = staged.shape[1]
    width, extent = o_start.shape
    wet = table[0:1]
    north_wet = north_wetness(table[0:MARGIN])[0:1]
    east_wet = wet * wet
    tu[...] = jnp.zeros_like(tu)
    tv[...] = jnp.zeros_like(tv)

    def level_step(k, carry):
        weight = table[pl.ds(MARGIN + k, 1)]

        def strip(index, carry):
            local = pl.ds(pl.multiple_of(index * PAD, PAD), PAD)
            later = pl.ds(pl.multiple_of(index * PAD + MARGIN, MARGIN), PAD)
            rows = pl.ds(pl.multiple_of(index * PAD, MARGIN), 2 * PAD)
            qu = u[k, rows]
            qv = v[k, rows]
            east, north = face_speeds(qu, qv, east_wet, north_wet)
            au = advect(qu, east, north, wet)
            av = advect(qv, east, north, wet)
            staged[2, k, local] = au.astype(staged.dtype)
            staged[3, k, local] = av.astype(staged.dtype)
            tu[later] += weight * au
            tv[later] += weight * av
            staged[0, k, local] = advect(heat[k, rows], east, north, wet).astype(staged.dtype)
            staged[1, k, local] = advect(salt[k, rows], east, north, wet).astype(staged.dtype)
            return carry

        lax.fori_loop(0, width // PAD, strip, 0, unroll=2)
        return carry

    lax.fori_loop(0, levels, level_step, 0)
    for first in range(0, width, PAD):
        keep = slice(first, first + PAD)
        flow = tu[first : first + 2 * PAD]
        cross = tv[first + MARGIN : first + BASE]
        east_part = (shift(flow, -1, 0) - shift(flow, 1, 0))[MARGIN:BASE]
        o_start[keep] = wet * (0.5 * (east_part + (north_of(cross) - south_of(cross))))


def inner_advance(table, bands):
    levels, padded, share = bands[0].shape
    width, extent = padded - PAD, share * PARTS
    f32 = jnp.float32
    vmem = pl.BlockSpec(memory_space=pltpu.VMEM)
    return pl.pallas_call(
        inner_kernel,
        out_shape=[
            jax.ShapeDtypeStruct((4, levels, width, extent), jnp.bfloat16),
            jax.ShapeDtypeStruct((width, extent), f32),
        ],
        in_specs=[vmem] * (1 + len(bands)),
        out_specs=[vmem] * 2,
        scratch_shapes=[
            pltpu.VMEM((width + PAD, extent), f32),
            pltpu.VMEM((width + PAD, extent), f32),
        ],
        cost_estimate=pl.CostEstimate(
            flops=10000000000, bytes_accessed=5000000, transcendentals=0
        ),
        compiler_params=pltpu.CompilerParams(vmem_limit_bytes=VMEM_BYTES - INNER_ROOM),
        name="inner_advance",
    )(table, *bands)


def edge_kernel(staged, start_in, damp, table, low, high, *refs):
    heat, salt, u, v = bands_of(refs)
    refs = refs[4 * PARTS :]
    levels = staged.shape[1]
    width, extent = start_in.shape
    span = width + 2 * BASE
    flows, tracers = (u, v), (heat, salt)
    o_heat, o_salt, o_u, o_v, fields, o_sums = refs[:6]
    ocean, half, diag, even, odd, edge_out, acc, out_sems = refs[6:]
    masked = (even, odd)
    targets = (o_heat, o_salt, o_u, o_v)
    inside = pl.ds(PAD, width - 2 * PAD)
    results = []
    for q in range(4):
        copy = pltpu.make_async_copy(
            staged.at[q, :, inside], targets[q].at[:, inside], out_sems.at[8 + q]
        )
        copy.start()
        results.append(copy)
    wet8 = table[0:MARGIN]
    row = rows_in((MARGIN, extent))
    for block in range(BASE // MARGIN, (BASE + width) // MARGIN):
        ocean[block * MARGIN : (block + 1) * MARGIN] = wet8
    diag[BASE : BASE + width] = (
        0.5 * (table[0:1] * (6.0 + damp[...]) + (1.0 - table[0:1])) - 2.0
    )
    fields[1, BASE : BASE + width] = start_in[...]

    for side, message in ((0, low), (1, high)):
        wet_out = jnp.broadcast_to(message[5, MARGIN - 1 : MARGIN], (MARGIN, extent))
        outer = 0 if side == 0 else BASE + width
        for block in range(BASE // MARGIN):
            ocean[outer + block * MARGIN : outer + (block + 1) * MARGIN] = wet_out
        wet_row = wet_out[0:1]
        near = 2 * MARGIN if side == 0 else BASE + width
        far = MARGIN if side == 0 else BASE + width + MARGIN
        for at, damping in ((near, message[1]), (far, shift(message[2], 4, 0))):
            diag[at : at + MARGIN] = 0.5 * (
                wet_row * (6.0 + damping) + (1.0 - wet_row)
            ) - 2.0
        if side == 0:
            around = jnp.concatenate([wet_out, wet8, wet8], axis=0)
        else:
            around = jnp.concatenate([wet8, wet8, wet_out], axis=0)
        east_own = (around * shift(around, -1, 0))[:PAD]
        north_own = north_wetness(wet8)

        mine_at = slice(MARGIN, BASE) if side == 0 else slice(width - MARGIN, width + MARGIN)
        rim_at = slice(0, PAD) if side == 0 else slice(width - PAD, width)

        def level_step(k, sums, side=side, message=message, east_own=east_own,
                       north_own=north_own, mine_at=mine_at, rim_at=rim_at):
            weight = table[pl.ds(MARGIN + k, 1)]
            windows = []
            for slot, pair in ((4, tracers), (3, flows)):
                for q in range(2):
                    mine = pair[q][k, mine_at]
                    piece = jnp.broadcast_to(
                        message[slot, pl.ds(q * levels + k, 1)], (MARGIN, extent)
                    )
                    pieces = [piece, mine] if side == 0 else [mine, piece]
                    windows.append(jnp.concatenate(pieces, axis=0))
            east, north = face_speeds(windows[2], windows[3], east_own, north_own)
            fluxes = [east_flow(window, east) for window in windows]
            fresh = [
                advect(window, east, north, wet8, flux)
                for window, flux in zip(windows, fluxes)
            ]
            for q in range(4):
                old = staged[q, k, rim_at].astype(jnp.float32)
                if side == 0:
                    value = jnp.concatenate([fresh[q], old[MARGIN:]], axis=0)
                else:
                    value = jnp.concatenate([old[:MARGIN], fresh[q]], axis=0)
                edge_out[q, side, k] = value.astype(edge_out.dtype)
            face_at = slice(0, MARGIN) if side == 0 else slice(MARGIN, PAD)
            return (
                sums[0] + weight * fresh[2],
                sums[1] + weight * fresh[3],
                sums[2] + weight * fluxes[2][face_at],
                sums[3] + weight * fluxes[3][face_at],
            )

        zero = jnp.zeros((MARGIN, extent), jnp.float32)
        flow, cross, flow_face, cross_face = lax.fori_loop(
            0, levels, level_step, (zero, zero, zero, zero), unroll=2
        )
        given, farther = message[0], message[2]
        known = [message[5, i : i + 1] for i in range(5)]
        change = (-COURANT if side == 0 else COURANT) * wet_out
        flow_tip = known[0] + change * jnp.broadcast_to(flow_face[MARGIN - 1 :], wet_out.shape)
        cross_tip = known[1] + change * jnp.broadcast_to(cross_face[MARGIN - 1 :], wet_out.shape)
        if side == 0:
            flow_out = jnp.where(row == MARGIN - 2, known[3], known[2])
            flow_out = jnp.where(row == MARGIN - 1, flow_tip, flow_out)
            cross_out = jnp.where(row == MARGIN - 1, cross_tip, known[4])
            whole = divergence(
                jnp.concatenate([wet_out, wet8], axis=0),
                jnp.concatenate([flow_out, flow], axis=0),
                jnp.concatenate([cross_out, cross], axis=0),
            )
            fields[1, MARGIN : 2 * MARGIN] = farther
            fields[1, 2 * MARGIN : BASE] = jnp.where(
                row >= MARGIN - 2, whole[:MARGIN], given
            )
            fields[1, BASE : BASE + MARGIN] = jnp.where(
                row < 2, whole[MARGIN:], start_in[0:MARGIN]
            )
        else:
            flow_out = jnp.where(row == 1, known[2], known[3])
            flow_out = jnp.where(row == 0, flow_tip, flow_out)
            cross_out = jnp.where(row == 0, cross_tip, known[4])
            whole = divergence(
                jnp.concatenate([wet8, wet_out], axis=0),
                jnp.concatenate([flow, flow_out], axis=0),
                jnp.concatenate([cross, cross_out], axis=0),
            )
            top = BASE + width
            fields[1, top - MARGIN : top] = jnp.where(
                row >= MARGIN - 2, whole[:MARGIN], start_in[width - MARGIN : width]
            )
            fields[1, top : top + MARGIN] = jnp.where(row < 2, whole[MARGIN:], given)
            fields[1, top + MARGIN : top + PAD] = farther

    for q, target in enumerate(targets):
        for side in range(2):
            first = 0 if side == 0 else width - PAD
            copy = pltpu.make_async_copy(
                edge_out.at[q, side],
                target.at[:, pl.ds(first, PAD)],
                out_sems.at[2 * q + side],
            )
            copy.start()
            results.append(copy)

    strips = (width + 2 * PAD) // PAD
    none = jnp.zeros((MARGIN, 128), jnp.float32)

    def inner(a, b, total):
        product = a * b
        part = product[:MARGIN] + product[MARGIN:]
        pieces = [part[:, i : i + 128] for i in range(0, extent, 128)]
        while len(pieces) > 1:
            pieces = [x + y for x, y in zip(pieces[::2], pieces[1::2])]
        s, e = two_sum(total[0], pieces[0])
        return s, total[1] + e

    square = (none, none)
    for strip in range(strips):
        keep = slice(MARGIN + strip * PAD, BASE + strip * PAD)
        half[keep] = 0.5 * ocean[keep]
        masked[0][keep] = half[keep] * fields[1, keep]
        fields[0, keep] = jnp.zeros((PAD, extent), jnp.float32)
        if 0 < strip < strips - 1:
            value = fields[1, keep]
            square = inner(value, value, square)
    acc[0, 0:MARGIN] = square[0]
    acc[1, 0:MARGIN] = square[1]
    for slot in range(2 * STEPS + 1, acc.shape[1] // MARGIN):
        acc[0, slot * MARGIN : (slot + 1) * MARGIN] = none
        acc[1, slot * MARGIN : (slot + 1) * MARGIN] = none

    def basis_step(j, now, scale, pieces):
        mixed, square = (none, none), (none, none)
        for start, rows in pieces:
            around = slice(start - MARGIN, start + rows + MARGIN)
            keep = slice(start, start + rows)
            wide = masked[now][around]
            sides = (shift(wide, -1, 0) + shift(wide, 1, 0))[MARGIN : MARGIN + rows]
            column = wide[MARGIN : MARGIN + rows] + 0.5 * sides
            near = sides + (north_of(column) + south_of(column))
            centre = fields[j + 1, keep]
            following = diag[keep] * centre - ocean[keep] * near
            if scale is not None:
                following = scale * following
            following = following - fields[j, keep]
            fields[j + 2, keep] = following
            masked[1 - now][keep] = half[keep] * following
            if BASE <= start < BASE + width:
                mixed = inner(centre, following, mixed)
                square = inner(following, following, square)
        for place, value in ((2 * j + 1, mixed), (2 * j + 2, square)):
            at = pl.ds(pl.multiple_of(place * MARGIN, MARGIN), MARGIN)
            acc[0, at] = value[0]
            acc[1, at] = value[1]

    own = [(BASE + first, PAD) for first in range(0, width, PAD)]
    whole = [(MARGIN, PAD), *own, (BASE + width, PAD)]
    short = [(2 * MARGIN, MARGIN), *own, (BASE + width, MARGIN)]

    def step_pair(pieces, first):
        def run(index, carry):
            scale = jnp.where(index == 0, 0.5, 1.0) if first else None
            basis_step(2 * index, 0, scale, pieces)
            basis_step(2 * index + 1, 1, None, pieces)
            return carry

        return run

    wide_pairs = -(-(STEPS - MARGIN) // 2)
    lax.fori_loop(0, wide_pairs, step_pair(whole, True), 0)
    lax.fori_loop(wide_pairs, STEPS // 2, step_pair(short, False), 0, unroll=UNROLL)

    slots = acc.shape[1] // MARGIN
    pairs = [
        (acc[0, pl.ds(s, slots, stride=MARGIN)], acc[1, pl.ds(s, slots, stride=MARGIN)])
        for s in range(MARGIN)
    ]
    while len(pairs) > 1:
        pairs = [pair_add(x, y) for x, y in zip(pairs[::2], pairs[1::2])]
    total = pairs[0]
    step = 64
    while step:
        total = pair_add(total, (shift(total[0], step, 1), shift(total[1], step, 1)))
        step //= 2
    row = lax.broadcasted_iota(jnp.int32, (MARGIN, 128), 0)
    place = lax.broadcasted_iota(jnp.int32, (MARGIN, 128), 1)
    lined = []
    for part in total:
        merged = none
        for group in range(slots // MARGIN):
            merged = jnp.where(
                place // MARGIN == group, part[group * MARGIN : (group + 1) * MARGIN], merged
            )
        merged = jnp.where(place % MARGIN == row, merged, 0.0)
        for s in (4, 2, 1):
            merged = merged + shift(merged, s, 0)
        lined.append(merged)
    packed = jnp.where(place < 64, lined[0], shift(lined[1], 64, 1))
    for first in range(0, o_sums.shape[0], MARGIN):
        o_sums[first : first + MARGIN] = packed
    for copy in results:
        copy.wait()


def edge_advance(staged, start, damp, table, low, high, bands, members):
    levels, width, extent = staged.shape[1:]
    span = width + 2 * BASE
    slots = 32
    anywhere = pl.BlockSpec(memory_space=pl.ANY)
    vmem = pl.BlockSpec(memory_space=pltpu.VMEM)
    tracer = jax.ShapeDtypeStruct((levels, width, extent), staged.dtype)
    f32 = jnp.float32
    return pl.pallas_call(
        edge_kernel,
        out_shape=[tracer] * 4
        + [
            jax.ShapeDtypeStruct((STEPS + 2, span, extent), f32),
            jax.ShapeDtypeStruct((members, 128), f32),
        ],
        in_specs=[vmem] * (6 + len(bands)),
        out_specs=[anywhere] * 4 + [vmem] * 2,
        scratch_shapes=[
            pltpu.VMEM((span, extent), f32),
            pltpu.VMEM((span, extent), f32),
            pltpu.VMEM((span, extent), f32),
            pltpu.VMEM((span, extent), f32),
            pltpu.VMEM((span, extent), f32),
            pltpu.VMEM((4, 2, levels, PAD, extent), jnp.bfloat16),
            pltpu.VMEM((2, slots * MARGIN, 128), f32),
            pltpu.SemaphoreType.DMA((12,)),
        ],
        cost_estimate=pl.CostEstimate(
            flops=10000000000, bytes_accessed=5000000, transcendentals=0
        ),
        compiler_params=pltpu.CompilerParams(vmem_limit_bytes=VMEM_BYTES - EDGE_ROOM),
        name="edge_advance",
    )(staged, start, damp, table, low, high, *bands)


def combine_kernel(sums, fields, height, resid):
    members = sums.shape[0]
    lane = lax.broadcasted_iota(jnp.int32, (MARGIN, 128), 1)
    nothing = jnp.zeros((MARGIN, 128), jnp.float32)
    pieces = [(sums[i : i + MARGIN], nothing) for i in range(0, members, MARGIN)]
    while len(pieces) > 1:
        merged = []
        for x, y in zip(pieces[::2], pieces[1::2]):
            s, e = two_sum(x[0], y[0])
            merged.append((s, (x[1] + y[1]) + e))
        if len(pieces) % 2:
            merged.append(pieces[-1])
        pieces = merged
    total, error = pieces[0]
    for step in (4, 2, 1):
        total, e = two_sum(total, shift(total, step, 0))
        error = (error + shift(error, step, 0)) + e
    dots = fast_two_sum(total, shift(total, 64, 1) + error)

    def at(x, k):
        return jnp.broadcast_to(x[:, k : k + 1], x.shape)

    odd = lane % 2 == 1
    anchor = tuple(jnp.where(odd, at(x, 1), at(x, 0)) for x in dots)
    moments = pair_add((2.0 * dots[0], 2.0 * dots[1]), (-anchor[0], -anchor[1]))
    inside = lane <= 2 * STEPS
    moments = tuple(jnp.where(inside, x, 0.0) for x in moments)

    def ahead(x):
        return shift(x, -1, 1)

    def behind(x):
        return shift(x, 1, 1)

    def image_of_products(x):
        after = tuple(ahead(c) for c in x)
        before = tuple(jnp.where(lane == 0, a, behind(c)) for a, c in zip(after, x))
        out = pair_add(pair_add(after, before), (2.0 * x[0], 2.0 * x[1]))
        return 0.25 * out[0], 0.25 * out[1]

    def image_of_coefficients(x):
        after = tuple(ahead(c) for c in x)
        before = tuple(
            jnp.where(lane == 0, 0.0, jnp.where(lane == 1, 2.0 * behind(c), behind(c))) for c in x
        )
        out = pair_add(pair_add(after, before), (2.0 * x[0], 2.0 * x[1]))
        return 0.25 * out[0], 0.25 * out[1]

    unit = jnp.where(lane == 0, 1.0, 0.0).astype(jnp.float32)
    zero = jnp.zeros_like(unit)
    r_products, p_products = moments, moments
    c_r, c_p, c_x = (unit, zero), (unit, zero), zero

    def pick(x, k):
        return at(x[0], k), at(x[1], k)

    def quarter_sum(before, here, after):
        out = pair_add(pair_add(after, before), (2.0 * here[0], 2.0 * here[1]))
        return 0.25 * out[0], 0.25 * out[1]

    norm = pick(r_products, 0)
    for k in range(STEPS):
        near = [pick(p_products, abs(k - 1)), pick(p_products, k)]
        near += [pick(p_products, k + 1), pick(p_products, k + 2)]
        energy = quarter_sum(near[0], near[1], near[2])
        alpha = norm[0] / energy[0]
        c_x = c_x + alpha * c_p[0]
        c_r = pair_add(c_r, pair_scale(image_of_coefficients(c_p), -alpha))
        if k + 1 < STEPS:
            change = pair_scale(image_of_products(p_products), -alpha)
            following = pair_scale(quarter_sum(near[1], near[2], near[3]), -alpha)
            following = pair_add(pick(r_products, k + 1), following)
            r_products = pair_add(r_products, change)
            lead = 0.5 if k == 0 else 0.25
            beta = (-lead * alpha) * following[0] / norm[0]
            p_products = pair_add(r_products, pair_scale(p_products, beta))
            c_p = pair_add(c_r, pair_scale(c_p, beta))
            norm = following

    width = height.shape[0]
    weights_x = [at(c_x, j) for j in range(STEPS + 1)]
    weights_r = [at(c_r[0], j) for j in range(STEPS + 1)]
    for first in range(0, width, MARGIN):
        keep = slice(first, first + MARGIN)
        wide = slice(BASE + first, BASE + first + MARGIN)
        for left in range(0, height.shape[1], 128):
            cols = slice(left, left + 128)
            value = fields[1, wide, cols]
            h, r = weights_x[0] * value, weights_r[0] * value
            for j in range(1, STEPS + 1):
                value = fields[j + 1, wide, cols]
                h, r = h + weights_x[j] * value, r + weights_r[j] * value
            height[keep, cols] = h
            resid[keep, cols] = r


def combine(sums, fields, width):
    plane = jax.ShapeDtypeStruct((width, fields.shape[2]), jnp.float32)
    vmem = pl.BlockSpec(memory_space=pltpu.VMEM)
    return pl.pallas_call(
        combine_kernel,
        out_shape=[plane, plane],
        in_specs=[vmem, vmem],
        out_specs=[vmem, vmem],
        compiler_params=pltpu.CompilerParams(vmem_limit_bytes=8 * 1024 * 1024),
        name="combine",
    )(sums, fields)


def on_device(
    heat_anomaly,
    saltiness_anomaly,
    first_axis_flow,
    second_axis_flow,
    layer_spacing,
    diagonal_shift,
    water_tile_flags,
):
    members = lax.axis_size("blk")
    bands = fetch(heat_anomaly, saltiness_anomaly, first_axis_flow, second_axis_flow)
    to_next, to_last, table = pack(water_tile_flags, layer_spacing[None], diagonal_shift, bands)
    forward = [(i, (i + 1) % members) for i in range(members)]
    backward = [(target, source) for source, target in forward]
    low = lax.ppermute(to_next, "blk", forward)
    high = lax.ppermute(to_last, "blk", backward)
    staged, start = inner_advance(table, bands)
    *tracers, basis, sums = edge_advance(
        staged, start, diagonal_shift, table, low, high, bands, members
    )
    gathered = lax.all_to_all(sums, "blk", 0, 0, tiled=True)
    height, resid = combine(gathered, basis, diagonal_shift.shape[0])
    return (*tracers, height, resid)


def solution(mesh):
    columns = P("member", "blk", None)
    return jax.shard_map(
        on_device,
        mesh=mesh,
        in_specs=(columns, columns, columns, columns, P(), P("blk", None), P("blk", None)),
        out_specs=(
            columns,
            columns,
            columns,
            columns,
            P(("member", "blk"), None),
            P(("member", "blk"), None),
        ),
        check_vma=False,
    )
```

```python
import functools

import jax
import jax.numpy as jnp
from jax import lax
from jax.experimental import pallas as pl
from jax.experimental.pallas import tpu as pltpu
from jax.sharding import PartitionSpec as P

SSTEP = 4
CG_BLOCKS = 3
STEPS = SSTEP * CG_BLOCKS
COURANT = 0.2
PAD = 16
MARGIN = 8
BASE = PAD + MARGIN
KIB = 1024
PARTS = 2
UNROLL = 2
VMEM_BYTES = 65472 * KIB
FETCH_ROOM = 14480 * KIB
PACK_ROOM = 32000 * KIB
INNER_ROOM = 32000 * KIB
EDGE_ROOM = 45 * KIB * KIB


def shift(value, amount, axis):
    return pltpu.roll(value, amount % value.shape[axis], axis)


def two_sum(a, b):
    s = a + b
    t = s - a
    return s, (a - (s - t)) + (b - t)


def fast_two_sum(a, b):
    s = a + b
    return s, b - (s - a)


def split(a):
    c = 4097.0 * a
    hi = c - (c - a)
    return hi, a - hi


def two_prod(a, b):
    p = a * b
    ah, al = split(a)
    bh, bl = split(b)
    return p, ((ah * bh - p) + ah * bl + al * bh) + al * bl


def pair_add(a, b):
    s, e = two_sum(a[0], b[0])
    return fast_two_sum(s, e + (a[1] + b[1]))


def pair_scale(a, c):
    p, e = two_prod(a[0], c)
    return p, e + a[1] * c


def upwind(speed, behind, ahead):
    return speed * jnp.where(speed > 0.0, behind, ahead)


def face_speeds(u, v, east_wet, north_wet):
    east = 0.5 * (u + shift(u, -1, 0))[:-MARGIN] * east_wet
    centre = v[MARGIN:-MARGIN]
    north = 0.5 * (centre + shift(centre, -1, 1)) * north_wet
    return east, north


def east_flow(q, east):
    return upwind(east, q[:-MARGIN], shift(q, -1, 0)[:-MARGIN])


def advect(q, east, north, wet, east_flux=None):
    if east_flux is None:
        east_flux = east_flow(q, east)
    centre = q[MARGIN:-MARGIN]
    north_flux = upwind(north, centre, shift(centre, -1, 1))
    spread = (east_flux - shift(east_flux, 1, 0))[MARGIN:] + (
        north_flux - shift(north_flux, 1, 1)
    )
    return wet * (centre - COURANT * spread)


def lanes(shape):
    return lax.broadcasted_iota(jnp.int32, shape, 1)


def rows_in(shape):
    return lax.broadcasted_iota(jnp.int32, shape, 0)


def north_of(x):
    return jnp.where(lanes(x.shape) == x.shape[1] - 1, 0.0, shift(x, -1, 1))


def south_of(x):
    return jnp.where(lanes(x.shape) == 0, 0.0, shift(x, 1, 1))


def north_wetness(wet):
    return wet * north_of(wet)


def divergence(wet, flow, cross):
    east_part = shift(flow, -1, 0) - shift(flow, 1, 0)
    return wet * (0.5 * (east_part + (north_of(cross) - south_of(cross))))


class Band:
    def __init__(self, parts):
        self.parts = parts

    def __getitem__(self, at):
        return jnp.concatenate([part[at] for part in self.parts], axis=-1)


def bands_of(refs):
    return [Band(refs[q * PARTS : (q + 1) * PARTS]) for q in range(4)]


def fetch_kernel(heat, salt, u, v, *refs):
    width, extent = u.shape[1:]
    parts, sems = refs[: 4 * PARTS], refs[4 * PARTS]
    share = extent // PARTS
    copies = []
    for q, source in enumerate((heat, salt, u, v)):
        for part in range(PARTS):
            copy = pltpu.make_async_copy(
                source.at[:, :, pl.ds(part * share, share)],
                parts[q * PARTS + part].at[:, pl.ds(MARGIN, width)],
                sems.at[len(copies)],
            )
            copy.start()
            copies.append(copy)
    for copy in copies:
        copy.wait()


def fetch(heat, salt, u, v):
    levels, width, extent = u.shape
    band = jax.ShapeDtypeStruct((levels, width + PAD, extent // PARTS), u.dtype)
    return pl.pallas_call(
        fetch_kernel,
        out_shape=[band] * (4 * PARTS),
        in_specs=[pl.BlockSpec(memory_space=pl.ANY)] * 4,
        out_specs=[pl.BlockSpec(memory_space=pltpu.VMEM)] * (4 * PARTS),
        scratch_shapes=[pltpu.SemaphoreType.DMA((4 * PARTS,))],
        cost_estimate=pl.CostEstimate(
            flops=10000000000, bytes_accessed=5000000, transcendentals=0
        ),
        compiler_params=pltpu.CompilerParams(vmem_limit_bytes=VMEM_BYTES - FETCH_ROOM),
        name="fetch",
    )(heat, salt, u, v)


def pack_kernel(flags, spacing, damp, *refs):
    heat, salt, u, v = bands_of(refs)
    o_low, o_high, o_table = refs[4 * PARTS :]
    levels = spacing.shape[1]
    width, extent = damp.shape
    tiles = flags.shape[1]
    flows, tracers = (u, v), (heat, salt)
    messages = (o_high, o_low)
    lane = lanes((MARGIN, extent))
    wet = jnp.zeros((MARGIN, extent), jnp.float32)
    flag = flags[...].astype(jnp.float32)
    for tile in range(tiles):
        inside = (lane >= tile * (extent // tiles)) & (lane < (tile + 1) * (extent // tiles))
        wet = jnp.where(inside, flag[:, tile : tile + 1], wet)
    o_table[0:MARGIN] = wet
    wet_row = wet[0:1]
    east_wet = wet_row * wet_row
    north_wet = north_wetness(wet)[0:1]
    row = rows_in((MARGIN, extent))
    thick = [spacing[:, k : k + 1] for k in range(levels)]
    total = thick[0]
    for k in range(1, levels):
        total = total + thick[k]
    weights = jnp.zeros((MARGIN, extent), jnp.float32)
    for k in range(levels):
        weights = jnp.where(row == k, thick[k], weights)
    o_table[MARGIN:PAD] = weights / total
    for end in range(2):
        message = messages[end]
        rows = slice(0, 2 * PAD) if end == 0 else slice(width - PAD, width + PAD)

        face = MARGIN - 1 if end == 0 else BASE - 1
        closed = rows_in((BASE, extent)) == face

        def level_step(k, sums, rows=rows, closed=closed):
            weight = o_table[pl.ds(MARGIN + k, 1)]
            qu = u[k, rows]
            qv = v[k, rows]
            east, north = face_speeds(qu, qv, east_wet, north_wet)
            fu = jnp.where(closed, 0.0, east_flow(qu, east))
            fv = jnp.where(closed, 0.0, east_flow(qv, east))
            au = advect(qu, east, north, wet_row, fu)
            av = advect(qv, east, north, wet_row, fv)
            return sums[0] + weight * au, sums[1] + weight * av

        zero = jnp.zeros((PAD, extent), jnp.float32)
        flow, cross = lax.fori_loop(0, levels, level_step, (zero, zero), unroll=4)
        start = divergence(wet_row, flow, cross)
        first = 0 if end == 0 else width - PAD
        damping = damp[first : first + PAD]
        near = slice(0, MARGIN) if end == 0 else slice(MARGIN, PAD)
        far = slice(MARGIN, PAD) if end == 0 else slice(0, MARGIN)
        message[0] = start[near]
        message[1] = damping[near]
        natural = row < 4 if end == 0 else row >= 4
        message[2] = jnp.where(natural, start[far], shift(damping[far], 4, 0))
        tip = slice(MARGIN, PAD) if end == 0 else slice(width, width + MARGIN)
        for slot, pair in ((3, flows), (4, tracers)):
            merged = jnp.zeros((MARGIN, extent), jnp.float32)
            for q in range(2):
                for k in range(levels):
                    place = q * levels + k
                    piece = shift(pair[q][k, tip], place if end == 0 else place + 1, 0)
                    merged = jnp.where(row == place, piece, merged)
            message[slot] = merged
        flow, cross = flow[near], cross[near]
        turns = (0, 1, 1, 3) if end == 0 else (1, 2, 5, 6)
        tail = jnp.where(row == 4, shift(cross, turns[3], 0), wet)
        tail = jnp.where((row == 2) | (row == 3), shift(flow, turns[2], 0), tail)
        tail = jnp.where(row == 1, shift(cross, turns[1], 0), tail)
        message[5] = jnp.where(row == 0, shift(flow, turns[0], 0) if end else flow, tail)


def pack(flags, spacing, damp, bands):
    extent = damp.shape[1]
    f32 = jnp.float32
    message = jax.ShapeDtypeStruct((6, MARGIN, extent), f32)
    vmem = pl.BlockSpec(memory_space=pltpu.VMEM)
    return pl.pallas_call(
        pack_kernel,
        out_shape=[message, message, jax.ShapeDtypeStruct((PAD, extent), f32)],
        in_specs=[vmem] * (3 + len(bands)),
        out_specs=[vmem] * 3,
        compiler_params=pltpu.CompilerParams(vmem_limit_bytes=VMEM_BYTES - PACK_ROOM),
        name="pack",
    )(flags, spacing, damp, *bands)


def inner_kernel(table, *refs):
    heat, salt, u, v = bands_of(refs)
    staged, o_start, tu, tv = refs[4 * PARTS :]
    levels = staged.shape[1]
    width, extent = o_start.shape
    wet = table[0:1]
    north_wet = north_wetness(table[0:MARGIN])[0:1]
    east_wet = wet * wet
    tu[...] = jnp.zeros_like(tu)
    tv[...] = jnp.zeros_like(tv)

    def level_step(k, carry):
        weight = table[pl.ds(MARGIN + k, 1)]

        def strip(index, carry):
            local = pl.ds(pl.multiple_of(index * PAD, PAD), PAD)
            later = pl.ds(pl.multiple_of(index * PAD + MARGIN, MARGIN), PAD)
            rows = pl.ds(pl.multiple_of(index * PAD, MARGIN), 2 * PAD)
            qu = u[k, rows]
            qv = v[k, rows]
            east, north = face_speeds(qu, qv, east_wet, north_wet)
            au = advect(qu, east, north, wet)
            av = advect(qv, east, north, wet)
            staged[2, k, local] = au.astype(staged.dtype)
            staged[3, k, local] = av.astype(staged.dtype)
            tu[later] += weight * au
            tv[later] += weight * av
            staged[0, k, local] = advect(heat[k, rows], east, north, wet).astype(staged.dtype)
            staged[1, k, local] = advect(salt[k, rows], east, north, wet).astype(staged.dtype)
            return carry

        lax.fori_loop(0, width // PAD, strip, 0, unroll=2)
        return carry

    lax.fori_loop(0, levels, level_step, 0)
    for first in range(0, width, PAD):
        keep = slice(first, first + PAD)
        flow = tu[first : first + 2 * PAD]
        cross = tv[first + MARGIN : first + BASE]
        east_part = (shift(flow, -1, 0) - shift(flow, 1, 0))[MARGIN:BASE]
        o_start[keep] = wet * (0.5 * (east_part + (north_of(cross) - south_of(cross))))


def inner_advance(table, bands):
    levels, padded, share = bands[0].shape
    width, extent = padded - PAD, share * PARTS
    f32 = jnp.float32
    vmem = pl.BlockSpec(memory_space=pltpu.VMEM)
    return pl.pallas_call(
        inner_kernel,
        out_shape=[
            jax.ShapeDtypeStruct((4, levels, width, extent), jnp.bfloat16),
            jax.ShapeDtypeStruct((width, extent), f32),
        ],
        in_specs=[vmem] * (1 + len(bands)),
        out_specs=[vmem] * 2,
        scratch_shapes=[
            pltpu.VMEM((width + PAD, extent), f32),
            pltpu.VMEM((width + PAD, extent), f32),
        ],
        cost_estimate=pl.CostEstimate(
            flops=10000000000, bytes_accessed=5000000, transcendentals=0
        ),
        compiler_params=pltpu.CompilerParams(vmem_limit_bytes=VMEM_BYTES - INNER_ROOM),
        name="inner_advance",
    )(table, *bands)


def edge_kernel(staged, start_in, damp, table, low, high, *refs):
    heat, salt, u, v = bands_of(refs)
    refs = refs[4 * PARTS :]
    levels = staged.shape[1]
    width, extent = start_in.shape
    span = width + 2 * BASE
    flows, tracers = (u, v), (heat, salt)
    o_heat, o_salt, o_u, o_v, fields, o_sums = refs[:6]
    ocean, half, diag, even, odd, edge_out, acc, out_sems = refs[6:]
    masked = (even, odd)
    targets = (o_heat, o_salt, o_u, o_v)
    inside = pl.ds(PAD, width - 2 * PAD)
    results = []
    for q in range(4):
        copy = pltpu.make_async_copy(
            staged.at[q, :, inside], targets[q].at[:, inside], out_sems.at[8 + q]
        )
        copy.start()
        results.append(copy)
    wet8 = table[0:MARGIN]
    row = rows_in((MARGIN, extent))
    for block in range(BASE // MARGIN, (BASE + width) // MARGIN):
        ocean[block * MARGIN : (block + 1) * MARGIN] = wet8
    diag[BASE : BASE + width] = (
        0.5 * (table[0:1] * (6.0 + damp[...]) + (1.0 - table[0:1])) - 2.0
    )
    fields[1, BASE : BASE + width] = start_in[...]

    for side, message in ((0, low), (1, high)):
        wet_out = jnp.broadcast_to(message[5, MARGIN - 1 : MARGIN], (MARGIN, extent))
        outer = 0 if side == 0 else BASE + width
        for block in range(BASE // MARGIN):
            ocean[outer + block * MARGIN : outer + (block + 1) * MARGIN] = wet_out
        wet_row = wet_out[0:1]
        near = 2 * MARGIN if side == 0 else BASE + width
        far = MARGIN if side == 0 else BASE + width + MARGIN
        for at, damping in ((near, message[1]), (far, shift(message[2], 4, 0))):
            diag[at : at + MARGIN] = 0.5 * (
                wet_row * (6.0 + damping) + (1.0 - wet_row)
            ) - 2.0
        if side == 0:
            around = jnp.concatenate([wet_out, wet8, wet8], axis=0)
        else:
            around = jnp.concatenate([wet8, wet8, wet_out], axis=0)
        east_own = (around * shift(around, -1, 0))[:PAD]
        north_own = north_wetness(wet8)

        mine_at = slice(MARGIN, BASE) if side == 0 else slice(width - MARGIN, width + MARGIN)
        rim_at = slice(0, PAD) if side == 0 else slice(width - PAD, width)

        def level_step(k, sums, side=side, message=message, east_own=east_own,
                       north_own=north_own, mine_at=mine_at, rim_at=rim_at):
            weight = table[pl.ds(MARGIN + k, 1)]
            windows = []
            for slot, pair in ((4, tracers), (3, flows)):
                for q in range(2):
                    mine = pair[q][k, mine_at]
                    piece = jnp.broadcast_to(
                        message[slot, pl.ds(q * levels + k, 1)], (MARGIN, extent)
                    )
                    pieces = [piece, mine] if side == 0 else [mine, piece]
                    windows.append(jnp.concatenate(pieces, axis=0))
            east, north = face_speeds(windows[2], windows[3], east_own, north_own)
            fluxes = [east_flow(window, east) for window in windows]
            fresh = [
                advect(window, east, north, wet8, flux)
                for window, flux in zip(windows, fluxes)
            ]
            for q in range(4):
                old = staged[q, k, rim_at].astype(jnp.float32)
                if side == 0:
                    value = jnp.concatenate([fresh[q], old[MARGIN:]], axis=0)
                else:
                    value = jnp.concatenate([old[:MARGIN], fresh[q]], axis=0)
                edge_out[q, side, k] = value.astype(edge_out.dtype)
            face_at = slice(0, MARGIN) if side == 0 else slice(MARGIN, PAD)
            return (
                sums[0] + weight * fresh[2],
                sums[1] + weight * fresh[3],
                sums[2] + weight * fluxes[2][face_at],
                sums[3] + weight * fluxes[3][face_at],
            )

        zero = jnp.zeros((MARGIN, extent), jnp.float32)
        flow, cross, flow_face, cross_face = lax.fori_loop(
            0, levels, level_step, (zero, zero, zero, zero), unroll=2
        )
        given, farther = message[0], message[2]
        known = [message[5, i : i + 1] for i in range(5)]
        change = (-COURANT if side == 0 else COURANT) * wet_out
        flow_tip = known[0] + change * jnp.broadcast_to(flow_face[MARGIN - 1 :], wet_out.shape)
        cross_tip = known[1] + change * jnp.broadcast_to(cross_face[MARGIN - 1 :], wet_out.shape)
        if side == 0:
            flow_out = jnp.where(row == MARGIN - 2, known[3], known[2])
            flow_out = jnp.where(row == MARGIN - 1, flow_tip, flow_out)
            cross_out = jnp.where(row == MARGIN - 1, cross_tip, known[4])
            whole = divergence(
                jnp.concatenate([wet_out, wet8], axis=0),
                jnp.concatenate([flow_out, flow], axis=0),
                jnp.concatenate([cross_out, cross], axis=0),
            )
            fields[1, MARGIN : 2 * MARGIN] = farther
            fields[1, 2 * MARGIN : BASE] = jnp.where(
                row >= MARGIN - 2, whole[:MARGIN], given
            )
            fields[1, BASE : BASE + MARGIN] = jnp.where(
                row < 2, whole[MARGIN:], start_in[0:MARGIN]
            )
        else:
            flow_out = jnp.where(row == 1, known[2], known[3])
            flow_out = jnp.where(row == 0, flow_tip, flow_out)
            cross_out = jnp.where(row == 0, cross_tip, known[4])
            whole = divergence(
                jnp.concatenate([wet8, wet_out], axis=0),
                jnp.concatenate([flow, flow_out], axis=0),
                jnp.concatenate([cross, cross_out], axis=0),
            )
            top = BASE + width
            fields[1, top - MARGIN : top] = jnp.where(
                row >= MARGIN - 2, whole[:MARGIN], start_in[width - MARGIN : width]
            )
            fields[1, top : top + MARGIN] = jnp.where(row < 2, whole[MARGIN:], given)
            fields[1, top + MARGIN : top + PAD] = farther

    for q, target in enumerate(targets):
        for side in range(2):
            first = 0 if side == 0 else width - PAD
            copy = pltpu.make_async_copy(
                edge_out.at[q, side],
                target.at[:, pl.ds(first, PAD)],
                out_sems.at[2 * q + side],
            )
            copy.start()
            results.append(copy)

    strips = (width + 2 * PAD) // PAD
    none = jnp.zeros((MARGIN, 128), jnp.float32)

    def inner(a, b, total):
        product = a * b
        part = product[:MARGIN] + product[MARGIN:]
        pieces = [part[:, i : i + 128] for i in range(0, extent, 128)]
        while len(pieces) > 1:
            pieces = [x + y for x, y in zip(pieces[::2], pieces[1::2])]
        s, e = two_sum(total[0], pieces[0])
        return s, total[1] + e

    square = (none, none)
    for strip in range(strips):
        keep = slice(MARGIN + strip * PAD, BASE + strip * PAD)
        half[keep] = 0.5 * ocean[keep]
        masked[0][keep] = half[keep] * fields[1, keep]
        fields[0, keep] = jnp.zeros((PAD, extent), jnp.float32)
        if 0 < strip < strips - 1:
            value = fields[1, keep]
            square = inner(value, value, square)
    acc[0, 0:MARGIN] = square[0]
    acc[1, 0:MARGIN] = square[1]
    for slot in range(2 * STEPS + 1, acc.shape[1] // MARGIN):
        acc[0, slot * MARGIN : (slot + 1) * MARGIN] = none
        acc[1, slot * MARGIN : (slot + 1) * MARGIN] = none

    def basis_step(j, now, scale, pieces):
        mixed, square = (none, none), (none, none)
        for start, rows in pieces:
            around = slice(start - MARGIN, start + rows + MARGIN)
            keep = slice(start, start + rows)
            wide = masked[now][around]
            sides = (shift(wide, -1, 0) + shift(wide, 1, 0))[MARGIN : MARGIN + rows]
            column = wide[MARGIN : MARGIN + rows] + 0.5 * sides
            near = sides + (north_of(column) + south_of(column))
            centre = fields[j + 1, keep]
            following = diag[keep] * centre - ocean[keep] * near
            if scale is not None:
                following = scale * following
            following = following - fields[j, keep]
            fields[j + 2, keep] = following
            masked[1 - now][keep] = half[keep] * following
            if BASE <= start < BASE + width:
                mixed = inner(centre, following, mixed)
                square = inner(following, following, square)
        for place, value in ((2 * j + 1, mixed), (2 * j + 2, square)):
            at = pl.ds(pl.multiple_of(place * MARGIN, MARGIN), MARGIN)
            acc[0, at] = value[0]
            acc[1, at] = value[1]

    own = [(BASE + first, PAD) for first in range(0, width, PAD)]
    whole = [(MARGIN, PAD), *own, (BASE + width, PAD)]
    short = [(2 * MARGIN, MARGIN), *own, (BASE + width, MARGIN)]

    def step_pair(pieces, first):
        def run(index, carry):
            scale = jnp.where(index == 0, 0.5, 1.0) if first else None
            basis_step(2 * index, 0, scale, pieces)
            basis_step(2 * index + 1, 1, None, pieces)
            return carry

        return run

    wide_pairs = -(-(STEPS - MARGIN) // 2)
    lax.fori_loop(0, wide_pairs, step_pair(whole, True), 0, unroll=UNROLL)
    lax.fori_loop(wide_pairs, STEPS // 2, step_pair(short, False), 0, unroll=UNROLL)

    slots = acc.shape[1] // MARGIN
    pairs = [
        (acc[0, pl.ds(s, slots, stride=MARGIN)], acc[1, pl.ds(s, slots, stride=MARGIN)])
        for s in range(MARGIN)
    ]
    while len(pairs) > 1:
        pairs = [pair_add(x, y) for x, y in zip(pairs[::2], pairs[1::2])]
    total = pairs[0]
    step = 64
    while step:
        total = pair_add(total, (shift(total[0], step, 1), shift(total[1], step, 1)))
        step //= 2
    row = lax.broadcasted_iota(jnp.int32, (MARGIN, 128), 0)
    place = lax.broadcasted_iota(jnp.int32, (MARGIN, 128), 1)
    lined = []
    for part in total:
        merged = none
        for group in range(slots // MARGIN):
            merged = jnp.where(
                place // MARGIN == group, part[group * MARGIN : (group + 1) * MARGIN], merged
            )
        merged = jnp.where(place % MARGIN == row, merged, 0.0)
        for s in (4, 2, 1):
            merged = merged + shift(merged, s, 0)
        lined.append(merged)
    packed = jnp.where(place < 64, lined[0], shift(lined[1], 64, 1))
    for first in range(0, o_sums.shape[0], MARGIN):
        o_sums[first : first + MARGIN] = packed
    for copy in results:
        copy.wait()


def edge_advance(staged, start, damp, table, low, high, bands, members):
    levels, width, extent = staged.shape[1:]
    span = width + 2 * BASE
    slots = 32
    anywhere = pl.BlockSpec(memory_space=pl.ANY)
    vmem = pl.BlockSpec(memory_space=pltpu.VMEM)
    tracer = jax.ShapeDtypeStruct((levels, width, extent), staged.dtype)
    f32 = jnp.float32
    return pl.pallas_call(
        edge_kernel,
        out_shape=[tracer] * 4
        + [
            jax.ShapeDtypeStruct((STEPS + 2, span, extent), f32),
            jax.ShapeDtypeStruct((members, 128), f32),
        ],
        in_specs=[vmem] * (6 + len(bands)),
        out_specs=[anywhere] * 4 + [vmem] * 2,
        scratch_shapes=[
            pltpu.VMEM((span, extent), f32),
            pltpu.VMEM((span, extent), f32),
            pltpu.VMEM((span, extent), f32),
            pltpu.VMEM((span, extent), f32),
            pltpu.VMEM((span, extent), f32),
            pltpu.VMEM((4, 2, levels, PAD, extent), jnp.bfloat16),
            pltpu.VMEM((2, slots * MARGIN, 128), f32),
            pltpu.SemaphoreType.DMA((12,)),
        ],
        cost_estimate=pl.CostEstimate(
            flops=10000000000, bytes_accessed=5000000, transcendentals=0
        ),
        compiler_params=pltpu.CompilerParams(vmem_limit_bytes=VMEM_BYTES - EDGE_ROOM),
        name="edge_advance",
    )(staged, start, damp, table, low, high, *bands)


def combine_kernel(sums, fields, height, resid):
    members = sums.shape[0]
    lane = lax.broadcasted_iota(jnp.int32, (MARGIN, 128), 1)
    nothing = jnp.zeros((MARGIN, 128), jnp.float32)
    pieces = [(sums[i : i + MARGIN], nothing) for i in range(0, members, MARGIN)]
    while len(pieces) > 1:
        merged = []
        for x, y in zip(pieces[::2], pieces[1::2]):
            s, e = two_sum(x[0], y[0])
            merged.append((s, (x[1] + y[1]) + e))
        if len(pieces) % 2:
            merged.append(pieces[-1])
        pieces = merged
    total, error = pieces[0]
    for step in (4, 2, 1):
        total, e = two_sum(total, shift(total, step, 0))
        error = (error + shift(error, step, 0)) + e
    dots = fast_two_sum(total, shift(total, 64, 1) + error)

    def at(x, k):
        return jnp.broadcast_to(x[:, k : k + 1], x.shape)

    odd = lane % 2 == 1
    anchor = tuple(jnp.where(odd, at(x, 1), at(x, 0)) for x in dots)
    moments = pair_add((2.0 * dots[0], 2.0 * dots[1]), (-anchor[0], -anchor[1]))
    inside = lane <= 2 * STEPS
    moments = tuple(jnp.where(inside, x, 0.0) for x in moments)

    def ahead(x):
        return shift(x, -1, 1)

    def behind(x):
        return shift(x, 1, 1)

    def image_of_products(x):
        after = tuple(ahead(c) for c in x)
        before = tuple(jnp.where(lane == 0, a, behind(c)) for a, c in zip(after, x))
        out = pair_add(pair_add(after, before), (2.0 * x[0], 2.0 * x[1]))
        return 0.25 * out[0], 0.25 * out[1]

    def image_of_coefficients(x):
        after = tuple(ahead(c) for c in x)
        before = tuple(
            jnp.where(lane == 0, 0.0, jnp.where(lane == 1, 2.0 * behind(c), behind(c))) for c in x
        )
        out = pair_add(pair_add(after, before), (2.0 * x[0], 2.0 * x[1]))
        return 0.25 * out[0], 0.25 * out[1]

    unit = jnp.where(lane == 0, 1.0, 0.0).astype(jnp.float32)
    zero = jnp.zeros_like(unit)
    r_products, p_products = moments, moments
    c_r, c_p, c_x = (unit, zero), (unit, zero), zero

    def pick(x, k):
        return at(x[0], k), at(x[1], k)

    def quarter_sum(before, here, after):
        out = pair_add(pair_add(after, before), (2.0 * here[0], 2.0 * here[1]))
        return 0.25 * out[0], 0.25 * out[1]

    norm = pick(r_products, 0)
    for k in range(STEPS):
        near = [pick(p_products, abs(k - 1)), pick(p_products, k)]
        near += [pick(p_products, k + 1), pick(p_products, k + 2)]
        energy = quarter_sum(near[0], near[1], near[2])
        alpha = norm[0] / energy[0]
        c_x = c_x + alpha * c_p[0]
        c_r = pair_add(c_r, pair_scale(image_of_coefficients(c_p), -alpha))
        if k + 1 < STEPS:
            change = pair_scale(image_of_products(p_products), -alpha)
            following = pair_scale(quarter_sum(near[1], near[2], near[3]), -alpha)
            following = pair_add(pick(r_products, k + 1), following)
            r_products = pair_add(r_products, change)
            lead = 0.5 if k == 0 else 0.25
            beta = (-lead * alpha) * following[0] / norm[0]
            p_products = pair_add(r_products, pair_scale(p_products, beta))
            c_p = pair_add(c_r, pair_scale(c_p, beta))
            norm = following

    width = height.shape[0]
    weights_x = [at(c_x, j) for j in range(STEPS + 1)]
    weights_r = [at(c_r[0], j) for j in range(STEPS + 1)]
    for first in range(0, width, MARGIN):
        keep = slice(first, first + MARGIN)
        wide = slice(BASE + first, BASE + first + MARGIN)
        for left in range(0, height.shape[1], 128):
            cols = slice(left, left + 128)
            value = fields[1, wide, cols]
            h, r = weights_x[0] * value, weights_r[0] * value
            for j in range(1, STEPS + 1):
                value = fields[j + 1, wide, cols]
                h, r = h + weights_x[j] * value, r + weights_r[j] * value
            height[keep, cols] = h
            resid[keep, cols] = r


def combine(sums, fields, width):
    plane = jax.ShapeDtypeStruct((width, fields.shape[2]), jnp.float32)
    vmem = pl.BlockSpec(memory_space=pltpu.VMEM)
    return pl.pallas_call(
        combine_kernel,
        out_shape=[plane, plane],
        in_specs=[vmem, vmem],
        out_specs=[vmem, vmem],
        compiler_params=pltpu.CompilerParams(vmem_limit_bytes=8 * 1024 * 1024),
        name="combine",
    )(sums, fields)


def on_device(
    heat_anomaly,
    saltiness_anomaly,
    first_axis_flow,
    second_axis_flow,
    layer_spacing,
    diagonal_shift,
    water_tile_flags,
):
    members = lax.axis_size("blk")
    bands = fetch(heat_anomaly, saltiness_anomaly, first_axis_flow, second_axis_flow)
    to_next, to_last, table = pack(water_tile_flags, layer_spacing[None], diagonal_shift, bands)
    forward = [(i, (i + 1) % members) for i in range(members)]
    backward = [(target, source) for source, target in forward]
    low = lax.ppermute(to_next, "blk", forward)
    high = lax.ppermute(to_last, "blk", backward)
    staged, start = inner_advance(table, bands)
    *tracers, basis, sums = edge_advance(
        staged, start, diagonal_shift, table, low, high, bands, members
    )
    gathered = lax.all_to_all(sums, "blk", 0, 0, tiled=True)
    height, resid = combine(gathered, basis, diagonal_shift.shape[0])
    return (*tracers, height, resid)


def solution(mesh):
    columns = P("member", "blk", None)
    return jax.shard_map(
        on_device,
        mesh=mesh,
        in_specs=(columns, columns, columns, columns, P(), P("blk", None), P("blk", None)),
        out_specs=(
            columns,
            columns,
            columns,
            columns,
            P(("member", "blk"), None),
            P(("member", "blk"), None),
        ),
        check_vma=False,
    )
```
